128 devices in a mesh: rad: 8 (over z, x_lo), ang: 16 (over y, x_hi, core).
Axes of the slice: x: 4 (x_hi: 2, x_lo: 2; x = x_hi * 2 + x_lo), y: 4, z: 4, core: 2. Of those that a mesh axis runs over, the one named last changes fastest.
Arguments:
- state: float32 [4, 64, 512, 1024], P(None, 'rad', 'ang'), may hold values from -4 to 4, as said below
Outputs:
- increment: float32 [4, 64, 512, 1024], P(None, 'rad', 'ang')
- potential: float32 [64, 512, 1024], P('rad', 'ang')
The draws below stay inside these ranges and needn't reach their ends.
Inputs may be any that keep to these rules, and one draw needn't show every extreme that they name: `state`: component 0 (density) lies between 0.5 and 2; components 1 to 3 (momentum) between -4 and 4.
All inputs are finite; a program needn't handle non-finite values.
Results may differ from the reference program's by a relative error of at most 0.0003.
Values sent between devices are 32-bit elements; how exact they have to be, the bound alone decides.
A program may use at most 192 MiB of HBM per device.

```python
import math
import jax
import jax.numpy as jnp
from jax import lax

NT = 512
NP = 1024
LMAX = 48
MPAD = 64
SHELL_DEV = 8
NR = 64
N_RAD = 8


def draw_state(key, part):
    first_key = jax.random.fold_in(key, 11)
    second_key = jax.random.fold_in(key, 12)
    width_key = jax.random.fold_in(key, 13)
    low_key = jax.random.fold_in(key, 14)
    high_key = jax.random.fold_in(key, 15)
    phase_key = jax.random.fold_in(key, 16)
    pitch_key = jax.random.fold_in(key, 17)
    amp_key = jax.random.fold_in(key, 18)
    tilt_key = jax.random.fold_in(key, 19)
    shell_pos = (jnp.arange(NR, dtype=jnp.float32) + 0.5) / NR
    theta = math.pi / NT * (jnp.arange(NT, dtype=jnp.float32) + 0.5)
    phi_angle = 2.0 * math.pi / NP * jnp.arange(NP, dtype=jnp.float32)
    low_orders = jax.random.randint(low_key, (2,), 1, LMAX // 2 + 1)
    high_orders = jax.random.randint(high_key, (2,), LMAX // 2 + 1, LMAX + 1)
    mode_orders = jnp.concatenate([low_orders, high_orders]).astype(jnp.float32)
    phases = jax.random.uniform(phase_key, (5,), jnp.float32, -math.pi, math.pi)
    pitches = jax.random.uniform(pitch_key, (4,), jnp.float32, 1.0, 4.0)
    disk_width = jax.random.uniform(width_key, (), jnp.float32, 0.25, 0.4)
    tilt = jax.random.uniform(tilt_key, (), jnp.float32, -0.5, 0.5)
    amps = jax.random.uniform(amp_key, (4,), jnp.float32, 0.4, 0.7)
    offset = -1.2
    noise = 0.3 * jnp.clip(jax.random.normal(first_key, (NR, NT, NP), jnp.float32), -4.0, 4.0)
    momentum = jnp.clip(jax.random.normal(second_key, (3, NR, NT, NP), jnp.float32), -4.0, 4.0)
    disk = jnp.exp(-((theta - 0.5 * math.pi) / disk_width) ** 2) * (1.0 + tilt * jnp.cos(theta))
    radial = 0.75 + 0.25 * jnp.cos(2.0 * math.pi * shell_pos + phases[4])
    spiral = jnp.zeros((NR, 1, NP), jnp.float32)
    for index in range(4):
        spiral = spiral + amps[index] * jnp.cos(mode_orders[index] * phi_angle[None, None, :] + (2.0 * math.pi * pitches[index] * shell_pos + phases[index])[:, None, None])
    level = offset + 2.4 * disk[None, :, None] * radial[:, None, None] + disk[None, :, None] * spiral + noise
    density = 0.5 + 1.5 * jax.nn.sigmoid(level)
    return jnp.concatenate([density[None], momentum], axis=0)


def setup_inputs(seed: int = 0) -> dict:
    key_list = jax.random.split(jax.random.key(seed), 2)
    state = draw_state(jax.random.fold_in(key_list[1], 71), 0)
    return dict(state=state)


sound_speed = 0.5
sound_sq = 0.25
grav_const = 100.0
section_step = 0.001
inner_radius = 1.0
radial_span = 0.1
face_weights = (1.0, -8.0, 37.0, 37.0, -8.0, 1.0)
precise = lax.Precision.HIGHEST

def legendre_table(cosine, sine_row, lmax, mpad):
    column = [jnp.full_like(cosine, 1.0 / math.sqrt(4.0 * math.pi))]
    for m_order in range(1, mpad):
        column.append(column[-1] * sine_row * math.sqrt((2.0 * m_order + 1.0) / (2.0 * m_order)))
    orders = jnp.arange(mpad, dtype=jnp.float32)
    start_level = jnp.stack(column, axis=1)
    levels = [start_level, start_level * cosine[:, None] * jnp.sqrt(2.0 * orders + 3.0)[None, :]]
    for offset in range(2, mpad):
        degree = orders + offset
        coef_alpha = jnp.sqrt((4.0 * degree * degree - 1.0) / (degree * degree - orders * orders))
        coef_beta = jnp.sqrt(((degree - 1.0) ** 2 - orders * orders) / (4.0 * (degree - 1.0) ** 2 - 1.0))
        levels.append(coef_alpha[None, :] * (cosine[:, None] * levels[-1] - coef_beta[None, :] * levels[-2]))
    leg_table = jnp.stack(levels, axis=2)
    keep_mask = orders[:, None] + orders[None, :] <= lmax
    return jnp.where(keep_mask[None], leg_table, 0.0)

def phi_basis(count, mpad):
    phi_angle = 2.0 * math.pi / count * jnp.arange(count, dtype=jnp.float32)
    orders = jnp.arange(mpad, dtype=jnp.float32)
    norm_scale = jnp.where(orders > 0.5, math.sqrt(2.0), 1.0)
    phi_phase = phi_angle[:, None] * orders[None, :]
    return jnp.concatenate([jnp.cos(phi_phase) * norm_scale, jnp.sin(phi_phase) * norm_scale], axis=1)

def degree_list(mpad):
    orders = jnp.arange(mpad, dtype=jnp.float32)
    degree_grid = (orders[:, None] + orders[None, :]).reshape(-1)
    return jnp.concatenate([degree_grid, degree_grid])

def coefficients(inner, outer, radii, degree):
    radial_power = jnp.power(radii[:, None], degree[None, :])
    norm_scale = -4.0 * math.pi / (2.0 * degree + 1.0)
    cell_rad = radii[:, None]
    coef_potential = norm_scale * (inner / (cell_rad * radial_power) + radial_power * outer)
    coef_slope = norm_scale * (-(degree + 1.0) * inner / (cell_rad * cell_rad * radial_power) + degree * radial_power * outer / cell_rad)
    return (coef_potential, coef_slope)

def face_terms(extended, axis, count, component):
    face_value = 0.0
    for offset, weight in enumerate(face_weights):
        face_value = face_value + weight * lax.slice_in_dim(extended, offset, offset + count + 1, axis=axis)
    face_value = face_value / 60.0
    face_jump = lax.slice_in_dim(extended, 3, 4 + count, axis=axis) - lax.slice_in_dim(extended, 2, 3 + count, axis=axis)
    density = face_value[0]
    face_speed = face_value[component] / density
    face_flux = face_value * face_speed[None]
    face_flux = face_flux.at[component].add(sound_sq * density)
    wave_speed = sound_speed + jnp.abs(face_speed)
    return face_flux - 0.5 * wave_speed[None] * face_jump

def section_increment(radial_ext, polar_ext, center, field_ext, slope, shell_start, total_shells, row_start, total_rows):
    shell_count = center.shape[1]
    row_count = center.shape[2]
    column_count = center.shape[3]
    step_r = radial_span / total_shells
    step_t = math.pi / total_rows
    step_p = 2.0 * math.pi / column_count
    face_index = (shell_start + jnp.arange(shell_count + 1)).astype(jnp.float32)
    open_r = (face_index > 0.5) & (face_index < total_shells - 0.5)
    face_radius = inner_radius + step_r * face_index
    area_r = jnp.where(open_r, face_radius * face_radius, 0.0)
    cell_radius = inner_radius + step_r * ((shell_start + jnp.arange(shell_count)).astype(jnp.float32) + 0.5)
    face_row = (row_start + jnp.arange(row_count + 1)).astype(jnp.float32)
    open_t = (face_row > 0.5) & (face_row < total_rows - 0.5)
    area_t = jnp.where(open_t, jnp.sin(step_t * face_row), 0.0)
    cell_theta = step_t * ((row_start + jnp.arange(row_count)).astype(jnp.float32) + 0.5)
    sine_cell = jnp.sin(cell_theta)[None, :, None]
    cosine = jnp.cos(cell_theta)[None, :, None]
    radius = cell_radius[:, None, None]
    flux_r = face_terms(radial_ext, 1, shell_count, 1)
    weighted = flux_r * area_r[None, :, None, None]
    tendency = -(weighted[:, 1:] - weighted[:, :-1]) * (sine_cell / step_r)[None]
    flux_t = face_terms(polar_ext, 2, row_count, 2)
    weighted = flux_t * area_t[None, None, :, None]
    tendency = tendency - (weighted[:, :, 1:] - weighted[:, :, :-1]) * (radius / step_t)[None]
    wrapped = jnp.concatenate([center[..., -3:], center, center[..., :3]], axis=3)
    flux_p = face_terms(wrapped, 3, column_count, 3)
    tendency = tendency - (flux_p[..., 1:] - flux_p[..., :-1]) * (radius / step_p)[None]
    density = center[0]
    vel_r = center[1] / density
    vel_t = center[2] / density
    vel_p = center[3] / density
    pressure = sound_sq * density
    potential = field_ext[:, 1:-1]
    grad_t = (field_ext[:, 2:] - field_ext[:, :-2]) / (2.0 * step_t)
    grad_p = (jnp.roll(potential, -1, axis=2) - jnp.roll(potential, 1, axis=2)) / (2.0 * step_p)
    source_r = radius * sine_cell * (density * (vel_t * vel_t + vel_p * vel_p) + 2.0 * pressure) - grav_const * radius * radius * sine_cell * density * slope
    source_t = radius * (-density * vel_r * vel_t * sine_cell + (density * vel_p * vel_p + pressure) * cosine) - grav_const * radius * sine_cell * density * grad_t
    source_p = -radius * density * vel_p * (vel_r * sine_cell + vel_t * cosine) - grav_const * radius * density * grad_p
    source = jnp.stack([jnp.zeros_like(density), source_r, source_t, source_p])
    return (section_step * (tendency + source), potential)

def reference(state):
    total_shells = state.shape[1]
    total_rows = state.shape[2]
    column_count = state.shape[3]
    step_r = radial_span / total_shells
    step_t = math.pi / total_rows
    step_p = 2.0 * math.pi / column_count
    theta_ext = step_t * ((jnp.arange(total_rows + 2) - 1).astype(jnp.float32) + 0.5)
    leg_ext = legendre_table(jnp.cos(theta_ext), jnp.sin(theta_ext), LMAX, MPAD)
    basis = phi_basis(column_count, MPAD)
    spectra = jnp.dot(state[0].reshape(-1, column_count), basis, precision=precise).reshape(total_shells, total_rows, 2, MPAD)
    weights = leg_ext[1:-1] * (jnp.sin(theta_ext[1:-1]) * step_t * step_p)[:, None, None]
    moments = jnp.einsum('rtsm,tmk->rsmk', spectra, weights, precision=precise).reshape(total_shells, -1)
    degree_all = degree_list(MPAD)
    radii = inner_radius + step_r * (jnp.arange(total_shells).astype(jnp.float32) + 0.5)
    radial_power = jnp.power(radii[:, None], degree_all[None, :])
    weighted = (radii * radii * step_r)[:, None] * moments
    up_terms = radial_power * weighted
    down_terms = weighted / (radii[:, None] * radial_power)
    inner = jnp.cumsum(up_terms, axis=0)
    down_cum = jnp.cumsum(down_terms, axis=0)
    outer = down_cum[-1][None] - down_cum
    coef_potential, coef_slope = coefficients(inner, outer, radii, degree_all)
    stacked = jnp.stack([coef_potential, coef_slope]).reshape(2, total_shells, 2, MPAD, MPAD)
    padded = jnp.pad(state, ((0, 0), (3, 3), (3, 3), (0, 0)))
    block = SHELL_DEV

    def one_block(index):
        first = (index * block).astype(jnp.int32)
        piece = lax.dynamic_slice_in_dim(padded, first, block + 6, axis=1)
        coef_piece = lax.dynamic_slice_in_dim(stacked, first, block, axis=1)
        synth = jnp.einsum('frsmk,tmk->frtsm', coef_piece, leg_ext, precision=precise)
        fields = jnp.dot(synth.reshape(-1, 2 * MPAD), basis.T, precision=precise).reshape(2, block, total_rows + 2, column_count)
        center = piece[:, 3:-3, 3:-3]
        return section_increment(piece[:, :, 3:-3], piece[:, 3:-3], center, fields[0], fields[1][:, 1:-1], first, total_shells, 0, total_rows)
    increments, potentials = lax.map(one_block, jnp.arange(N_RAD, dtype=jnp.int32))
    increment = jnp.moveaxis(increments, 0, 1).reshape(4, total_shells, total_rows, column_count)
    potential = potentials.reshape(total_shells, total_rows, column_count)
    return (increment, potential)
```

```python
import functools
import math

import jax
import jax.numpy as jnp
import numpy as np
from jax import lax
from jax.experimental import pallas as pl
from jax.experimental.pallas import tpu as pltpu
from jax.sharding import PartitionSpec as P

LMAX = 48
MPAD = 64
LANES = 128
NK = 56
GROUPS = 8
KD = 7
PADR = 8
WIDTH = 3
ROWS = 8

sound_speed = 0.5
sound_sq = 0.25
grav_const = 100.0
section_step = 0.001
inner_radius = 1.0
radial_span = 0.1
MESH = pl.DeviceIdType.MESH
f32 = jnp.float32
bf16 = jnp.bfloat16


def split_np(table):
    high = table.astype(bf16)
    low = (table - high.astype(np.float64)).astype(bf16)
    return high, low


def phi_tables(count):
    order = np.arange(MPAD, dtype=np.float64)
    norm = np.where(order > 0.5, math.sqrt(2.0), 1.0)
    phase = (2.0 * math.pi / count) * (np.outer(np.arange(count), np.arange(MPAD)) % count)
    table = np.concatenate([np.cos(phase) * norm, np.sin(phase) * norm], axis=1)
    high, low = split_np(table)
    back = np.concatenate([high.T, high.T, low.T], axis=0)
    step = 2.0 * math.pi / count
    slope = np.sin(order * step) / step
    return high, low, back, np.concatenate([slope, -slope])


def row_tables(blocks, rows):
    total = blocks * rows
    step_t = math.pi / total
    row = np.arange(blocks)[:, None] * rows + np.arange(rows + 2 * PADR)[None, :] - PADR
    theta = step_t * (row + 0.5)
    face = np.where((row > 0) & (row < total), np.sin(step_t * row), 0.0)
    table = np.zeros((blocks, rows + 2 * PADR, LANES))
    table[:, :, 0] = np.cos(theta)
    table[:, :, 1] = np.sin(theta)
    table[:, :, 2] = face
    return table.astype(np.float32)


def degree_tables(slope):
    m = np.arange(LANES) % MPAD
    k = np.arange(NK)[:, None]
    l = (m + k).astype(np.float64)
    alpha = np.zeros((NK, LANES))
    beta = np.zeros((NK, LANES))
    norm = np.full(LANES, 1.0 / math.sqrt(4.0 * math.pi))
    for q in range(1, MPAD):
        norm = np.where(m >= q, norm * math.sqrt((2.0 * q + 1.0) / (2.0 * q)), norm)
    alpha[0] = norm
    alpha[1:] = np.sqrt((4.0 * l[1:] ** 2 - 1.0) / (l[1:] ** 2 - m**2))
    beta[2:] = np.sqrt(((l[2:] - 1.0) ** 2 - m**2) / (4.0 * (l[2:] - 1.0) ** 2 - 1.0))
    alpha = np.where(l <= LMAX, alpha, 0.0)
    extra = np.zeros((8, LANES))
    extra[0] = slope
    return np.concatenate([alpha, beta, extra]).astype(np.float32)


def log_radii(blocks, shells):
    radius = inner_radius + radial_span / (blocks * shells) * (np.arange(blocks * shells) + 0.5)
    table = np.log(radius).reshape(blocks, shells, 1)
    return np.broadcast_to(table, (blocks, shells, LANES)).astype(np.float32)


def split(value):
    high = value.astype(bf16)
    return high, (value - high.astype(f32)).astype(bf16)


def dot(a, b):
    return jnp.dot(a, b, preferred_element_type=f32)


def flux(sums, jumps, component):
    inverse = 1.0 / sums[0]
    speed = sums[component] * inverse
    scaled = speed * (1.0 / 60.0)
    wave = 0.5 * (sound_speed + jnp.abs(speed))
    out = [s * scaled - wave * j for s, j in zip(sums, jumps)]
    out[component] = out[component] + (sound_sq / 60.0) * sums[0]
    return out


def kernel(
    n_rad,
    n_ang,
    shells,
    rows,
    cols,
    x_ref,
    fwd_high_ref,
    fwd_low_ref,
    back_ref,
    row_ref,
    degree_ref,
    log_ref,
    inc_ref,
    pot_ref,
    ext,
    lo,
    hi,
    tend,
    pot,
    fields,
    table,
    spec,
    rowtab,
    leg,
    partial,
    got_a,
    mine,
    got_b,
    tot_up,
    tot_down,
    got_up,
    got_down,
    coef,
    local_sem,
    out_sem,
    ang_send,
    ang_recv,
    rad_send,
    rad_recv,
    a_send,
    a_recv,
    b_send,
    b_recv,
    c_send,
    c_recv,
    d_send,
    d_recv,
):
    r = lax.axis_index("rad")
    a = lax.axis_index("ang")
    y, x_hi, core = a // 4, (a // 2) % 2, a % 2
    g = y * 2 + core
    chunks = rows // ROWS
    span = rows + 2 * PADR
    own = pl.ds(PADR, rows)
    step_r = radial_span / (n_rad * shells)
    step_t = math.pi / (n_ang * rows)
    step_p = 2.0 * math.pi / cols

    def peer(d):
        q = (g + d) % GROUPS
        return (r, (q // 2) * 4 + x_hi * 2 + q % 2)

    partner = (r, y * 4 + (1 - x_hi) * 2 + core)

    def when(cond, run):
        @pl.when(cond)
        def _():
            run()

    def remote(src, dst, send, recv, dev):
        return pltpu.make_async_remote_copy(
            src_ref=src,
            dst_ref=dst,
            send_sem=send,
            recv_sem=recv,
            device_id=dev,
            device_id_type=MESH,
        )

    load_density = pltpu.make_async_copy(x_ref.at[0], ext.at[0, :, own], local_sem.at[0])
    load_rest = pltpu.make_async_copy(
        x_ref.at[1:4], ext.at[1:4, :, own], local_sem.at[1]
    )
    load_rows = pltpu.make_async_copy(row_ref.at[a], rowtab, local_sem.at[2])
    load_density.start()
    load_rest.start()
    load_rows.start()

    got_up[...] = jnp.zeros_like(got_up)
    got_down[...] = jnp.zeros_like(got_down)

    @pl.when(a == 0)
    def _():
        ext[:, :, 0:PADR, :] = jnp.zeros((4, shells, PADR, cols), f32)

    @pl.when(a == n_ang - 1)
    def _():
        ext[:, :, PADR + rows : span, :] = jnp.zeros((4, shells, PADR, cols), f32)

    @pl.when(r == 0)
    def _():
        lo[...] = jnp.zeros_like(lo)

    @pl.when(r == n_rad - 1)
    def _():
        hi[...] = jnp.zeros_like(hi)

    barrier = pltpu.get_barrier_semaphore()

    def greet(cond, dev):
        when(
            cond,
            lambda: pl.semaphore_signal(barrier, inc=1, device_id=dev, device_id_type=MESH),
        )

    for d in range(1, n_rad):
        greet(r + d < n_rad, (r + d, a))
        greet(r - d >= 0, (r - d, a))
    for d in range(1, GROUPS):
        pl.semaphore_signal(barrier, inc=1, device_id=peer(d), device_id_type=MESH)
    pl.semaphore_signal(barrier, inc=1, device_id=partner, device_id_type=MESH)
    greet(a + 1 < n_ang, (r, a + 1))
    greet(a > 0, (r, a - 1))
    ends = jnp.where(a > 0, 1, 0) + jnp.where(a + 1 < n_ang, 1, 0)

    pl.semaphore_wait(barrier, n_rad - 1 + GROUPS + ends)

    ang_up = remote(
        x_ref.at[:, :, rows - WIDTH : rows],
        ext.at[:, :, PADR - WIDTH : PADR],
        ang_send.at[0],
        ang_recv.at[0],
        (r, a + 1),
    )
    ang_down = remote(
        x_ref.at[:, :, 0:WIDTH],
        ext.at[:, :, PADR + rows : PADR + rows + WIDTH],
        ang_send.at[1],
        ang_recv.at[1],
        (r, a - 1),
    )
    rad_up = []
    rad_down = []
    for c in range(chunks):
        part = pl.ds(c * ROWS, ROWS)
        rad_up.append(
            remote(
                x_ref.at[:, shells - WIDTH : shells, part],
                lo.at[:, :, part],
                rad_send.at[0, c],
                rad_recv.at[0, c],
                (r + 1, a),
            )
        )
        rad_down.append(
            remote(
                x_ref.at[:, 0:WIDTH, part],
                hi.at[:, :, part],
                rad_send.at[1, c],
                rad_recv.at[1, c],
                (r - 1, a),
            )
        )

    def start_chunk(c):
        when(r + 1 < n_rad, rad_up[c].start)
        when(r > 0, rad_down[c].start)

    when(a + 1 < n_ang, ang_up.start)
    when(a > 0, ang_down.start)
    start_chunk(0)

    load_rows.wait()
    cosine = jnp.broadcast_to(rowtab[:, 0:1], (span, LANES))
    sine = jnp.broadcast_to(rowtab[:, 1:2], (span, LANES))
    order = lax.broadcasted_iota(jnp.int32, (span, LANES), 1) % MPAD
    power = jnp.full((span, LANES), 1.0, f32)
    square = sine
    for bit in range(6):
        power = jnp.where((order // (1 << bit)) % 2 == 1, power * square, power)
        square = square * square
    level = power * degree_ref[0:1, :]
    leg[0] = level

    def next_level(k, carry):
        last, before = carry
        alpha = degree_ref[pl.ds(k, 1), :]
        beta = degree_ref[pl.ds(NK + k, 1), :]
        new = alpha * (cosine * last - beta * before)
        leg[k] = new
        return (new, last)

    lax.fori_loop(1, NK, next_level, (level, jnp.zeros_like(level)))

    load_density.wait()
    weight = sine[PADR : PADR + rows] * (step_t * step_p)
    half = shells // 2
    for h in range(2):
        cells = ext[0, h * half : (h + 1) * half, PADR : PADR + rows, :]
        high, low = split(cells.reshape(half * rows, cols))
        sums = dot(high, fwd_high_ref[...]) + (
            dot(low, fwd_high_ref[...]) + dot(high, fwd_low_ref[...])
        )
        for q in range(half):
            spec[pl.ds((h * half + q) * rows, rows), :] = (
                sums[q * rows : (q + 1) * rows] * weight
            )
    spectra = [spec[pl.ds(j, shells, stride=rows), :] for j in range(rows)]

    def moment(k, carry):
        parts = [jnp.zeros((shells, LANES), f32) for _ in range(4)]
        for j in range(rows):
            parts[j % 4] = parts[j % 4] + spectra[j] * leg[k, PADR + j : PADR + j + 1, :]
        partial[k // KD, k % KD] = (parts[0] + parts[1]) + (parts[2] + parts[3])
        return carry

    lax.fori_loop(0, NK, moment, 0)

    def exchange_a(d):
        return remote(
            partial.at[(g + d) % GROUPS], got_a.at[d], a_send.at[d], a_recv.at[d], peer(d)
        )

    for d in range(1, GROUPS):
        exchange_a(d).start()

    load_rest.wait()

    def phi_flux(index, carry):
        i = index // chunks
        at = pl.multiple_of((index % chunks) * ROWS, ROWS)
        cell_radius = inner_radius + step_r * ((r * shells + i).astype(f32) + 0.5)
        sums, jumps = [], []
        for c in range(4):
            u = ext[c, i, pl.ds(PADR + at, ROWS), :]
            left = pltpu.roll(u, 1, 1)
            near = u + left
            mid = pltpu.roll(u, cols - 1, 1) + pltpu.roll(u, 2, 1)
            far = pltpu.roll(u, cols - 2, 1) + pltpu.roll(u, 3, 1)
            sums.append(37.0 * near - 8.0 * mid + far)
            jumps.append(u - left)
        for c, face in enumerate(flux(sums, jumps, 3)):
            tend[c, i, pl.ds(at, ROWS), :] = (face - pltpu.roll(face, cols - 1, 1)) * (
                cell_radius / step_p
            )
        return carry

    lax.fori_loop(0, shells * chunks // 2, phi_flux, 0)

    for d in range(1, GROUPS):
        exchange_a(d).wait_recv()
    total = partial[g]
    for d in range(1, GROUPS):
        total = total + got_a[d]
    mine[...] = total
    exchange_b = remote(mine, got_b, b_send.at[0], b_recv.at[0], partner)
    exchange_b.start()
    start_chunk(1)

    lax.fori_loop(shells * chunks // 2, shells * chunks, phi_flux, 0)

    when(a > 0, ang_up.wait_recv)
    when(a + 1 < n_ang, ang_down.wait_recv)
    tiles = cols // LANES

    def theta_flux(index, carry):
        i = index // tiles
        lanes = pl.ds(pl.multiple_of((index % tiles) * LANES, LANES), LANES)
        cell_radius = inner_radius + step_r * ((r * shells + i).astype(f32) + 0.5)
        area = jnp.broadcast_to(rowtab[:, 2:3], (span, LANES)) * (cell_radius / step_t)
        sums, jumps = [], []
        for c in range(4):
            u = ext[c, i, :, lanes]
            left = pltpu.roll(u, 1, 0)
            near = u + left
            mid = pltpu.roll(u, span - 1, 0) + pltpu.roll(u, 2, 0)
            far = pltpu.roll(u, span - 2, 0) + pltpu.roll(u, 3, 0)
            sums.append(37.0 * near - 8.0 * mid + far)
            jumps.append(u - left)
        for c, face in enumerate(flux(sums, jumps, 2)):
            face = face * area
            change = face - pltpu.roll(face, span - 1, 0)
            tend[c, i, :, lanes] = tend[c, i, :, lanes] + change[PADR : PADR + rows]
        return carry

    lax.fori_loop(0, shells * tiles // 2, theta_flux, 0)

    exchange_b.wait_recv()
    total = mine[...] + got_b[...]
    log_radius = log_ref[r]
    shell = lax.broadcasted_iota(jnp.int32, (shells, LANES), 0)
    radius = inner_radius + step_r * ((r * shells + shell).astype(f32) + 0.5)
    order = lax.broadcasted_iota(jnp.int32, (shells, LANES), 1) % MPAD
    ups, downs, powers, degrees = [], [], [], []
    for q in range(KD):
        degree = (order + (g * KD + q)).astype(f32)
        grow = jnp.exp(degree * log_radius)
        weighted = (radius * radius * step_r) * total[q]
        up = grow * weighted
        down = weighted / (radius * grow)
        for s in (1, 2, 4):
            up = up + jnp.where(shell >= s, pltpu.roll(up, s, 0), 0.0)
            down = down + jnp.where(shell >= s, pltpu.roll(down, s, 0), 0.0)
        tot_up[q : q + 1, :] = up[shells - 1 : shells]
        tot_down[q : q + 1, :] = down[shells - 1 : shells]
        ups.append(up)
        downs.append(down)
        powers.append(grow)
        degrees.append(degree)

    def exchange_up(d):
        return remote(tot_up, got_up.at[d], c_send.at[0, d], c_recv.at[0, d], (r + d, a))

    def exchange_down(d):
        return remote(tot_down, got_down.at[d], c_send.at[1, d], c_recv.at[1, d], (r - d, a))

    for d in range(1, n_rad):
        when(r + d < n_rad, exchange_up(d).start)
        when(r - d >= 0, exchange_down(d).start)
    start_chunk(2)

    lax.fori_loop(shells * tiles // 2, shells * tiles, theta_flux, 0)

    for d in range(1, n_rad):
        when(r - d >= 0, exchange_up(d).wait_recv)
        when(r + d < n_rad, exchange_down(d).wait_recv)
    below = got_up[1]
    above = got_down[1]
    for d in range(2, n_rad):
        below = below + got_up[d]
        above = above + got_down[d]
    inverse_radius = 1.0 / radius
    for q in range(KD):
        inner = below[q : q + 1] + ups[q]
        outer = above[q : q + 1] + (downs[q][shells - 1 : shells] - downs[q])
        degree = degrees[q]
        norm = (-4.0 * math.pi) / (2.0 * degree + 1.0)
        inner_term = inner * inverse_radius / powers[q]
        outer_term = powers[q] * outer
        coef[g, 0, q] = norm * (inner_term + outer_term)
        coef[g, 1, q] = (
            norm * (degree * outer_term - (degree + 1.0) * inner_term) * inverse_radius
        )

    def exchange_d(d):
        return remote(coef.at[g], coef.at[g], d_send.at[d], d_recv.at[d], peer(d))

    for d in range(1, GROUPS):
        exchange_d(d).start()
    start_chunk(3)
    for d in range(1, GROUPS):
        exchange_d(d).wait_recv()

    slope_row = degree_ref[2 * NK : 2 * NK + 1, :]
    theta_scale = 1.0 / (2.0 * step_t)
    for i in range(0, shells, 2):

        def synthesize(h, carry):
            sums = list(carry)
            for q in range(KD):
                k = h * KD + q
                full = leg[k]
                value = full[PADR : PADR + rows]
                change = pltpu.roll(full, span - 1, 0) - pltpu.roll(full, 1, 0)
                change = change[PADR : PADR + rows]
                for p in range(2):
                    cp = coef[h, 0, q, i + p : i + p + 1, :]
                    cs = coef[h, 1, q, i + p : i + p + 1, :]
                    sums[3 * p] = sums[3 * p] + value * cp
                    sums[3 * p + 1] = sums[3 * p + 1] + value * cs
                    sums[3 * p + 2] = sums[3 * p + 2] + change * cp
            return tuple(sums)

        zero = jnp.zeros((rows, LANES), f32)
        sums = lax.fori_loop(0, (LMAX + KD) // KD, synthesize, (zero,) * 6)
        for p in range(2):
            base, slope, change = sums[3 * p : 3 * p + 3]
            at = (i + p) * 4 * rows
            table[at : at + rows, :] = base
            table[at + rows : at + 2 * rows, :] = slope
            table[at + 2 * rows : at + 3 * rows, :] = change * theta_scale
            table[at + 3 * rows : at + 4 * rows, :] = pltpu.roll(base, MPAD, 1) * slope_row

    def sources(i, carry):
        at = pl.multiple_of(i * 4 * rows, 4 * rows)
        high, low = split(table[pl.ds(at, 4 * rows), :])
        fields[...] = dot(jnp.concatenate([high, low, high], axis=1), back_ref[...])
        pot[i] = fields[0:rows, :]
        cell_radius = inner_radius + step_r * ((r * shells + i).astype(f32) + 0.5)
        for c in range(chunks):
            at = c * ROWS
            inside = pl.ds(PADR + at, ROWS)
            sine = jnp.broadcast_to(rowtab[inside, 1:2], (ROWS, cols)) * cell_radius
            cosine = jnp.broadcast_to(rowtab[inside, 0:1], (ROWS, cols)) * cell_radius
            density = ext[0, i, inside, :]
            mom_r = ext[1, i, inside, :]
            mom_t = ext[2, i, inside, :]
            mom_p = ext[3, i, inside, :]
            inverse = 1.0 / density
            vel_t = mom_t * inverse
            vel_p = mom_p * inverse
            pull = grav_const * density
            slope = fields[rows + at : rows + at + ROWS, :]
            grad_t = fields[2 * rows + at : 2 * rows + at + ROWS, :]
            grad_p = fields[3 * rows + at : 3 * rows + at + ROWS, :]
            twist = mom_p * vel_p
            source_r = sine * (
                (mom_t * vel_t + twist)
                + (2.0 * sound_sq) * density
                - (cell_radius * pull) * slope
            )
            source_t = cosine * (twist + sound_sq * density) - sine * (
                mom_r * vel_t + pull * grad_t
            )
            source_p = -(
                vel_p * (mom_r * sine + mom_t * cosine) + (cell_radius * pull) * grad_p
            )
            spot = pl.ds(at, ROWS)
            tend[1, i, spot, :] = tend[1, i, spot, :] + source_r
            tend[2, i, spot, :] = tend[2, i, spot, :] + source_t
            tend[3, i, spot, :] = tend[3, i, spot, :] + source_p
        return carry

    lax.fori_loop(0, shells, sources, 0)
    store_pot = pltpu.make_async_copy(pot, pot_ref, out_sem.at[chunks])
    store_pot.start()

    stores = []
    for chunk in range(chunks):
        when(r > 0, rad_up[chunk].wait_recv)
        when(r + 1 < n_rad, rad_down[chunk].wait_recv)
        at = chunk * ROWS
        spot = pl.ds(at, ROWS)

        def radial_flux(tile, carry):
            lanes = pl.ds(pl.multiple_of(tile * LANES, LANES), LANES)
            sine = jnp.broadcast_to(
                rowtab[PADR + at : PADR + at + ROWS, 1:2], (ROWS, LANES)
            ) * (section_step / step_r)

            def cell(c, s):
                if s < 0:
                    return lo[c, s + WIDTH, spot, lanes]
                if s >= shells:
                    return hi[c, s - shells, spot, lanes]
                return ext[c, s, pl.ds(PADR + at, ROWS), lanes]

            u = [[cell(c, s) for s in range(-WIDTH, shells + WIDTH)] for c in range(4)]
            last = None
            for f in range(shells + 1):
                place = r * shells + f
                face_radius = inner_radius + step_r * place.astype(f32)
                area = jnp.where(
                    (place > 0) & (place < n_rad * shells), face_radius * face_radius, 0.0
                )
                sums, jumps = [], []
                for c in range(4):
                    w = u[c][f : f + 6]
                    sums.append(37.0 * (w[2] + w[3]) - 8.0 * (w[1] + w[4]) + (w[0] + w[5]))
                    jumps.append(w[3] - w[2])
                face = [value * area for value in flux(sums, jumps, 1)]
                if f > 0:
                    for c in range(4):
                        tend[c, f - 1, spot, lanes] = (
                            section_step * tend[c, f - 1, spot, lanes]
                            - (face[c] - last[c]) * sine
                        )
                last = face
            return carry

        lax.fori_loop(0, tiles, radial_flux, 0)
        store = pltpu.make_async_copy(
            tend.at[:, :, spot], inc_ref.at[:, :, spot], out_sem.at[chunk]
        )
        store.start()
        stores.append(store)

    when(a + 1 < n_ang, ang_up.wait_send)
    when(a > 0, ang_down.wait_send)
    for c in range(chunks):
        when(r + 1 < n_rad, rad_up[c].wait_send)
        when(r > 0, rad_down[c].wait_send)
    for d in range(1, GROUPS):
        exchange_a(d).wait_send()
        exchange_d(d).wait_send()
    exchange_b.wait_send()
    for d in range(1, n_rad):
        when(r + d < n_rad, exchange_up(d).wait_send)
        when(r - d >= 0, exchange_down(d).wait_send)
    store_pot.wait()
    for store in stores:
        store.wait()


def solution(mesh):
    n_rad = mesh.shape["rad"]
    n_ang = mesh.shape["ang"]

    def body(state):
        _, shells, rows, cols = state.shape
        high, low, back, slope = phi_tables(cols)
        operands = (
            state,
            jnp.asarray(high),
            jnp.asarray(low),
            jnp.asarray(back),
            jnp.asarray(row_tables(n_ang, rows)),
            jnp.asarray(degree_tables(slope)),
            jnp.asarray(log_radii(n_rad, shells)),
        )
        span = rows + 2 * PADR
        chunks = rows // ROWS
        anywhere = pl.BlockSpec(memory_space=pl.ANY)
        inside = pl.BlockSpec(memory_space=pltpu.VMEM)
        dma = pltpu.SemaphoreType.DMA
        increment, potential = pl.pallas_call(
            functools.partial(kernel, n_rad, n_ang, shells, rows, cols),
            out_shape=(
                jax.ShapeDtypeStruct(state.shape, f32),
                jax.ShapeDtypeStruct(state.shape[1:], f32),
            ),
            in_specs=[anywhere, inside, inside, inside, anywhere, inside, inside],
            out_specs=(anywhere, anywhere),
            scratch_shapes=[
                pltpu.VMEM((4, shells, span, cols), f32),
                pltpu.VMEM((4, WIDTH, rows, cols), f32),
                pltpu.VMEM((4, WIDTH, rows, cols), f32),
                pltpu.VMEM((4, shells, rows, cols), f32),
                pltpu.VMEM((shells, rows, cols), f32),
                pltpu.VMEM((4 * rows, cols), f32),
                pltpu.VMEM((shells * 4 * rows, LANES), f32),
                pltpu.VMEM((shells * rows, LANES), f32),
                pltpu.VMEM((span, LANES), f32),
                pltpu.VMEM((NK, span, LANES), f32),
                pltpu.VMEM((GROUPS, KD, shells, LANES), f32),
                pltpu.VMEM((GROUPS, KD, shells, LANES), f32),
                pltpu.VMEM((KD, shells, LANES), f32),
                pltpu.VMEM((KD, shells, LANES), f32),
                pltpu.VMEM((8, LANES), f32),
                pltpu.VMEM((8, LANES), f32),
                pltpu.VMEM((n_rad, 8, LANES), f32),
                pltpu.VMEM((n_rad, 8, LANES), f32),
                pltpu.VMEM((GROUPS, 2, KD, shells, LANES), f32),
                dma((3,)),
                dma((chunks + 1,)),
                dma((2,)),
                dma((2,)),
                dma((2, chunks)),
                dma((2, chunks)),
                dma((GROUPS,)),
                dma((GROUPS,)),
                dma((1,)),
                dma((1,)),
                dma((2, n_rad)),
                dma((2, n_rad)),
                dma((GROUPS,)),
                dma((GROUPS,)),
            ],
            compiler_params=pltpu.CompilerParams(
                collective_id=0, has_side_effects=True, vmem_limit_bytes=56 << 20
            ),
        )(*operands)
        return increment, potential

    return jax.shard_map(
        body,
        mesh=mesh,
        in_specs=(P(None, "rad", "ang", None),),
        out_specs=(P(None, "rad", "ang", None), P("rad", "ang", None)),
        check_vma=False,
    )
```

```python
import functools
import math

import jax
import jax.numpy as jnp
import numpy as np
from jax import lax
from jax.experimental import pallas as pl
from jax.experimental.pallas import tpu as pltpu
from jax.sharding import PartitionSpec as P

LMAX = 48
MPAD = 64
LANES = 128
NK = 56
GROUPS = 8
KD = 7
PADR = 8
WIDTH = 3
ROWS = 8

sound_speed = 0.5
sound_sq = 0.25
grav_const = 100.0
section_step = 0.001
inner_radius = 1.0
radial_span = 0.1
MESH = pl.DeviceIdType.MESH
f32 = jnp.float32
bf16 = jnp.bfloat16


def split_np(table):
    high = table.astype(bf16)
    low = (table - high.astype(np.float64)).astype(bf16)
    return high, low


def phi_tables(count):
    order = np.arange(MPAD, dtype=np.float64)
    norm = np.where(order > 0.5, math.sqrt(2.0), 1.0)
    phase = (2.0 * math.pi / count) * (np.outer(np.arange(count), np.arange(MPAD)) % count)
    table = np.concatenate([np.cos(phase) * norm, np.sin(phase) * norm], axis=1)
    high, low = split_np(table)
    back = np.concatenate([high.T, high.T, low.T], axis=0)
    step = 2.0 * math.pi / count
    slope = np.sin(order * step) / step
    return high, low, back, np.concatenate([slope, -slope])


def row_tables(blocks, rows):
    total = blocks * rows
    step_t = math.pi / total
    row = np.arange(blocks)[:, None] * rows + np.arange(rows + 2 * PADR)[None, :] - PADR
    theta = step_t * (row + 0.5)
    face = np.where((row > 0) & (row < total), np.sin(step_t * row), 0.0)
    table = np.zeros((blocks, rows + 2 * PADR, LANES))
    table[:, :, 0] = np.cos(theta)
    table[:, :, 1] = np.sin(theta)
    table[:, :, 2] = face
    return table.astype(np.float32)


def degree_tables(slope):
    m = np.arange(LANES) % MPAD
    k = np.arange(NK)[:, None]
    l = (m + k).astype(np.float64)
    alpha = np.zeros((NK, LANES))
    beta = np.zeros((NK, LANES))
    norm = np.full(LANES, 1.0 / math.sqrt(4.0 * math.pi))
    for q in range(1, MPAD):
        norm = np.where(m >= q, norm * math.sqrt((2.0 * q + 1.0) / (2.0 * q)), norm)
    alpha[0] = norm
    alpha[1:] = np.sqrt((4.0 * l[1:] ** 2 - 1.0) / (l[1:] ** 2 - m**2))
    beta[2:] = np.sqrt(((l[2:] - 1.0) ** 2 - m**2) / (4.0 * (l[2:] - 1.0) ** 2 - 1.0))
    alpha = np.where(l <= LMAX, alpha, 0.0)
    extra = np.zeros((8, LANES))
    extra[0] = slope
    return np.concatenate([alpha, beta, extra]).astype(np.float32)


def log_radii(blocks, shells):
    radius = inner_radius + radial_span / (blocks * shells) * (np.arange(blocks * shells) + 0.5)
    table = np.log(radius).reshape(blocks, shells, 1)
    return np.broadcast_to(table, (blocks, shells, LANES)).astype(np.float32)


def split(value):
    high = value.astype(bf16)
    return high, (value - high.astype(f32)).astype(bf16)


def dot(a, b):
    return jnp.dot(a, b, preferred_element_type=f32)


def flux(sums, jumps, component):
    inverse = 1.0 / sums[0]
    speed = sums[component] * inverse
    scaled = speed * (1.0 / 60.0)
    wave = 0.5 * (sound_speed + jnp.abs(speed))
    out = [s * scaled - wave * j for s, j in zip(sums, jumps)]
    out[component] = out[component] + (sound_sq / 60.0) * sums[0]
    return out


def kernel(
    n_rad,
    n_ang,
    shells,
    rows,
    cols,
    x_ref,
    fwd_high_hbm,
    fwd_low_hbm,
    back_hbm,
    row_hbm,
    degree_hbm,
    log_hbm,
    tend,
    pot,
    ext,
    lo,
    hi,
    relay,
    fields,
    table,
    spec,
    fwd_high_ref,
    fwd_low_ref,
    back_ref,
    rowtab,
    degree_ref,
    log_ref,
    leg,
    partial,
    got_a,
    mine,
    got_b,
    tot_up,
    tot_down,
    got_up,
    got_down,
    coef,
    local_sem,
    ang_send,
    ang_recv,
    rad_send,
    rad_recv,
    far_recv,
    pass_send,
    a_send,
    a_recv,
    b_send,
    b_recv,
    c_send,
    c_recv,
    d_send,
    d_recv,
):
    r = lax.axis_index("rad")
    a = lax.axis_index("ang")
    y, x_hi, core = a // 4, (a // 2) % 2, a % 2
    g = y * 2 + core
    chunks = rows // ROWS
    span = rows + 2 * PADR
    own = pl.ds(PADR, rows)
    step_r = radial_span / (n_rad * shells)
    step_t = math.pi / (n_ang * rows)
    step_p = 2.0 * math.pi / cols

    def peer(d):
        q = (g + d) % GROUPS
        return (r, (q // 2) * 4 + x_hi * 2 + q % 2)

    partner = (r, y * 4 + (1 - x_hi) * 2 + core)

    def when(cond, run):
        @pl.when(cond)
        def _():
            run()

    def remote(src, dst, send, recv, dev):
        return pltpu.make_async_remote_copy(
            src_ref=src,
            dst_ref=dst,
            send_sem=send,
            recv_sem=recv,
            device_id=dev,
            device_id_type=MESH,
        )

    load_density = pltpu.make_async_copy(x_ref.at[0], ext.at[0, :, own], local_sem.at[0])
    load_rest = pltpu.make_async_copy(
        x_ref.at[1:4], ext.at[1:4, :, own], local_sem.at[1]
    )
    load_rows = pltpu.make_async_copy(row_hbm.at[a], rowtab, local_sem.at[2])
    load_degree = pltpu.make_async_copy(degree_hbm, degree_ref, local_sem.at[3])
    load_high = pltpu.make_async_copy(fwd_high_hbm, fwd_high_ref, local_sem.at[4])
    load_low = pltpu.make_async_copy(fwd_low_hbm, fwd_low_ref, local_sem.at[5])
    load_log = pltpu.make_async_copy(log_hbm.at[r], log_ref, local_sem.at[6])
    load_back = pltpu.make_async_copy(back_hbm, back_ref, local_sem.at[7])
    barrier = pltpu.get_barrier_semaphore()

    def greet(cond, dev):
        when(
            cond,
            lambda: pl.semaphore_signal(barrier, inc=1, device_id=dev, device_id_type=MESH),
        )

    for d in range(1, n_rad):
        greet(r + d < n_rad, (r + d, a))
        greet(r - d >= 0, (r - d, a))
    for d in range(1, GROUPS):
        pl.semaphore_signal(barrier, inc=1, device_id=peer(d), device_id_type=MESH)
    pl.semaphore_signal(barrier, inc=1, device_id=partner, device_id_type=MESH)
    greet(a + 1 < n_ang, (r, a + 1))
    greet(a > 0, (r, a - 1))
    ends = jnp.where(a > 0, 1, 0) + jnp.where(a + 1 < n_ang, 1, 0)

    for load in (load_rows, load_degree, load_density, load_high, load_low):
        load.start()
    for load in (load_rest, load_log, load_back):
        load.start()
    pl.semaphore_wait(barrier, n_rad - 1 + GROUPS + ends)

    ang_up = remote(
        x_ref.at[:, :, rows - WIDTH : rows],
        ext.at[:, :, PADR - WIDTH : PADR],
        ang_send.at[0],
        ang_recv.at[0],
        (r, a + 1),
    )
    ang_down = remote(
        x_ref.at[:, :, 0:WIDTH],
        ext.at[:, :, PADR + rows : PADR + rows + WIDTH],
        ang_send.at[1],
        ang_recv.at[1],
        (r, a - 1),
    )
    rad_up, rad_down, far_up, far_down, pass_up, pass_down = [], [], [], [], [], []
    for c in range(chunks):
        part = pl.ds(c * ROWS, ROWS)
        above = x_ref.at[:, shells - WIDTH : shells, part]
        below = x_ref.at[:, 0:WIDTH, part]
        lo_part, hi_part = lo.at[:, :, part], hi.at[:, :, part]
        up_sems = rad_send.at[0, c], rad_recv.at[0, c]
        down_sems = rad_send.at[1, c], rad_recv.at[1, c]
        rad_up.append(remote(above, lo_part, *up_sems, (r + 1, a)))
        rad_down.append(remote(below, hi_part, *down_sems, (r - 1, a)))
        if c < chunks - 1:
            spot = relay.at[c]
            far_up.append(remote(above, spot, up_sems[0], far_recv.at[c], (r + 2, a)))
            far_down.append(remote(below, spot, down_sems[0], far_recv.at[c], (r - 2, a)))
            pass_up.append(remote(spot, lo_part, pass_send.at[c], up_sems[1], (r - 1, a)))
            pass_down.append(remote(spot, hi_part, pass_send.at[c], down_sems[1], (r + 1, a)))
    odd = r % 2 == 1
    even = r % 2 == 0
    n_up_far = jnp.where(odd & (r + 2 < n_rad), (r + 1) // 2, 0)
    n_down_far = jnp.where(even & (r > 0), chunks - r // 2, 0)
    n_up_pass = jnp.where(odd & (r > 1), (r - 1) // 2, 0)
    n_down_pass = jnp.where(even & (r + 2 < n_rad), chunks - 1 - r // 2, 0)

    def start_far(c):
        when(c < n_up_far, far_up[c].start)
        when(c < n_down_far, far_down[c].start)

    def start_chunk(c):
        when((r + 1 < n_rad) & (c >= n_up_far), rad_up[c].start)
        when((r > 0) & (c >= n_down_far), rad_down[c].start)

    def pass_on(c):
        @pl.when(c < n_up_pass)
        def _():
            far_up[c].wait_recv()
            pass_up[c].start()

        @pl.when(c < n_down_pass)
        def _():
            far_down[c].wait_recv()
            pass_down[c].start()

    when(a + 1 < n_ang, ang_up.start)
    when(a > 0, ang_down.start)
    for c in range(chunks - 1):
        start_far(c)
    start_chunk(0)

    @pl.when(a == 0)
    def _():
        ext[:, :, 0:PADR, :] = jnp.zeros((4, shells, PADR, cols), f32)

    @pl.when(a == n_ang - 1)
    def _():
        ext[:, :, PADR + rows : span, :] = jnp.zeros((4, shells, PADR, cols), f32)

    @pl.when(r == 0)
    def _():
        lo[...] = jnp.zeros_like(lo)

    @pl.when(r == n_rad - 1)
    def _():
        hi[...] = jnp.zeros_like(hi)

    for d in range(1, n_rad):

        @pl.when(r - d < 0)
        def _():
            got_up[d] = jnp.zeros((8, LANES), f32)

        @pl.when(r + d >= n_rad)
        def _():
            got_down[d] = jnp.zeros((8, LANES), f32)

    load_rows.wait()
    load_degree.wait()
    cosine = jnp.broadcast_to(rowtab[:, 0:1], (span, LANES))
    sine = jnp.broadcast_to(rowtab[:, 1:2], (span, LANES))
    order = lax.broadcasted_iota(jnp.int32, (span, LANES), 1) % MPAD
    power = jnp.full((span, LANES), 1.0, f32)
    square = sine
    for bit in range(6):
        power = jnp.where((order // (1 << bit)) % 2 == 1, power * square, power)
        square = square * square
    level = power * degree_ref[0:1, :]
    leg[0] = level

    def next_level(k, carry):
        last, before = carry
        alpha = degree_ref[pl.ds(k, 1), :]
        beta = degree_ref[pl.ds(NK + k, 1), :]
        new = alpha * (cosine * last - beta * before)
        leg[k] = new
        return (new, last)

    lax.fori_loop(1, NK, next_level, (level, jnp.zeros_like(level)))

    load_density.wait()
    load_high.wait()
    load_low.wait()
    weight = sine[PADR : PADR + rows] * (step_t * step_p)
    half = shells // 2
    for h in range(2):
        cells = ext[0, h * half : (h + 1) * half, PADR : PADR + rows, :]
        high, low = split(cells.reshape(half * rows, cols))
        sums = dot(high, fwd_high_ref[...]) + (
            dot(low, fwd_high_ref[...]) + dot(high, fwd_low_ref[...])
        )
        for q in range(half):
            spec[pl.ds((h * half + q) * rows, rows), :] = (
                sums[q * rows : (q + 1) * rows] * weight
            )
    spectra = [spec[pl.ds(j, shells, stride=rows), :] for j in range(rows)]

    def moment(k, carry):
        parts = [jnp.zeros((shells, LANES), f32) for _ in range(4)]
        for j in range(rows):
            parts[j % 4] = parts[j % 4] + spectra[j] * leg[k, PADR + j : PADR + j + 1, :]
        partial[k // KD, k % KD] = (parts[0] + parts[1]) + (parts[2] + parts[3])
        return carry

    lax.fori_loop(0, NK, moment, 0)

    def exchange_a(d):
        return remote(
            partial.at[(g + d) % GROUPS], got_a.at[d], a_send.at[d], a_recv.at[d], peer(d)
        )

    for d in range(1, GROUPS):
        exchange_a(d).start()

    load_rest.wait()

    def phi_flux(index, carry):
        i = index // chunks
        at = pl.multiple_of((index % chunks) * ROWS, ROWS)
        cell_radius = inner_radius + step_r * ((r * shells + i).astype(f32) + 0.5)
        sums, jumps = [], []
        for c in range(4):
            u = ext[c, i, pl.ds(PADR + at, ROWS), :]
            left = pltpu.roll(u, 1, 1)
            near = u + left
            mid = pltpu.roll(u, cols - 1, 1) + pltpu.roll(u, 2, 1)
            far = pltpu.roll(u, cols - 2, 1) + pltpu.roll(u, 3, 1)
            sums.append(37.0 * near - 8.0 * mid + far)
            jumps.append(u - left)
        for c, face in enumerate(flux(sums, jumps, 3)):
            tend[c, i, pl.ds(at, ROWS), :] = (face - pltpu.roll(face, cols - 1, 1)) * (
                cell_radius / step_p
            )
        return carry

    lax.fori_loop(0, shells * chunks // 2, phi_flux, 0)

    for d in range(1, GROUPS):
        exchange_a(d).wait_recv()
    total = partial[g]
    for d in range(1, GROUPS):
        total = total + got_a[d]
    mine[...] = total
    exchange_b = remote(mine, got_b, b_send.at[0], b_recv.at[0], partner)
    exchange_b.start()
    start_chunk(1)

    lax.fori_loop(shells * chunks // 2, shells * chunks, phi_flux, 0)

    when(a > 0, ang_up.wait_recv)
    when(a + 1 < n_ang, ang_down.wait_recv)
    tiles = cols // LANES

    def theta_flux(index, carry):
        i = index // tiles
        lanes = pl.ds(pl.multiple_of((index % tiles) * LANES, LANES), LANES)
        cell_radius = inner_radius + step_r * ((r * shells + i).astype(f32) + 0.5)
        area = jnp.broadcast_to(rowtab[:, 2:3], (span, LANES)) * (cell_radius / step_t)
        sums, jumps = [], []
        for c in range(4):
            u = ext[c, i, :, lanes]
            left = pltpu.roll(u, 1, 0)
            near = u + left
            mid = pltpu.roll(u, span - 1, 0) + pltpu.roll(u, 2, 0)
            far = pltpu.roll(u, span - 2, 0) + pltpu.roll(u, 3, 0)
            sums.append(37.0 * near - 8.0 * mid + far)
            jumps.append(u - left)
        for c, face in enumerate(flux(sums, jumps, 2)):
            face = face * area
            change = face - pltpu.roll(face, span - 1, 0)
            tend[c, i, :, lanes] = tend[c, i, :, lanes] + change[PADR : PADR + rows]
        return carry

    lax.fori_loop(0, shells * tiles // 2, theta_flux, 0)

    exchange_b.wait_recv()
    total = mine[...] + got_b[...]
    load_log.wait()
    log_radius = log_ref[...]
    shell = lax.broadcasted_iota(jnp.int32, (shells, LANES), 0)
    radius = inner_radius + step_r * ((r * shells + shell).astype(f32) + 0.5)
    order = lax.broadcasted_iota(jnp.int32, (shells, LANES), 1) % MPAD
    ups, downs, powers, degrees = [], [], [], []
    for q in range(KD):
        degree = (order + (g * KD + q)).astype(f32)
        grow = jnp.exp(degree * log_radius)
        weighted = (radius * radius * step_r) * total[q]
        up = grow * weighted
        down = weighted / (radius * grow)
        for s in (1, 2, 4):
            up = up + jnp.where(shell >= s, pltpu.roll(up, s, 0), 0.0)
            down = down + jnp.where(shell >= s, pltpu.roll(down, s, 0), 0.0)
        tot_up[q : q + 1, :] = up[shells - 1 : shells]
        tot_down[q : q + 1, :] = down[shells - 1 : shells]
        ups.append(up)
        downs.append(down)
        powers.append(grow)
        degrees.append(degree)

    def exchange_up(d):
        return remote(tot_up, got_up.at[d], c_send.at[0, d], c_recv.at[0, d], (r + d, a))

    def exchange_down(d):
        return remote(tot_down, got_down.at[d], c_send.at[1, d], c_recv.at[1, d], (r - d, a))

    for d in range(1, n_rad):
        when(r + d < n_rad, exchange_up(d).start)
        when(r - d >= 0, exchange_down(d).start)
    pass_on(0)
    start_chunk(2)
    pass_on(1)

    lax.fori_loop(shells * tiles // 2, shells * tiles, theta_flux, 0)

    for d in range(1, n_rad):
        when(r - d >= 0, exchange_up(d).wait_recv)
        when(r + d < n_rad, exchange_down(d).wait_recv)
    below = got_up[1]
    above = got_down[1]
    for d in range(2, n_rad):
        below = below + got_up[d]
        above = above + got_down[d]
    inverse_radius = 1.0 / radius
    for q in range(KD):
        inner = below[q : q + 1] + ups[q]
        outer = above[q : q + 1] + (downs[q][shells - 1 : shells] - downs[q])
        degree = degrees[q]
        norm = (-4.0 * math.pi) / (2.0 * degree + 1.0)
        inner_term = inner * inverse_radius / powers[q]
        outer_term = powers[q] * outer
        coef[g, 0, q] = norm * (inner_term + outer_term)
        coef[g, 1, q] = (
            norm * (degree * outer_term - (degree + 1.0) * inner_term) * inverse_radius
        )

    def exchange_d(d):
        return remote(coef.at[g], coef.at[g], d_send.at[d], d_recv.at[d], peer(d))

    for d in range(1, GROUPS):
        exchange_d(d).start()
    pass_on(2)
    start_chunk(3)
    for d in range(1, GROUPS):
        exchange_d(d).wait_recv()

    slope_row = degree_ref[2 * NK : 2 * NK + 1, :]
    theta_scale = 1.0 / (2.0 * step_t)
    for i in range(0, shells, 2):

        def synthesize(h, carry):
            sums = list(carry)
            for q in range(KD):
                k = h * KD + q
                full = leg[k]
                value = full[PADR : PADR + rows]
                change = pltpu.roll(full, span - 1, 0) - pltpu.roll(full, 1, 0)
                change = change[PADR : PADR + rows]
                for p in range(2):
                    cp = coef[h, 0, q, i + p : i + p + 1, :]
                    cs = coef[h, 1, q, i + p : i + p + 1, :]
                    sums[3 * p] = sums[3 * p] + value * cp
                    sums[3 * p + 1] = sums[3 * p + 1] + value * cs
                    sums[3 * p + 2] = sums[3 * p + 2] + change * cp
            return tuple(sums)

        zero = jnp.zeros((rows, LANES), f32)
        sums = lax.fori_loop(0, (LMAX + KD) // KD, synthesize, (zero,) * 6)
        for p in range(2):
            base, slope, change = sums[3 * p : 3 * p + 3]
            at = (i + p) * 4 * rows
            table[at : at + rows, :] = base
            table[at + rows : at + 2 * rows, :] = slope
            table[at + 2 * rows : at + 3 * rows, :] = change * theta_scale
            table[at + 3 * rows : at + 4 * rows, :] = pltpu.roll(base, MPAD, 1) * slope_row

    load_back.wait()

    def sources(i, carry):
        at = pl.multiple_of(i * 4 * rows, 4 * rows)
        high, low = split(table[pl.ds(at, 4 * rows), :])
        fields[...] = dot(jnp.concatenate([high, low, high], axis=1), back_ref[...])
        pot[i] = fields[0:rows, :]
        cell_radius = inner_radius + step_r * ((r * shells + i).astype(f32) + 0.5)
        for c in range(chunks):
            at = c * ROWS
            inside = pl.ds(PADR + at, ROWS)
            sine = jnp.broadcast_to(rowtab[inside, 1:2], (ROWS, cols)) * cell_radius
            cosine = jnp.broadcast_to(rowtab[inside, 0:1], (ROWS, cols)) * cell_radius
            density = ext[0, i, inside, :]
            mom_r = ext[1, i, inside, :]
            mom_t = ext[2, i, inside, :]
            mom_p = ext[3, i, inside, :]
            inverse = 1.0 / density
            vel_t = mom_t * inverse
            vel_p = mom_p * inverse
            pull = grav_const * density
            slope = fields[rows + at : rows + at + ROWS, :]
            grad_t = fields[2 * rows + at : 2 * rows + at + ROWS, :]
            grad_p = fields[3 * rows + at : 3 * rows + at + ROWS, :]
            twist = mom_p * vel_p
            source_r = sine * (
                (mom_t * vel_t + twist)
                + (2.0 * sound_sq) * density
                - (cell_radius * pull) * slope
            )
            source_t = cosine * (twist + sound_sq * density) - sine * (
                mom_r * vel_t + pull * grad_t
            )
            source_p = -(
                vel_p * (mom_r * sine + mom_t * cosine) + (cell_radius * pull) * grad_p
            )
            spot = pl.ds(at, ROWS)
            tend[1, i, spot, :] = tend[1, i, spot, :] + source_r
            tend[2, i, spot, :] = tend[2, i, spot, :] + source_t
            tend[3, i, spot, :] = tend[3, i, spot, :] + source_p
        return carry

    lax.fori_loop(0, shells, sources, 0)

    for chunk in range(chunks):
        when(r > 0, rad_up[chunk].wait_recv)
        when(r + 1 < n_rad, rad_down[chunk].wait_recv)
        at = chunk * ROWS
        spot = pl.ds(at, ROWS)

        def radial_flux(tile, carry):
            lanes = pl.ds(pl.multiple_of(tile * LANES, LANES), LANES)
            sine = jnp.broadcast_to(
                rowtab[PADR + at : PADR + at + ROWS, 1:2], (ROWS, LANES)
            ) * (section_step / step_r)

            def cell(c, s):
                if s < 0:
                    return lo[c, s + WIDTH, spot, lanes]
                if s >= shells:
                    return hi[c, s - shells, spot, lanes]
                return ext[c, s, pl.ds(PADR + at, ROWS), lanes]

            u = [[cell(c, s) for s in range(-WIDTH, shells + WIDTH)] for c in range(4)]
            last = None
            for f in range(shells + 1):
                place = r * shells + f
                face_radius = inner_radius + step_r * place.astype(f32)
                area = jnp.where(
                    (place > 0) & (place < n_rad * shells), face_radius * face_radius, 0.0
                )
                sums, jumps = [], []
                for c in range(4):
                    w = u[c][f : f + 6]
                    sums.append(37.0 * (w[2] + w[3]) - 8.0 * (w[1] + w[4]) + (w[0] + w[5]))
                    jumps.append(w[3] - w[2])
                face = [value * area for value in flux(sums, jumps, 1)]
                if f > 0:
                    for c in range(4):
                        tend[c, f - 1, spot, lanes] = (
                            section_step * tend[c, f - 1, spot, lanes]
                            - (face[c] - last[c]) * sine
                        )
                last = face
            return carry

        lax.fori_loop(0, tiles, radial_flux, 0)

    when(a + 1 < n_ang, ang_up.wait_send)
    when(a > 0, ang_down.wait_send)
    for c in range(chunks):
        when(r + 1 < n_rad, rad_up[c].wait_send)
        when(r > 0, rad_down[c].wait_send)
        if c < chunks - 1:
            when((c < n_up_pass) | (c < n_down_pass), pass_up[c].wait_send)
    for d in range(1, GROUPS):
        exchange_a(d).wait_send()
        exchange_d(d).wait_send()
    exchange_b.wait_send()
    for d in range(1, n_rad):
        when(r + d < n_rad, exchange_up(d).wait_send)
        when(r - d >= 0, exchange_down(d).wait_send)


def solution(mesh):
    n_rad = mesh.shape["rad"]
    n_ang = mesh.shape["ang"]

    def body(state):
        _, shells, rows, cols = state.shape
        high, low, back, slope = phi_tables(cols)
        operands = (
            state,
            jnp.asarray(high),
            jnp.asarray(low),
            jnp.asarray(back),
            jnp.asarray(row_tables(n_ang, rows)),
            jnp.asarray(degree_tables(slope)),
            jnp.asarray(log_radii(n_rad, shells)),
        )
        span = rows + 2 * PADR
        chunks = rows // ROWS
        inside = pl.BlockSpec(memory_space=pltpu.VMEM)
        dma = pltpu.SemaphoreType.DMA
        increment, potential = pl.pallas_call(
            functools.partial(kernel, n_rad, n_ang, shells, rows, cols),
            out_shape=(
                pltpu.VMEM(state.shape, f32),
                pltpu.VMEM(state.shape[1:], f32),
            ),
            in_specs=[pl.BlockSpec(memory_space=pltpu.HBM)] * 7,
            out_specs=(inside, inside),
            scratch_shapes=[
                pltpu.VMEM((4, shells, span, cols), f32),
                pltpu.VMEM((4, WIDTH, rows, cols), f32),
                pltpu.VMEM((4, WIDTH, rows, cols), f32),
                pltpu.VMEM((chunks - 1, 4, WIDTH, ROWS, cols), f32),
                pltpu.VMEM((4 * rows, cols), f32),
                pltpu.VMEM((shells * 4 * rows, LANES), f32),
                pltpu.VMEM((shells * rows, LANES), f32),
                pltpu.VMEM((cols, LANES), bf16),
                pltpu.VMEM((cols, LANES), bf16),
                pltpu.VMEM((3 * LANES, cols), bf16),
                pltpu.VMEM((span, LANES), f32),
                pltpu.VMEM((2 * NK + 8, LANES), f32),
                pltpu.VMEM((shells, LANES), f32),
                pltpu.VMEM((NK, span, LANES), f32),
                pltpu.VMEM((GROUPS, KD, shells, LANES), f32),
                pltpu.VMEM((GROUPS, KD, shells, LANES), f32),
                pltpu.VMEM((KD, shells, LANES), f32),
                pltpu.VMEM((KD, shells, LANES), f32),
                pltpu.VMEM((8, LANES), f32),
                pltpu.VMEM((8, LANES), f32),
                pltpu.VMEM((n_rad, 8, LANES), f32),
                pltpu.VMEM((n_rad, 8, LANES), f32),
                pltpu.VMEM((GROUPS, 2, KD, shells, LANES), f32),
                dma((8,)),
                dma((2,)),
                dma((2,)),
                dma((2, chunks)),
                dma((2, chunks)),
                dma((chunks - 1,)),
                dma((chunks - 1,)),
                dma((GROUPS,)),
                dma((GROUPS,)),
                dma((1,)),
                dma((1,)),
                dma((2, n_rad)),
                dma((2, n_rad)),
                dma((GROUPS,)),
                dma((GROUPS,)),
            ],
            compiler_params=pltpu.CompilerParams(
                collective_id=0, has_side_effects=True, vmem_limit_bytes=61_700_000
            ),
        )(*operands)
        return increment, potential

    return jax.shard_map(
        body,
        mesh=mesh,
        in_specs=(P(None, "rad", "ang", None),),
        out_specs=(P(None, "rad", "ang", None), P("rad", "ang", None)),
        check_vma=False,
    )
```

```python
import functools
import math

import jax
import jax.numpy as jnp
import numpy as np
from jax import lax
from jax.experimental import pallas as pl
from jax.experimental.pallas import tpu as pltpu
from jax.sharding import PartitionSpec as P

LMAX = 48
MPAD = 64
LANES = 128
NK = 56
GROUPS = 8
KD = 7
PADR = 8
WIDTH = 3
ROWS = 8
CUTS = 2

sound_speed = 0.5
sound_sq = 0.25
grav_const = 100.0
section_step = 0.001
inner_radius = 1.0
radial_span = 0.1
MESH = pl.DeviceIdType.MESH
f32 = jnp.float32
bf16 = jnp.bfloat16


def split_np(table):
    high = table.astype(bf16)
    low = (table - high.astype(np.float64)).astype(bf16)
    return high, low


def phi_tables(count):
    order = np.arange(MPAD, dtype=np.float64)
    norm = np.where(order > 0.5, math.sqrt(2.0), 1.0)
    phase = (2.0 * math.pi / count) * (np.outer(np.arange(count), np.arange(MPAD)) % count)
    table = np.concatenate([np.cos(phase) * norm, np.sin(phase) * norm], axis=1)
    high, low = split_np(table)
    back = np.concatenate([high.T, high.T, low.T], axis=0)
    step = 2.0 * math.pi / count
    slope = np.sin(order * step) / step
    return high, low, back, np.concatenate([slope, -slope])


def row_tables(blocks, rows):
    total = blocks * rows
    step_t = math.pi / total
    row = np.arange(blocks)[:, None] * rows + np.arange(rows + 2 * PADR)[None, :] - PADR
    theta = step_t * (row + 0.5)
    face = np.where((row > 0) & (row < total), np.sin(step_t * row), 0.0)
    table = np.zeros((blocks, rows + 2 * PADR, LANES))
    table[:, :, 0] = np.cos(theta)
    table[:, :, 1] = np.sin(theta)
    table[:, :, 2] = face
    return table.astype(np.float32)


def degree_tables(slope):
    m = np.arange(LANES) % MPAD
    k = np.arange(NK)[:, None]
    l = (m + k).astype(np.float64)
    alpha = np.zeros((NK, LANES))
    beta = np.zeros((NK, LANES))
    norm = np.full(LANES, 1.0 / math.sqrt(4.0 * math.pi))
    for q in range(1, MPAD):
        norm = np.where(m >= q, norm * math.sqrt((2.0 * q + 1.0) / (2.0 * q)), norm)
    alpha[0] = norm
    alpha[1:] = np.sqrt((4.0 * l[1:] ** 2 - 1.0) / (l[1:] ** 2 - m**2))
    beta[2:] = np.sqrt(((l[2:] - 1.0) ** 2 - m**2) / (4.0 * (l[2:] - 1.0) ** 2 - 1.0))
    alpha = np.where(l <= LMAX, alpha, 0.0)
    extra = np.zeros((8, LANES))
    extra[0] = slope
    return np.concatenate([alpha, beta, extra]).astype(np.float32)


def log_radii(blocks, shells):
    radius = inner_radius + radial_span / (blocks * shells) * (np.arange(blocks * shells) + 0.5)
    table = np.log(radius).reshape(blocks, shells, 1)
    return np.broadcast_to(table, (blocks, shells, LANES)).astype(np.float32)


def split(value):
    high = value.astype(bf16)
    return high, (value - high.astype(f32)).astype(bf16)


def dot(a, b):
    return jnp.dot(a, b, preferred_element_type=f32)


def flux(sums, jumps, component):
    inverse = 1.0 / sums[0]
    speed = sums[component] * inverse
    scaled = speed * (1.0 / 60.0)
    wave = 0.5 * (sound_speed + jnp.abs(speed))
    out = [s * scaled - wave * j for s, j in zip(sums, jumps)]
    out[component] = out[component] + (sound_sq / 60.0) * sums[0]
    return out


def kernel(
    n_rad,
    n_ang,
    shells,
    rows,
    cols,
    x_ref,
    fwd_high_hbm,
    fwd_low_hbm,
    back_hbm,
    row_hbm,
    degree_hbm,
    log_hbm,
    tend,
    pot,
    ext,
    lo,
    hi,
    relay,
    fields,
    table,
    spec,
    fwd_high_ref,
    fwd_low_ref,
    back_ref,
    rowtab,
    degree_ref,
    log_ref,
    leg,
    partial,
    got_a,
    mine,
    got_b,
    totals,
    got_pair,
    chain_up,
    chain_down,
    coef,
    local_sem,
    ang_send,
    ang_recv,
    rad_send,
    rad_recv,
    far_recv,
    pass_send,
    a_send,
    a_recv,
    b_send,
    b_recv,
    c_send,
    c_recv,
    d_send,
    d_recv,
):
    r = lax.axis_index("rad")
    a = lax.axis_index("ang")
    y, x_hi, core = a // 4, (a // 2) % 2, a % 2
    g = y * 2 + core
    chunks = rows // ROWS
    parts = chunks * CUTS
    wide = cols // CUTS
    n_far = parts - CUTS
    span = rows + 2 * PADR
    own = pl.ds(PADR, rows)
    step_r = radial_span / (n_rad * shells)
    step_t = math.pi / (n_ang * rows)
    step_p = 2.0 * math.pi / cols

    def peer(d):
        q = (g + d) % GROUPS
        return (r, (q // 2) * 4 + x_hi * 2 + q % 2)

    partner = (r, y * 4 + (1 - x_hi) * 2 + core)

    def when(cond, run):
        @pl.when(cond)
        def _():
            run()

    def remote(src, dst, send, recv, dev):
        return pltpu.make_async_remote_copy(
            src_ref=src,
            dst_ref=dst,
            send_sem=send,
            recv_sem=recv,
            device_id=dev,
            device_id_type=MESH,
        )

    load_density = pltpu.make_async_copy(x_ref.at[0], ext.at[0, :, own], local_sem.at[0])
    load_rest = pltpu.make_async_copy(
        x_ref.at[1:4], ext.at[1:4, :, own], local_sem.at[1]
    )
    load_rows = pltpu.make_async_copy(row_hbm.at[a], rowtab, local_sem.at[2])
    load_degree = pltpu.make_async_copy(degree_hbm, degree_ref, local_sem.at[3])
    load_high = pltpu.make_async_copy(fwd_high_hbm, fwd_high_ref, local_sem.at[4])
    load_low = pltpu.make_async_copy(fwd_low_hbm, fwd_low_ref, local_sem.at[5])
    load_log = pltpu.make_async_copy(log_hbm.at[r], log_ref, local_sem.at[6])
    load_back = pltpu.make_async_copy(back_hbm, back_ref, local_sem.at[7])
    barrier = pltpu.get_barrier_semaphore()

    def greet(cond, dev):
        when(
            cond,
            lambda: pl.semaphore_signal(barrier, inc=1, device_id=dev, device_id_type=MESH),
        )

    ends = jnp.where(a > 0, 1, 0) + jnp.where(a + 1 < n_ang, 1, 0)
    for d in (1, 2):
        greet(r + d < n_rad, (r + d, a))
        greet(r - d >= 0, (r - d, a))
        ends = ends + jnp.where(r + d < n_rad, 1, 0) + jnp.where(r - d >= 0, 1, 0)
    for d in range(1, GROUPS):
        pl.semaphore_signal(barrier, inc=1, device_id=peer(d), device_id_type=MESH)
    pl.semaphore_signal(barrier, inc=1, device_id=partner, device_id_type=MESH)
    greet(a + 1 < n_ang, (r, a + 1))
    greet(a > 0, (r, a - 1))

    for load in (load_rows, load_degree, load_density, load_high, load_low):
        load.start()
    for load in (load_rest, load_log, load_back):
        load.start()
    pl.semaphore_wait(barrier, GROUPS + ends)

    ang_up = remote(
        x_ref.at[:, :, rows - WIDTH : rows],
        ext.at[:, :, PADR - WIDTH : PADR],
        ang_send.at[0],
        ang_recv.at[0],
        (r, a + 1),
    )
    ang_down = remote(
        x_ref.at[:, :, 0:WIDTH],
        ext.at[:, :, PADR + rows : PADR + rows + WIDTH],
        ang_send.at[1],
        ang_recv.at[1],
        (r, a - 1),
    )
    rad_up, rad_down, far_up, far_down, pass_up, pass_down = [], [], [], [], [], []
    for c in range(parts):
        part = pl.ds((c // CUTS) * ROWS, ROWS)
        band = pl.ds((c % CUTS) * wide, wide)
        above = x_ref.at[:, shells - WIDTH : shells, part, band]
        below = x_ref.at[:, 0:WIDTH, part, band]
        lo_part, hi_part = lo.at[:, :, part, band], hi.at[:, :, part, band]
        up_sems = rad_send.at[0, c], rad_recv.at[0, c]
        down_sems = rad_send.at[1, c], rad_recv.at[1, c]
        rad_up.append(remote(above, lo_part, *up_sems, (r + 1, a)))
        rad_down.append(remote(below, hi_part, *down_sems, (r - 1, a)))
        if c < n_far:
            spot = relay.at[c]
            far_up.append(remote(above, spot, up_sems[0], far_recv.at[c], (r + 2, a)))
            far_down.append(remote(below, spot, down_sems[0], far_recv.at[c], (r - 2, a)))
            pass_up.append(remote(spot, lo_part, pass_send.at[c], up_sems[1], (r - 1, a)))
            pass_down.append(remote(spot, hi_part, pass_send.at[c], down_sems[1], (r + 1, a)))
    odd = r % 2 == 1
    even = r % 2 == 0
    n_up_far = jnp.where(odd & (r + 2 < n_rad), CUTS * ((r + 1) // 2), 0)
    n_down_far = jnp.where(even & (r > 0), parts - CUTS * (r // 2), 0)
    n_up_pass = jnp.where(odd & (r > 1), CUTS * ((r - 1) // 2), 0)
    n_down_pass = jnp.where(even & (r + 2 < n_rad), n_far - CUTS * (r // 2), 0)

    def start_far(c):
        when(c < n_up_far, far_up[c].start)
        when(c < n_down_far, far_down[c].start)

    def start_chunk(c):
        when((r + 1 < n_rad) & (c >= n_up_far), rad_up[c].start)
        when((r > 0) & (c >= n_down_far), rad_down[c].start)

    def pass_on(c):
        @pl.when(c < n_up_pass)
        def _():
            far_up[c].wait_recv()
            pass_up[c].start()

        @pl.when(c < n_down_pass)
        def _():
            far_down[c].wait_recv()
            pass_down[c].start()

    when(a + 1 < n_ang, ang_up.start)
    when(a > 0, ang_down.start)
    for c in range(n_far):
        start_far(c)
    for c in range(CUTS):
        start_chunk(c)

    @pl.when(a == 0)
    def _():
        ext[:, :, 0:PADR, :] = jnp.zeros((4, shells, PADR, cols), f32)

    @pl.when(a == n_ang - 1)
    def _():
        ext[:, :, PADR + rows : span, :] = jnp.zeros((4, shells, PADR, cols), f32)

    @pl.when(r == 0)
    def _():
        lo[...] = jnp.zeros_like(lo)

    @pl.when(r == n_rad - 1)
    def _():
        hi[...] = jnp.zeros_like(hi)

    @pl.when(r < 2)
    def _():
        chain_up[1:] = jnp.zeros((n_rad // 2 - 1, 8, LANES), f32)

    @pl.when(r + 2 >= n_rad)
    def _():
        chain_down[1:] = jnp.zeros((n_rad // 2 - 1, 8, LANES), f32)

    load_rows.wait()
    load_degree.wait()
    cosine = jnp.broadcast_to(rowtab[:, 0:1], (span, LANES))
    sine = jnp.broadcast_to(rowtab[:, 1:2], (span, LANES))
    order = lax.broadcasted_iota(jnp.int32, (span, LANES), 1) % MPAD
    power = jnp.full((span, LANES), 1.0, f32)
    square = sine
    for bit in range(6):
        power = jnp.where((order // (1 << bit)) % 2 == 1, power * square, power)
        square = square * square
    level = power * degree_ref[0:1, :]
    leg[0] = level

    def next_level(k, carry):
        last, before = carry
        alpha = degree_ref[pl.ds(k, 1), :]
        beta = degree_ref[pl.ds(NK + k, 1), :]
        new = alpha * (cosine * last - beta * before)
        leg[k] = new
        return (new, last)

    lax.fori_loop(1, NK, next_level, (level, jnp.zeros_like(level)))

    load_density.wait()
    load_high.wait()
    load_low.wait()
    weight = sine[PADR : PADR + rows] * (step_t * step_p)
    half = shells // 2
    for h in range(2):
        cells = ext[0, h * half : (h + 1) * half, PADR : PADR + rows, :]
        high, low = split(cells.reshape(half * rows, cols))
        sums = dot(high, fwd_high_ref[...]) + (
            dot(low, fwd_high_ref[...]) + dot(high, fwd_low_ref[...])
        )
        for q in range(half):
            spec[pl.ds((h * half + q) * rows, rows), :] = (
                sums[q * rows : (q + 1) * rows] * weight
            )
    spectra = [spec[pl.ds(j, shells, stride=rows), :] for j in range(rows)]

    def moment(k, carry):
        parts = [jnp.zeros((shells, LANES), f32) for _ in range(4)]
        for j in range(rows):
            parts[j % 4] = parts[j % 4] + spectra[j] * leg[k, PADR + j : PADR + j + 1, :]
        partial[k // KD, k % KD] = (parts[0] + parts[1]) + (parts[2] + parts[3])
        return carry

    lax.fori_loop(0, NK, moment, 0)

    def exchange_a(d):
        return remote(
            partial.at[(g + d) % GROUPS], got_a.at[d], a_send.at[d], a_recv.at[d], peer(d)
        )

    for d in range(1, GROUPS):
        exchange_a(d).start()

    load_rest.wait()

    def phi_flux(index, carry):
        i = index // chunks
        at = pl.multiple_of((index % chunks) * ROWS, ROWS)
        cell_radius = inner_radius + step_r * ((r * shells + i).astype(f32) + 0.5)
        sums, jumps = [], []
        for c in range(4):
            u = ext[c, i, pl.ds(PADR + at, ROWS), :]
            left = pltpu.roll(u, 1, 1)
            near = u + left
            mid = pltpu.roll(u, cols - 1, 1) + pltpu.roll(u, 2, 1)
            far = pltpu.roll(u, cols - 2, 1) + pltpu.roll(u, 3, 1)
            sums.append(37.0 * near - 8.0 * mid + far)
            jumps.append(u - left)
        for c, face in enumerate(flux(sums, jumps, 3)):
            tend[c, i, pl.ds(at, ROWS), :] = (face - pltpu.roll(face, cols - 1, 1)) * (
                cell_radius / step_p
            )
        return carry

    lax.fori_loop(0, shells * chunks // 2, phi_flux, 0)

    for d in range(1, GROUPS):
        exchange_a(d).wait_recv()
    total = partial[g]
    for d in range(1, GROUPS):
        total = total + got_a[d]
    mine[...] = total
    exchange_b = remote(mine, got_b, b_send.at[0], b_recv.at[0], partner)
    exchange_b.start()
    for c in range(CUTS, 2 * CUTS):
        start_chunk(c)

    lax.fori_loop(shells * chunks // 2, shells * chunks, phi_flux, 0)

    when(a > 0, ang_up.wait_recv)
    when(a + 1 < n_ang, ang_down.wait_recv)
    tiles = cols // LANES

    def theta_flux(index, carry):
        i = index // tiles
        lanes = pl.ds(pl.multiple_of((index % tiles) * LANES, LANES), LANES)
        cell_radius = inner_radius + step_r * ((r * shells + i).astype(f32) + 0.5)
        area = jnp.broadcast_to(rowtab[:, 2:3], (span, LANES)) * (cell_radius / step_t)
        sums, jumps = [], []
        for c in range(4):
            u = ext[c, i, :, lanes]
            left = pltpu.roll(u, 1, 0)
            near = u + left
            mid = pltpu.roll(u, span - 1, 0) + pltpu.roll(u, 2, 0)
            far = pltpu.roll(u, span - 2, 0) + pltpu.roll(u, 3, 0)
            sums.append(37.0 * near - 8.0 * mid + far)
            jumps.append(u - left)
        for c, face in enumerate(flux(sums, jumps, 2)):
            face = face * area
            change = face - pltpu.roll(face, span - 1, 0)
            tend[c, i, :, lanes] = tend[c, i, :, lanes] + change[PADR : PADR + rows]
        return carry

    lax.fori_loop(0, shells * tiles // 4, theta_flux, 0)

    exchange_b.wait_recv()
    total = mine[...] + got_b[...]
    load_log.wait()
    log_radius = log_ref[...]
    shell = lax.broadcasted_iota(jnp.int32, (shells, LANES), 0)
    radius = inner_radius + step_r * ((r * shells + shell).astype(f32) + 0.5)
    order = lax.broadcasted_iota(jnp.int32, (shells, LANES), 1) % MPAD
    ups, downs, powers, degrees = [], [], [], []
    for q in range(KD):
        degree = (order + (g * KD + q)).astype(f32)
        grow = jnp.exp(degree * log_radius)
        weighted = (radius * radius * step_r) * total[q]
        up = grow * weighted
        down = weighted / (radius * grow)
        for s in (1, 2, 4):
            up = up + jnp.where(shell >= s, pltpu.roll(up, s, 0), 0.0)
            down = down + jnp.where(shell >= s, pltpu.roll(down, s, 0), 0.0)
        totals[0, q : q + 1, :] = up[shells - 1 : shells]
        totals[1, q : q + 1, :] = down[shells - 1 : shells]
        ups.append(up)
        downs.append(down)
        powers.append(grow)
        degrees.append(degree)

    pair = remote(totals, got_pair, c_send.at[0, 0], c_recv.at[0, 0], (r + 1 - 2 * (r % 2), a))
    pair.start()

    def hop_up(d):
        return remote(
            chain_up.at[d - 1], chain_up.at[d], c_send.at[0, d], c_recv.at[0, d], (r + 2, a)
        )

    def hop_down(d):
        return remote(
            chain_down.at[d - 1], chain_down.at[d], c_send.at[1, d], c_recv.at[1, d], (r - 2, a)
        )

    def start_hop(d):
        when(r + 2 < n_rad, hop_up(d).start)
        when(r - 2 >= 0, hop_down(d).start)

    def end_hop(d):
        when(r - 2 >= 0, hop_up(d).wait_recv)
        when(r + 2 < n_rad, hop_down(d).wait_recv)

    for c in range(2 * CUTS, 3 * CUTS):
        pass_on(c - 2 * CUTS)
        start_chunk(c)
    for c in range(CUTS, 2 * CUTS):
        pass_on(c)

    quarter = shells * tiles // 4
    lax.fori_loop(quarter, 2 * quarter, theta_flux, 0)
    pair.wait_recv()
    pair_up = got_pair[0]
    pair_down = got_pair[1]
    chain_up[0] = totals[0] + pair_up
    chain_down[0] = totals[1] + pair_down
    start_hop(1)
    lax.fori_loop(2 * quarter, 3 * quarter, theta_flux, 0)
    end_hop(1)
    start_hop(2)
    lax.fori_loop(3 * quarter, 4 * quarter, theta_flux, 0)
    end_hop(2)
    start_hop(3)
    below = jnp.where(odd, pair_up, 0.0)
    above = jnp.where(even, pair_down, 0.0)
    end_hop(3)
    for d in range(1, n_rad // 2):
        below = below + chain_up[d]
        above = above + chain_down[d]
    inverse_radius = 1.0 / radius
    for q in range(KD):
        inner = below[q : q + 1] + ups[q]
        outer = above[q : q + 1] + (downs[q][shells - 1 : shells] - downs[q])
        degree = degrees[q]
        norm = (-4.0 * math.pi) / (2.0 * degree + 1.0)
        inner_term = inner * inverse_radius / powers[q]
        outer_term = powers[q] * outer
        coef[g, 0, q] = norm * (inner_term + outer_term)
        coef[g, 1, q] = (
            norm * (degree * outer_term - (degree + 1.0) * inner_term) * inverse_radius
        )

    def exchange_d(d):
        return remote(coef.at[g], coef.at[g], d_send.at[d], d_recv.at[d], peer(d))

    for d in range(1, GROUPS):
        exchange_d(d).start()
    for c in range(2 * CUTS, 3 * CUTS):
        pass_on(c)
        start_chunk(c + CUTS)
    for d in range(1, GROUPS):
        exchange_d(d).wait_recv()

    slope_row = degree_ref[2 * NK : 2 * NK + 1, :]
    theta_scale = 1.0 / (2.0 * step_t)
    for i in range(0, shells, 2):

        def synthesize(h, carry):
            sums = list(carry)
            for q in range(KD):
                k = h * KD + q
                full = leg[k]
                value = full[PADR : PADR + rows]
                change = pltpu.roll(full, span - 1, 0) - pltpu.roll(full, 1, 0)
                change = change[PADR : PADR + rows]
                for p in range(2):
                    cp = coef[h, 0, q, i + p : i + p + 1, :]
                    cs = coef[h, 1, q, i + p : i + p + 1, :]
                    sums[3 * p] = sums[3 * p] + value * cp
                    sums[3 * p + 1] = sums[3 * p + 1] + value * cs
                    sums[3 * p + 2] = sums[3 * p + 2] + change * cp
            return tuple(sums)

        zero = jnp.zeros((rows, LANES), f32)
        sums = lax.fori_loop(0, (LMAX + KD) // KD, synthesize, (zero,) * 6)
        for p in range(2):
            base, slope, change = sums[3 * p : 3 * p + 3]
            at = (i + p) * 4 * rows
            table[at : at + rows, :] = base
            table[at + rows : at + 2 * rows, :] = slope
            table[at + 2 * rows : at + 3 * rows, :] = change * theta_scale
            table[at + 3 * rows : at + 4 * rows, :] = pltpu.roll(base, MPAD, 1) * slope_row

    load_back.wait()

    def sources(i, carry):
        at = pl.multiple_of(i * 4 * rows, 4 * rows)
        high, low = split(table[pl.ds(at, 4 * rows), :])
        fields[...] = dot(jnp.concatenate([high, low, high], axis=1), back_ref[...])
        pot[i] = fields[0:rows, :]
        cell_radius = inner_radius + step_r * ((r * shells + i).astype(f32) + 0.5)
        for c in range(chunks):
            at = c * ROWS
            inside = pl.ds(PADR + at, ROWS)
            sine = jnp.broadcast_to(rowtab[inside, 1:2], (ROWS, cols)) * cell_radius
            cosine = jnp.broadcast_to(rowtab[inside, 0:1], (ROWS, cols)) * cell_radius
            density = ext[0, i, inside, :]
            mom_r = ext[1, i, inside, :]
            mom_t = ext[2, i, inside, :]
            mom_p = ext[3, i, inside, :]
            inverse = 1.0 / density
            vel_t = mom_t * inverse
            vel_p = mom_p * inverse
            pull = grav_const * density
            slope = fields[rows + at : rows + at + ROWS, :]
            grad_t = fields[2 * rows + at : 2 * rows + at + ROWS, :]
            grad_p = fields[3 * rows + at : 3 * rows + at + ROWS, :]
            twist = mom_p * vel_p
            source_r = sine * (
                (mom_t * vel_t + twist)
                + (2.0 * sound_sq) * density
                - (cell_radius * pull) * slope
            )
            source_t = cosine * (twist + sound_sq * density) - sine * (
                mom_r * vel_t + pull * grad_t
            )
            source_p = -(
                vel_p * (mom_r * sine + mom_t * cosine) + (cell_radius * pull) * grad_p
            )
            spot = pl.ds(at, ROWS)
            tend[1, i, spot, :] = tend[1, i, spot, :] + source_r
            tend[2, i, spot, :] = tend[2, i, spot, :] + source_t
            tend[3, i, spot, :] = tend[3, i, spot, :] + source_p
        return carry

    lax.fori_loop(0, shells, sources, 0)

    per = wide // LANES
    for chunk in range(parts):
        when(r > 0, rad_up[chunk].wait_recv)
        when(r + 1 < n_rad, rad_down[chunk].wait_recv)
        at = (chunk // CUTS) * ROWS
        spot = pl.ds(at, ROWS)
        first = (chunk % CUTS) * per

        def radial_flux(tile, carry):
            lanes = pl.ds(pl.multiple_of(tile * LANES, LANES), LANES)
            sine = jnp.broadcast_to(
                rowtab[PADR + at : PADR + at + ROWS, 1:2], (ROWS, LANES)
            ) * (section_step / step_r)

            def cell(c, s):
                if s < 0:
                    return lo[c, s + WIDTH, spot, lanes]
                if s >= shells:
                    return hi[c, s - shells, spot, lanes]
                return ext[c, s, pl.ds(PADR + at, ROWS), lanes]

            u = [[cell(c, s) for s in range(-WIDTH, shells + WIDTH)] for c in range(4)]
            last = None
            for f in range(shells + 1):
                place = r * shells + f
                face_radius = inner_radius + step_r * place.astype(f32)
                area = jnp.where(
                    (place > 0) & (place < n_rad * shells), face_radius * face_radius, 0.0
                )
                sums, jumps = [], []
                for c in range(4):
                    w = u[c][f : f + 6]
                    sums.append(37.0 * (w[2] + w[3]) - 8.0 * (w[1] + w[4]) + (w[0] + w[5]))
                    jumps.append(w[3] - w[2])
                face = [value * area for value in flux(sums, jumps, 1)]
                if f > 0:
                    for c in range(4):
                        tend[c, f - 1, spot, lanes] = (
                            section_step * tend[c, f - 1, spot, lanes]
                            - (face[c] - last[c]) * sine
                        )
                last = face
            return carry

        lax.fori_loop(first, first + per, radial_flux, 0)

    when(a + 1 < n_ang, ang_up.wait_send)
    when(a > 0, ang_down.wait_send)
    for c in range(parts):
        when(r + 1 < n_rad, rad_up[c].wait_send)
        when(r > 0, rad_down[c].wait_send)
        if c < n_far:
            when((c < n_up_pass) | (c < n_down_pass), pass_up[c].wait_send)
    for d in range(1, GROUPS):
        exchange_a(d).wait_send()
        exchange_d(d).wait_send()
    exchange_b.wait_send()
    pair.wait_send()
    for d in range(1, n_rad // 2):
        when(r + 2 < n_rad, hop_up(d).wait_send)
        when(r - 2 >= 0, hop_down(d).wait_send)


def store(tend, pot, inc_ref, pot_ref, sem):
    copies = [
        pltpu.make_async_copy(tend.at[c], inc_ref.at[c], sem.at[c]) for c in range(tend.shape[0])
    ]
    copies.append(pltpu.make_async_copy(pot, pot_ref, sem.at[len(copies)]))
    for copy in copies:
        copy.start()
    for copy in copies:
        copy.wait()


def solution(mesh):
    n_rad = mesh.shape["rad"]
    n_ang = mesh.shape["ang"]

    def body(state):
        _, shells, rows, cols = state.shape
        high, low, back, slope = phi_tables(cols)
        operands = (
            state,
            jnp.asarray(high),
            jnp.asarray(low),
            jnp.asarray(back),
            jnp.asarray(row_tables(n_ang, rows)),
            jnp.asarray(degree_tables(slope)),
            jnp.asarray(log_radii(n_rad, shells)),
        )
        span = rows + 2 * PADR
        parts = (rows // ROWS) * CUTS
        inside = pl.BlockSpec(memory_space=pltpu.VMEM)
        dma = pltpu.SemaphoreType.DMA
        increment, potential = pl.pallas_call(
            functools.partial(kernel, n_rad, n_ang, shells, rows, cols),
            out_shape=(
                pltpu.VMEM(state.shape, f32),
                pltpu.VMEM(state.shape[1:], f32),
            ),
            in_specs=[pl.BlockSpec(memory_space=pltpu.HBM)] * 7,
            out_specs=(inside, inside),
            scratch_shapes=[
                pltpu.VMEM((4, shells, span, cols), f32),
                pltpu.VMEM((4, WIDTH, rows, cols), f32),
                pltpu.VMEM((4, WIDTH, rows, cols), f32),
                pltpu.VMEM((parts - CUTS, 4, WIDTH, ROWS, cols // CUTS), f32),
                pltpu.VMEM((4 * rows, cols), f32),
                pltpu.VMEM((shells * 4 * rows, LANES), f32),
                pltpu.VMEM((shells * rows, LANES), f32),
                pltpu.VMEM((cols, LANES), bf16),
                pltpu.VMEM((cols, LANES), bf16),
                pltpu.VMEM((3 * LANES, cols), bf16),
                pltpu.VMEM((span, LANES), f32),
                pltpu.VMEM((2 * NK + 8, LANES), f32),
                pltpu.VMEM((shells, LANES), f32),
                pltpu.VMEM((NK, span, LANES), f32),
                pltpu.VMEM((GROUPS, KD, shells, LANES), f32),
                pltpu.VMEM((GROUPS, KD, shells, LANES), f32),
                pltpu.VMEM((KD, shells, LANES), f32),
                pltpu.VMEM((KD, shells, LANES), f32),
                pltpu.VMEM((2, 8, LANES), f32),
                pltpu.VMEM((2, 8, LANES), f32),
                pltpu.VMEM((n_rad // 2, 8, LANES), f32),
                pltpu.VMEM((n_rad // 2, 8, LANES), f32),
                pltpu.VMEM((GROUPS, 2, KD, shells, LANES), f32),
                dma((8,)),
                dma((2,)),
                dma((2,)),
                dma((2, parts)),
                dma((2, parts)),
                dma((parts - CUTS,)),
                dma((parts - CUTS,)),
                dma((GROUPS,)),
                dma((GROUPS,)),
                dma((1,)),
                dma((1,)),
                dma((2, n_rad // 2)),
                dma((2, n_rad // 2)),
                dma((GROUPS,)),
                dma((GROUPS,)),
            ],
            compiler_params=pltpu.CompilerParams(
                collective_id=0, has_side_effects=True, vmem_limit_bytes=61_700_000
            ),
        )(*operands)
        outside = pl.BlockSpec(memory_space=pltpu.HBM)
        return pl.pallas_call(
            store,
            out_shape=(
                jax.ShapeDtypeStruct(state.shape, f32),
                jax.ShapeDtypeStruct(state.shape[1:], f32),
            ),
            in_specs=(inside, inside),
            out_specs=(outside, outside),
            scratch_shapes=[dma((5,))],
            compiler_params=pltpu.CompilerParams(vmem_limit_bytes=1 << 20),
        )(increment, potential)

    return jax.shard_map(
        body,
        mesh=mesh,
        in_specs=(P(None, "rad", "ang", None),),
        out_specs=(P(None, "rad", "ang", None), P("rad", "ang", None)),
        check_vma=False,
    )
```

```python
import functools
import math

import jax
import jax.numpy as jnp
import numpy as np
from jax import lax
from jax.experimental import pallas as pl
from jax.experimental.pallas import tpu as pltpu
from jax.sharding import PartitionSpec as P

LMAX = 48
MPAD = 64
LANES = 128
NK = 56
GROUPS = 8
KD = 7
PADR = 8
WIDTH = 3
ROWS = 8
QUARTERS = 4
CUTS = 2

sound_speed = 0.5
sound_sq = 0.25
grav_const = 100.0
section_step = 0.001
inner_radius = 1.0
radial_span = 0.1
MESH = pl.DeviceIdType.MESH
f32 = jnp.float32
bf16 = jnp.bfloat16


def split_np(table):
    high = table.astype(bf16)
    low = (table - high.astype(np.float64)).astype(bf16)
    return high, low


def phi_tables(count):
    order = np.arange(MPAD, dtype=np.float64)
    norm = np.where(order > 0.5, math.sqrt(2.0), 1.0)
    phase = (2.0 * math.pi / count) * (np.outer(np.arange(count), np.arange(MPAD)) % count)
    table = np.concatenate([np.cos(phase) * norm, np.sin(phase) * norm], axis=1)
    high, low = split_np(table)
    back = np.concatenate([high.T, high.T, low.T], axis=0)
    step = 2.0 * math.pi / count
    slope = np.sin(order * step) / step
    return high, low, back, np.concatenate([slope, -slope])


def row_tables(blocks, rows):
    total = blocks * rows
    step_t = math.pi / total
    row = np.arange(blocks)[:, None] * rows + np.arange(rows + 2 * PADR)[None, :] - PADR
    theta = step_t * (row + 0.5)
    face = np.where((row > 0) & (row < total), np.sin(step_t * row), 0.0)
    table = np.zeros((blocks, rows + 2 * PADR, LANES))
    table[:, :, 0] = np.cos(theta)
    table[:, :, 1] = np.sin(theta)
    table[:, :, 2] = face
    return table.astype(np.float32)


def degree_tables(slope):
    m = np.arange(LANES) % MPAD
    k = np.arange(NK)[:, None]
    l = (m + k).astype(np.float64)
    alpha = np.zeros((NK, LANES))
    beta = np.zeros((NK, LANES))
    norm = np.full(LANES, 1.0 / math.sqrt(4.0 * math.pi))
    for q in range(1, MPAD):
        norm = np.where(m >= q, norm * math.sqrt((2.0 * q + 1.0) / (2.0 * q)), norm)
    alpha[0] = norm
    alpha[1:] = np.sqrt((4.0 * l[1:] ** 2 - 1.0) / (l[1:] ** 2 - m**2))
    beta[2:] = np.sqrt(((l[2:] - 1.0) ** 2 - m**2) / (4.0 * (l[2:] - 1.0) ** 2 - 1.0))
    alpha = np.where(l <= LMAX, alpha, 0.0)
    extra = np.zeros((8, LANES))
    extra[0] = slope
    return np.concatenate([alpha, beta, extra]).astype(np.float32)


def log_radii(blocks, shells):
    radius = inner_radius + radial_span / (blocks * shells) * (np.arange(blocks * shells) + 0.5)
    table = np.log(radius).reshape(blocks, shells, 1)
    return np.broadcast_to(table, (blocks, shells, LANES)).astype(np.float32)


def split(value):
    high = value.astype(bf16)
    return high, (value - high.astype(f32)).astype(bf16)


def dot(a, b):
    return jnp.dot(a, b, preferred_element_type=f32)


def flux(sums, jumps, component):
    inverse = 1.0 / sums[0]
    speed = sums[component] * inverse
    scaled = speed * (1.0 / 60.0)
    wave = 0.5 * (sound_speed + jnp.abs(speed))
    out = [s * scaled - wave * j for s, j in zip(sums, jumps)]
    out[component] = out[component] + (sound_sq / 60.0) * sums[0]
    return out


def kernel(
    n_rad,
    n_ang,
    shells,
    rows,
    cols,
    x_ref,
    fwd_high_hbm,
    fwd_low_hbm,
    back_hbm,
    row_hbm,
    degree_hbm,
    log_hbm,
    tend,
    pot,
    ext,
    lo,
    hi,
    relay,
    row_relay,
    fields,
    table,
    spec,
    fwd_high_ref,
    fwd_low_ref,
    back_ref,
    rowtab,
    degree_ref,
    log_ref,
    leg,
    partial,
    got_a,
    mine,
    got_b,
    totals,
    got_pair,
    chain_up,
    chain_down,
    coef,
    local_sem,
    ang_send,
    ang_recv,
    skip_recv,
    hand_send,
    rad_send,
    rad_recv,
    far_recv,
    pass_send,
    a_send,
    a_recv,
    b_send,
    b_recv,
    c_send,
    c_recv,
    d_send,
    d_recv,
):
    r = lax.axis_index("rad")
    a = lax.axis_index("ang")
    y, x_hi, core = a // 4, (a // 2) % 2, a % 2
    g = y * 2 + core
    chunks = rows // ROWS
    parts = chunks * CUTS
    wide = cols // CUTS
    n_far = parts - CUTS
    span = rows + 2 * PADR
    own = pl.ds(PADR, rows)
    step_r = radial_span / (n_rad * shells)
    step_t = math.pi / (n_ang * rows)
    step_p = 2.0 * math.pi / cols

    def peer(d):
        q = (g + d) % GROUPS
        return (r, (q // 2) * 4 + x_hi * 2 + q % 2)

    partner = (r, y * 4 + (1 - x_hi) * 2 + core)

    def when(cond, run):
        @pl.when(cond)
        def _():
            run()

    def remote(src, dst, send, recv, dev):
        return pltpu.make_async_remote_copy(
            src_ref=src,
            dst_ref=dst,
            send_sem=send,
            recv_sem=recv,
            device_id=dev,
            device_id_type=MESH,
        )

    load_density = pltpu.make_async_copy(x_ref.at[0], ext.at[0, :, own], local_sem.at[0])
    load_rest = pltpu.make_async_copy(
        x_ref.at[1:4], ext.at[1:4, :, own], local_sem.at[1]
    )
    load_rows = pltpu.make_async_copy(row_hbm.at[a], rowtab, local_sem.at[2])
    load_degree = pltpu.make_async_copy(degree_hbm, degree_ref, local_sem.at[3])
    load_high = pltpu.make_async_copy(fwd_high_hbm, fwd_high_ref, local_sem.at[4])
    load_low = pltpu.make_async_copy(fwd_low_hbm, fwd_low_ref, local_sem.at[5])
    load_log = pltpu.make_async_copy(log_hbm.at[r], log_ref, local_sem.at[6])
    load_back = pltpu.make_async_copy(back_hbm, back_ref, local_sem.at[7])
    barrier = pltpu.get_barrier_semaphore()

    def greet(cond, dev):
        when(
            cond,
            lambda: pl.semaphore_signal(barrier, inc=1, device_id=dev, device_id_type=MESH),
        )

    first = a % 4 == 0
    last = a % 4 == 3
    greet(a + 1 < n_ang, (r, a + 1))
    greet(a > 0, (r, a - 1))
    greet(first, (r, a + 3))
    greet(last, (r, a - 3))
    ends = jnp.where(a > 0, 1, 0) + jnp.where(a + 1 < n_ang, 1, 0)
    ends = ends + jnp.where(first | last, 1, 0)
    for d in (1, 2):
        greet(r + d < n_rad, (r + d, a))
        greet(r - d >= 0, (r - d, a))
        ends = ends + jnp.where(r + d < n_rad, 1, 0) + jnp.where(r - d >= 0, 1, 0)
    pl.semaphore_signal(barrier, inc=1, device_id=partner, device_id_type=MESH)
    for d in range(1, GROUPS):
        pl.semaphore_signal(barrier, inc=1, device_id=peer(d), device_id_type=MESH)
    for load in (load_rows, load_degree, load_density, load_high, load_low):
        load.start()
    for load in (load_rest, load_log, load_back):
        load.start()
    pl.semaphore_wait(barrier, GROUPS + ends)

    deep = shells // QUARTERS
    rows_up, rows_down, skip_up, skip_down, hand_up, hand_down = [], [], [], [], [], []
    for c in range(QUARTERS):
        part = pl.ds(c * deep, deep)
        high = x_ref.at[:, part, rows - WIDTH : rows]
        low = x_ref.at[:, part, 0:WIDTH]
        under = ext.at[:, part, PADR - WIDTH : PADR]
        over = ext.at[:, part, PADR + rows : PADR + rows + WIDTH]
        up_sems = ang_send.at[0, c], ang_recv.at[0, c]
        down_sems = ang_send.at[1, c], ang_recv.at[1, c]
        rows_up.append(remote(high, under, *up_sems, (r, a + 1)))
        rows_down.append(remote(low, over, *down_sems, (r, a - 1)))
        if c < QUARTERS - 1:
            spot = row_relay.at[c]
            skip_up.append(remote(high, spot, up_sems[0], skip_recv.at[c], (r, a + 4)))
            skip_down.append(remote(low, spot, down_sems[0], skip_recv.at[c], (r, a - 4)))
            hand_up.append(remote(spot, under, hand_send.at[c], up_sems[1], (r, a - 3)))
            hand_down.append(remote(spot, over, hand_send.at[c], down_sems[1], (r, a + 3)))
    n_up_skip = jnp.where(last & (a + 1 < n_ang), y + 1, 0)
    n_down_skip = jnp.where(first & (a > 0), QUARTERS - y, 0)
    n_up_hand = jnp.where(last, y, 0)
    n_down_hand = jnp.where(first, QUARTERS - 1 - y, 0)

    def start_rows(c):
        when((a + 1 < n_ang) & (c >= n_up_skip), rows_up[c].start)
        when((a > 0) & (c >= n_down_skip), rows_down[c].start)

    def start_skip(c):
        when(c < n_up_skip, skip_up[c].start)
        when(c < n_down_skip, skip_down[c].start)

    def hand_on(c):
        @pl.when(c < n_up_hand)
        def _():
            skip_up[c].wait_recv()
            hand_up[c].start()

        @pl.when(c < n_down_hand)
        def _():
            skip_down[c].wait_recv()
            hand_down[c].start()

    rad_up, rad_down, far_up, far_down, pass_up, pass_down = [], [], [], [], [], []
    for c in range(parts):
        part = pl.ds((c // CUTS) * ROWS, ROWS)
        band = pl.ds((c % CUTS) * wide, wide)
        above = x_ref.at[:, shells - WIDTH : shells, part, band]
        below = x_ref.at[:, 0:WIDTH, part, band]
        lo_part, hi_part = lo.at[:, :, part, band], hi.at[:, :, part, band]
        up_sems = rad_send.at[0, c], rad_recv.at[0, c]
        down_sems = rad_send.at[1, c], rad_recv.at[1, c]
        rad_up.append(remote(above, lo_part, *up_sems, (r + 1, a)))
        rad_down.append(remote(below, hi_part, *down_sems, (r - 1, a)))
        if c < n_far:
            spot = relay.at[c]
            far_up.append(remote(above, spot, up_sems[0], far_recv.at[c], (r + 2, a)))
            far_down.append(remote(below, spot, down_sems[0], far_recv.at[c], (r - 2, a)))
            pass_up.append(remote(spot, lo_part, pass_send.at[c], up_sems[1], (r - 1, a)))
            pass_down.append(remote(spot, hi_part, pass_send.at[c], down_sems[1], (r + 1, a)))
    odd = r % 2 == 1
    even = r % 2 == 0
    n_up_far = jnp.where(odd & (r + 2 < n_rad), CUTS * ((r + 1) // 2), 0)
    n_down_far = jnp.where(even & (r > 0), parts - CUTS * (r // 2), 0)
    n_up_pass = jnp.where(odd & (r > 1), CUTS * ((r - 1) // 2), 0)
    n_down_pass = jnp.where(even & (r + 2 < n_rad), n_far - CUTS * (r // 2), 0)

    def start_far(c):
        when(c < n_up_far, far_up[c].start)
        when(c < n_down_far, far_down[c].start)

    def start_chunk(c):
        when((r + 1 < n_rad) & (c >= n_up_far), rad_up[c].start)
        when((r > 0) & (c >= n_down_far), rad_down[c].start)

    def pass_on(c):
        @pl.when(c < n_up_pass)
        def _():
            far_up[c].wait_recv()
            pass_up[c].start()

        @pl.when(c < n_down_pass)
        def _():
            far_down[c].wait_recv()
            pass_down[c].start()

    for c in range(QUARTERS - 1):
        start_skip(c)
    for c in range(QUARTERS):
        start_rows(c)
    for c in range(n_far):
        start_far(c)
    for c in range(CUTS):
        start_chunk(c)

    @pl.when(a == 0)
    def _():
        ext[:, :, 0:PADR, :] = jnp.zeros((4, shells, PADR, cols), f32)

    @pl.when(a == n_ang - 1)
    def _():
        ext[:, :, PADR + rows : span, :] = jnp.zeros((4, shells, PADR, cols), f32)

    @pl.when(r == 0)
    def _():
        lo[...] = jnp.zeros_like(lo)

    @pl.when(r == n_rad - 1)
    def _():
        hi[...] = jnp.zeros_like(hi)

    @pl.when(r < 2)
    def _():
        chain_up[1:] = jnp.zeros((n_rad // 2 - 1, 8, LANES), f32)

    @pl.when(r + 2 >= n_rad)
    def _():
        chain_down[1:] = jnp.zeros((n_rad // 2 - 1, 8, LANES), f32)

    load_rows.wait()
    load_degree.wait()
    cosine = jnp.broadcast_to(rowtab[:, 0:1], (span, LANES))
    sine = jnp.broadcast_to(rowtab[:, 1:2], (span, LANES))
    order = lax.broadcasted_iota(jnp.int32, (span, LANES), 1) % MPAD
    power = jnp.full((span, LANES), 1.0, f32)
    square = sine
    for bit in range(6):
        power = jnp.where((order // (1 << bit)) % 2 == 1, power * square, power)
        square = square * square
    level = power * degree_ref[0:1, :]
    leg[0] = level

    def next_level(k, carry):
        last, before = carry
        alpha = degree_ref[pl.ds(k, 1), :]
        beta = degree_ref[pl.ds(NK + k, 1), :]
        new = alpha * (cosine * last - beta * before)
        leg[k] = new
        return (new, last)

    lax.fori_loop(1, NK, next_level, (level, jnp.zeros_like(level)))

    for c in range(QUARTERS - 1):
        hand_on(c)

    load_density.wait()
    load_high.wait()
    load_low.wait()
    weight = sine[PADR : PADR + rows] * (step_t * step_p)
    half = shells // 2
    for h in range(2):
        cells = ext[0, h * half : (h + 1) * half, PADR : PADR + rows, :]
        high, low = split(cells.reshape(half * rows, cols))
        sums = dot(high, fwd_high_ref[...]) + (
            dot(low, fwd_high_ref[...]) + dot(high, fwd_low_ref[...])
        )
        for q in range(half):
            spec[pl.ds((h * half + q) * rows, rows), :] = (
                sums[q * rows : (q + 1) * rows] * weight
            )
    spectra = [spec[pl.ds(j, shells, stride=rows), :] for j in range(rows)]

    def moment(k, carry):
        parts = [jnp.zeros((shells, LANES), f32) for _ in range(4)]
        for j in range(rows):
            parts[j % 4] = parts[j % 4] + spectra[j] * leg[k, PADR + j : PADR + j + 1, :]
        partial[k // KD, k % KD] = (parts[0] + parts[1]) + (parts[2] + parts[3])
        return carry

    lax.fori_loop(0, NK, moment, 0)

    def exchange_a(d):
        return remote(
            partial.at[(g + d) % GROUPS], got_a.at[d], a_send.at[d], a_recv.at[d], peer(d)
        )

    for d in range(1, GROUPS):
        exchange_a(d).start()

    load_rest.wait()

    def phi_flux(index, carry):
        i = index // chunks
        at = pl.multiple_of((index % chunks) * ROWS, ROWS)
        cell_radius = inner_radius + step_r * ((r * shells + i).astype(f32) + 0.5)
        sums, jumps = [], []
        for c in range(4):
            u = ext[c, i, pl.ds(PADR + at, ROWS), :]
            left = pltpu.roll(u, 1, 1)
            near = u + left
            mid = pltpu.roll(u, cols - 1, 1) + pltpu.roll(u, 2, 1)
            far = pltpu.roll(u, cols - 2, 1) + pltpu.roll(u, 3, 1)
            sums.append(37.0 * near - 8.0 * mid + far)
            jumps.append(u - left)
        for c, face in enumerate(flux(sums, jumps, 3)):
            tend[c, i, pl.ds(at, ROWS), :] = (face - pltpu.roll(face, cols - 1, 1)) * (
                cell_radius / step_p
            )
        return carry

    lax.fori_loop(0, shells * chunks // 2, phi_flux, 0)

    for d in range(1, GROUPS):
        exchange_a(d).wait_recv()
    total = partial[g]
    for d in range(1, GROUPS):
        total = total + got_a[d]
    mine[...] = total
    exchange_b = remote(mine, got_b, b_send.at[0], b_recv.at[0], partner)
    exchange_b.start()
    for c in range(CUTS, 2 * CUTS):
        start_chunk(c)

    lax.fori_loop(shells * chunks // 2, shells * chunks, phi_flux, 0)

    for c in range(QUARTERS):
        when(a > 0, rows_up[c].wait_recv)
        when(a + 1 < n_ang, rows_down[c].wait_recv)
    tiles = cols // LANES

    def theta_flux(index, carry):
        i = index // tiles
        lanes = pl.ds(pl.multiple_of((index % tiles) * LANES, LANES), LANES)
        cell_radius = inner_radius + step_r * ((r * shells + i).astype(f32) + 0.5)
        area = jnp.broadcast_to(rowtab[:, 2:3], (span, LANES)) * (cell_radius / step_t)
        sums, jumps = [], []
        for c in range(4):
            u = ext[c, i, :, lanes]
            left = pltpu.roll(u, 1, 0)
            near = u + left
            mid = pltpu.roll(u, span - 1, 0) + pltpu.roll(u, 2, 0)
            far = pltpu.roll(u, span - 2, 0) + pltpu.roll(u, 3, 0)
            sums.append(37.0 * near - 8.0 * mid + far)
            jumps.append(u - left)
        for c, face in enumerate(flux(sums, jumps, 2)):
            face = face * area
            change = face - pltpu.roll(face, span - 1, 0)
            tend[c, i, :, lanes] = tend[c, i, :, lanes] + change[PADR : PADR + rows]
        return carry

    lax.fori_loop(0, shells * tiles // 4, theta_flux, 0)

    exchange_b.wait_recv()
    total = mine[...] + got_b[...]
    load_log.wait()
    log_radius = log_ref[...]
    shell = lax.broadcasted_iota(jnp.int32, (shells, LANES), 0)
    radius = inner_radius + step_r * ((r * shells + shell).astype(f32) + 0.5)
    order = lax.broadcasted_iota(jnp.int32, (shells, LANES), 1) % MPAD
    ups, downs, powers, degrees = [], [], [], []
    for q in range(KD):
        degree = (order + (g * KD + q)).astype(f32)
        grow = jnp.exp(degree * log_radius)
        weighted = (radius * radius * step_r) * total[q]
        up = grow * weighted
        down = weighted / (radius * grow)
        for s in (1, 2, 4):
            up = up + jnp.where(shell >= s, pltpu.roll(up, s, 0), 0.0)
            down = down + jnp.where(shell >= s, pltpu.roll(down, s, 0), 0.0)
        totals[0, q : q + 1, :] = up[shells - 1 : shells]
        totals[1, q : q + 1, :] = down[shells - 1 : shells]
        ups.append(up)
        downs.append(down)
        powers.append(grow)
        degrees.append(degree)

    pair = remote(totals, got_pair, c_send.at[0, 0], c_recv.at[0, 0], (r + 1 - 2 * (r % 2), a))
    pair.start()

    def hop_up(d):
        return remote(
            chain_up.at[d - 1], chain_up.at[d], c_send.at[0, d], c_recv.at[0, d], (r + 2, a)
        )

    def hop_down(d):
        return remote(
            chain_down.at[d - 1], chain_down.at[d], c_send.at[1, d], c_recv.at[1, d], (r - 2, a)
        )

    def start_hop(d):
        when(r + 2 < n_rad, hop_up(d).start)
        when(r - 2 >= 0, hop_down(d).start)

    def end_hop(d):
        when(r - 2 >= 0, hop_up(d).wait_recv)
        when(r + 2 < n_rad, hop_down(d).wait_recv)

    for c in range(2 * CUTS, 3 * CUTS):
        pass_on(c - 2 * CUTS)
        start_chunk(c)
    for c in range(CUTS, 2 * CUTS):
        pass_on(c)

    quarter = shells * tiles // 4
    lax.fori_loop(quarter, 2 * quarter, theta_flux, 0)
    pair.wait_recv()
    pair_up = got_pair[0]
    pair_down = got_pair[1]
    chain_up[0] = totals[0] + pair_up
    chain_down[0] = totals[1] + pair_down
    start_hop(1)
    lax.fori_loop(2 * quarter, 3 * quarter, theta_flux, 0)
    end_hop(1)
    start_hop(2)
    lax.fori_loop(3 * quarter, 4 * quarter, theta_flux, 0)
    end_hop(2)
    start_hop(3)
    below = jnp.where(odd, pair_up, 0.0)
    above = jnp.where(even, pair_down, 0.0)
    end_hop(3)
    for d in range(1, n_rad // 2):
        below = below + chain_up[d]
        above = above + chain_down[d]
    inverse_radius = 1.0 / radius
    for q in range(KD):
        inner = below[q : q + 1] + ups[q]
        outer = above[q : q + 1] + (downs[q][shells - 1 : shells] - downs[q])
        degree = degrees[q]
        norm = (-4.0 * math.pi) / (2.0 * degree + 1.0)
        inner_term = inner * inverse_radius / powers[q]
        outer_term = powers[q] * outer
        coef[g, 0, q] = norm * (inner_term + outer_term)
        coef[g, 1, q] = (
            norm * (degree * outer_term - (degree + 1.0) * inner_term) * inverse_radius
        )

    def exchange_d(d):
        return remote(coef.at[g], coef.at[g], d_send.at[d], d_recv.at[d], peer(d))

    for d in range(1, GROUPS):
        exchange_d(d).start()
    for c in range(2 * CUTS, 3 * CUTS):
        pass_on(c)
        start_chunk(c + CUTS)
    for d in range(1, GROUPS):
        exchange_d(d).wait_recv()

    slope_row = degree_ref[2 * NK : 2 * NK + 1, :]
    theta_scale = 1.0 / (2.0 * step_t)
    for i in range(0, shells, 2):

        def synthesize(h, carry):
            sums = list(carry)
            for q in range(KD):
                k = h * KD + q
                full = leg[k]
                value = full[PADR : PADR + rows]
                change = pltpu.roll(full, span - 1, 0) - pltpu.roll(full, 1, 0)
                change = change[PADR : PADR + rows]
                for p in range(2):
                    cp = coef[h, 0, q, i + p : i + p + 1, :]
                    cs = coef[h, 1, q, i + p : i + p + 1, :]
                    sums[3 * p] = sums[3 * p] + value * cp
                    sums[3 * p + 1] = sums[3 * p + 1] + value * cs
                    sums[3 * p + 2] = sums[3 * p + 2] + change * cp
            return tuple(sums)

        zero = jnp.zeros((rows, LANES), f32)
        sums = lax.fori_loop(0, (LMAX + KD) // KD, synthesize, (zero,) * 6)
        for p in range(2):
            base, slope, change = sums[3 * p : 3 * p + 3]
            at = (i + p) * 4 * rows
            table[at : at + rows, :] = base
            table[at + rows : at + 2 * rows, :] = slope
            table[at + 2 * rows : at + 3 * rows, :] = change * theta_scale
            table[at + 3 * rows : at + 4 * rows, :] = pltpu.roll(base, MPAD, 1) * slope_row

    load_back.wait()

    def sources(i, carry):
        at = pl.multiple_of(i * 4 * rows, 4 * rows)
        high, low = split(table[pl.ds(at, 4 * rows), :])
        fields[...] = dot(jnp.concatenate([high, low, high], axis=1), back_ref[...])
        pot[i] = fields[0:rows, :]
        cell_radius = inner_radius + step_r * ((r * shells + i).astype(f32) + 0.5)
        for c in range(chunks):
            at = c * ROWS
            inside = pl.ds(PADR + at, ROWS)
            sine = jnp.broadcast_to(rowtab[inside, 1:2], (ROWS, cols)) * cell_radius
            cosine = jnp.broadcast_to(rowtab[inside, 0:1], (ROWS, cols)) * cell_radius
            density = ext[0, i, inside, :]
            mom_r = ext[1, i, inside, :]
            mom_t = ext[2, i, inside, :]
            mom_p = ext[3, i, inside, :]
            inverse = 1.0 / density
            vel_t = mom_t * inverse
            vel_p = mom_p * inverse
            pull = grav_const * density
            slope = fields[rows + at : rows + at + ROWS, :]
            grad_t = fields[2 * rows + at : 2 * rows + at + ROWS, :]
            grad_p = fields[3 * rows + at : 3 * rows + at + ROWS, :]
            twist = mom_p * vel_p
            source_r = sine * (
                (mom_t * vel_t + twist)
                + (2.0 * sound_sq) * density
                - (cell_radius * pull) * slope
            )
            source_t = cosine * (twist + sound_sq * density) - sine * (
                mom_r * vel_t + pull * grad_t
            )
            source_p = -(
                vel_p * (mom_r * sine + mom_t * cosine) + (cell_radius * pull) * grad_p
            )
            spot = pl.ds(at, ROWS)
            tend[1, i, spot, :] = tend[1, i, spot, :] + source_r
            tend[2, i, spot, :] = tend[2, i, spot, :] + source_t
            tend[3, i, spot, :] = tend[3, i, spot, :] + source_p
        return carry

    lax.fori_loop(0, shells, sources, 0)

    per = wide // LANES
    for chunk in range(parts):
        when(r > 0, rad_up[chunk].wait_recv)
        when(r + 1 < n_rad, rad_down[chunk].wait_recv)
        at = (chunk // CUTS) * ROWS
        spot = pl.ds(at, ROWS)
        first = (chunk % CUTS) * per

        def radial_flux(tile, carry):
            lanes = pl.ds(pl.multiple_of(tile * LANES, LANES), LANES)
            sine = jnp.broadcast_to(
                rowtab[PADR + at : PADR + at + ROWS, 1:2], (ROWS, LANES)
            ) * (section_step / step_r)

            def cell(c, s):
                if s < 0:
                    return lo[c, s + WIDTH, spot, lanes]
                if s >= shells:
                    return hi[c, s - shells, spot, lanes]
                return ext[c, s, pl.ds(PADR + at, ROWS), lanes]

            u = [[cell(c, s) for s in range(-WIDTH, shells + WIDTH)] for c in range(4)]
            last = None
            for f in range(shells + 1):
                place = r * shells + f
                face_radius = inner_radius + step_r * place.astype(f32)
                area = jnp.where(
                    (place > 0) & (place < n_rad * shells), face_radius * face_radius, 0.0
                )
                sums, jumps = [], []
                for c in range(4):
                    w = u[c][f : f + 6]
                    sums.append(37.0 * (w[2] + w[3]) - 8.0 * (w[1] + w[4]) + (w[0] + w[5]))
                    jumps.append(w[3] - w[2])
                face = [value * area for value in flux(sums, jumps, 1)]
                if f > 0:
                    for c in range(4):
                        tend[c, f - 1, spot, lanes] = (
                            section_step * tend[c, f - 1, spot, lanes]
                            - (face[c] - last[c]) * sine
                        )
                last = face
            return carry

        lax.fori_loop(first, first + per, radial_flux, 0)

    for c in range(QUARTERS):
        when(a + 1 < n_ang, rows_up[c].wait_send)
        when(a > 0, rows_down[c].wait_send)
        if c < QUARTERS - 1:
            when((c < n_up_hand) | (c < n_down_hand), hand_up[c].wait_send)
    for c in range(parts):
        when(r + 1 < n_rad, rad_up[c].wait_send)
        when(r > 0, rad_down[c].wait_send)
        if c < n_far:
            when((c < n_up_pass) | (c < n_down_pass), pass_up[c].wait_send)
    for d in range(1, GROUPS):
        exchange_a(d).wait_send()
        exchange_d(d).wait_send()
    exchange_b.wait_send()
    pair.wait_send()
    for d in range(1, n_rad // 2):
        when(r + 2 < n_rad, hop_up(d).wait_send)
        when(r - 2 >= 0, hop_down(d).wait_send)


def store(tend, pot, inc_ref, pot_ref, sem):
    copies = [
        pltpu.make_async_copy(tend.at[c], inc_ref.at[c], sem.at[c]) for c in range(tend.shape[0])
    ]
    copies.append(pltpu.make_async_copy(pot, pot_ref, sem.at[len(copies)]))
    for copy in copies:
        copy.start()
    for copy in copies:
        copy.wait()


def solution(mesh):
    n_rad = mesh.shape["rad"]
    n_ang = mesh.shape["ang"]

    def body(state):
        _, shells, rows, cols = state.shape
        high, low, back, slope = phi_tables(cols)
        operands = (
            state,
            jnp.asarray(high),
            jnp.asarray(low),
            jnp.asarray(back),
            jnp.asarray(row_tables(n_ang, rows)),
            jnp.asarray(degree_tables(slope)),
            jnp.asarray(log_radii(n_rad, shells)),
        )
        span = rows + 2 * PADR
        parts = (rows // ROWS) * CUTS
        inside = pl.BlockSpec(memory_space=pltpu.VMEM)
        dma = pltpu.SemaphoreType.DMA
        increment, potential = pl.pallas_call(
            functools.partial(kernel, n_rad, n_ang, shells, rows, cols),
            out_shape=(
                pltpu.VMEM(state.shape, f32),
                pltpu.VMEM(state.shape[1:], f32),
            ),
            in_specs=[pl.BlockSpec(memory_space=pltpu.HBM)] * 7,
            out_specs=(inside, inside),
            scratch_shapes=[
                pltpu.VMEM((4, shells, span, cols), f32),
                pltpu.VMEM((4, WIDTH, rows, cols), f32),
                pltpu.VMEM((4, WIDTH, rows, cols), f32),
                pltpu.VMEM((parts - CUTS, 4, WIDTH, ROWS, cols // CUTS), f32),
                pltpu.VMEM((QUARTERS - 1, 4, shells // QUARTERS, WIDTH, cols), f32),
                pltpu.VMEM((4 * rows, cols), f32),
                pltpu.VMEM((shells * 4 * rows, LANES), f32),
                pltpu.VMEM((shells * rows, LANES), f32),
                pltpu.VMEM((cols, LANES), bf16),
                pltpu.VMEM((cols, LANES), bf16),
                pltpu.VMEM((3 * LANES, cols), bf16),
                pltpu.VMEM((span, LANES), f32),
                pltpu.VMEM((2 * NK + 8, LANES), f32),
                pltpu.VMEM((shells, LANES), f32),
                pltpu.VMEM((NK, span, LANES), f32),
                pltpu.VMEM((GROUPS, KD, shells, LANES), f32),
                pltpu.VMEM((GROUPS, KD, shells, LANES), f32),
                pltpu.VMEM((KD, shells, LANES), f32),
                pltpu.VMEM((KD, shells, LANES), f32),
                pltpu.VMEM((2, 8, LANES), f32),
                pltpu.VMEM((2, 8, LANES), f32),
                pltpu.VMEM((n_rad // 2, 8, LANES), f32),
                pltpu.VMEM((n_rad // 2, 8, LANES), f32),
                pltpu.VMEM((GROUPS, 2, KD, shells, LANES), f32),
                dma((8,)),
                dma((2, QUARTERS)),
                dma((2, QUARTERS)),
                dma((QUARTERS - 1,)),
                dma((QUARTERS - 1,)),
                dma((2, parts)),
                dma((2, parts)),
                dma((parts - CUTS,)),
                dma((parts - CUTS,)),
                dma((GROUPS,)),
                dma((GROUPS,)),
                dma((1,)),
                dma((1,)),
                dma((2, n_rad // 2)),
                dma((2, n_rad // 2)),
                dma((GROUPS,)),
                dma((GROUPS,)),
            ],
            compiler_params=pltpu.CompilerParams(
                collective_id=0, has_side_effects=True, vmem_limit_bytes=61_700_000
            ),
        )(*operands)
        outside = pl.BlockSpec(memory_space=pltpu.HBM)
        return pl.pallas_call(
            store,
            out_shape=(
                jax.ShapeDtypeStruct(state.shape, f32),
                jax.ShapeDtypeStruct(state.shape[1:], f32),
            ),
            in_specs=(inside, inside),
            out_specs=(outside, outside),
            scratch_shapes=[dma((5,))],
            compiler_params=pltpu.CompilerParams(vmem_limit_bytes=1 << 20),
        )(increment, potential)

    return jax.shard_map(
        body,
        mesh=mesh,
        in_specs=(P(None, "rad", "ang", None),),
        out_specs=(P(None, "rad", "ang", None), P("rad", "ang", None)),
        check_vma=False,
    )
```

```python
import functools
import math

import jax
import jax.numpy as jnp
import numpy as np
from jax import lax
from jax.experimental import pallas as pl
from jax.experimental.pallas import tpu as pltpu
from jax.sharding import PartitionSpec as P

LMAX = 48
MPAD = 64
LANES = 128
NK = 56
GROUPS = 8
KD = 7
PADR = 8
WIDTH = 3
ROWS = 8
QUARTERS = 4
CUTS = 2

sound_speed = 0.5
sound_sq = 0.25
grav_const = 100.0
section_step = 0.001
inner_radius = 1.0
radial_span = 0.1
MESH = pl.DeviceIdType.MESH
f32 = jnp.float32
bf16 = jnp.bfloat16


def split_np(table):
    high = table.astype(bf16)
    low = (table - high.astype(np.float64)).astype(bf16)
    return high, low


def phi_tables(count):
    order = np.arange(MPAD, dtype=np.float64)
    norm = np.where(order > 0.5, math.sqrt(2.0), 1.0)
    phase = (2.0 * math.pi / count) * (np.outer(np.arange(count), np.arange(MPAD)) % count)
    table = np.concatenate([np.cos(phase) * norm, np.sin(phase) * norm], axis=1)
    high, low = split_np(table)
    back = np.concatenate([high.T, high.T, low.T], axis=0)
    step = 2.0 * math.pi / count
    slope = np.sin(order * step) / step
    return high, low, back, np.concatenate([slope, -slope])


def row_tables(blocks, rows):
    total = blocks * rows
    step_t = math.pi / total
    row = np.arange(blocks)[:, None] * rows + np.arange(rows + 2 * PADR)[None, :] - PADR
    theta = step_t * (row + 0.5)
    face = np.where((row > 0) & (row < total), np.sin(step_t * row), 0.0)
    table = np.zeros((blocks, rows + 2 * PADR, LANES))
    table[:, :, 0] = np.cos(theta)
    table[:, :, 1] = np.sin(theta)
    table[:, :, 2] = face
    return table.astype(np.float32)


def degree_tables(slope):
    m = np.arange(LANES) % MPAD
    k = np.arange(NK)[:, None]
    l = (m + k).astype(np.float64)
    alpha = np.zeros((NK, LANES))
    beta = np.zeros((NK, LANES))
    norm = np.full(LANES, 1.0 / math.sqrt(4.0 * math.pi))
    for q in range(1, MPAD):
        norm = np.where(m >= q, norm * math.sqrt((2.0 * q + 1.0) / (2.0 * q)), norm)
    alpha[0] = norm
    alpha[1:] = np.sqrt((4.0 * l[1:] ** 2 - 1.0) / (l[1:] ** 2 - m**2))
    beta[2:] = np.sqrt(((l[2:] - 1.0) ** 2 - m**2) / (4.0 * (l[2:] - 1.0) ** 2 - 1.0))
    alpha = np.where(l <= LMAX, alpha, 0.0)
    extra = np.zeros((8, LANES))
    extra[0] = slope
    return np.concatenate([alpha, beta, extra]).astype(np.float32)


def log_radii(blocks, shells):
    radius = inner_radius + radial_span / (blocks * shells) * (np.arange(blocks * shells) + 0.5)
    table = np.log(radius).reshape(blocks, shells, 1)
    return np.broadcast_to(table, (blocks, shells, LANES)).astype(np.float32)


def split(value):
    high = value.astype(bf16)
    return high, (value - high.astype(f32)).astype(bf16)


def dot(a, b):
    return jnp.dot(a, b, preferred_element_type=f32)


def flux(sums, jumps, component):
    inverse = 1.0 / sums[0]
    speed = sums[component] * inverse
    scaled = speed * (1.0 / 60.0)
    wave = 0.5 * (sound_speed + jnp.abs(speed))
    out = [s * scaled - wave * j for s, j in zip(sums, jumps)]
    out[component] = out[component] + (sound_sq / 60.0) * sums[0]
    return out


def kernel(
    n_rad,
    n_ang,
    shells,
    rows,
    cols,
    x_ref,
    fwd_high_hbm,
    fwd_low_hbm,
    back_hbm,
    row_hbm,
    degree_hbm,
    log_hbm,
    tend,
    pot,
    ext,
    lo,
    hi,
    relay,
    row_relay,
    fields,
    table,
    spec,
    fwd_high_ref,
    fwd_low_ref,
    back_ref,
    rowtab,
    degree_ref,
    log_ref,
    leg,
    partial,
    got_a,
    mine,
    got_b,
    totals,
    got_pair,
    chain_up,
    chain_down,
    coef,
    rounds,
    local_sem,
    ang_send,
    ang_recv,
    skip_recv,
    hand_send,
    rad_send,
    rad_recv,
    far_recv,
    pass_send,
    a_send,
    a_recv,
    b_send,
    b_recv,
    c_send,
    c_recv,
    d_send,
    d_recv,
):
    r = lax.axis_index("rad")
    a = lax.axis_index("ang")
    y, x_hi, core = a // 4, (a // 2) % 2, a % 2
    g = y * 2 + core
    chunks = rows // ROWS
    parts = chunks * CUTS
    wide = cols // CUTS
    n_far = parts - CUTS
    span = rows + 2 * PADR
    own = pl.ds(PADR, rows)
    step_r = radial_span / (n_rad * shells)
    step_t = math.pi / (n_ang * rows)
    step_p = 2.0 * math.pi / cols

    def peer(d):
        q = (g + d) % GROUPS
        return (r, (q // 2) * 4 + x_hi * 2 + q % 2)

    partner = (r, y * 4 + (1 - x_hi) * 2 + core)

    def when(cond, run):
        @pl.when(cond)
        def _():
            run()

    def remote(src, dst, send, recv, dev):
        return pltpu.make_async_remote_copy(
            src_ref=src,
            dst_ref=dst,
            send_sem=send,
            recv_sem=recv,
            device_id=dev,
            device_id_type=MESH,
        )

    load_density = pltpu.make_async_copy(x_ref.at[0], ext.at[0, :, own], local_sem.at[0])
    load_rest = pltpu.make_async_copy(
        x_ref.at[1:4], ext.at[1:4, :, own], local_sem.at[1]
    )
    load_rows = pltpu.make_async_copy(row_hbm.at[a], rowtab, local_sem.at[2])
    load_degree = pltpu.make_async_copy(degree_hbm, degree_ref, local_sem.at[3])
    load_high = pltpu.make_async_copy(fwd_high_hbm, fwd_high_ref, local_sem.at[4])
    load_low = pltpu.make_async_copy(fwd_low_hbm, fwd_low_ref, local_sem.at[5])
    load_log = pltpu.make_async_copy(log_hbm.at[r], log_ref, local_sem.at[6])
    load_back = pltpu.make_async_copy(back_hbm, back_ref, local_sem.at[7])
    barrier = pltpu.get_barrier_semaphore()
    first = a % 4 == 0
    last = a % 4 == 3
    odd = r % 2 == 1
    even = r % 2 == 0
    x = x_hi * 2 + r % 2

    def along_x(step):
        to = (x + step) % 4
        return ((r // 2) * 2 + to % 2, y * 4 + (to // 2) * 2 + core)

    near = [
        (None, along_x(1)),
        (None, along_x(3)),
        (r + 2 < n_rad, (r + 2, a)),
        (r - 2 >= 0, (r - 2, a)),
        (a + 4 < n_ang, (r, a + 4)),
        (a - 4 >= 0, (r, a - 4)),
        (None, (r, a + 1 - 2 * core)),
    ]
    n_near = 3
    for cond, _ in near:
        if cond is not None:
            n_near = n_near + jnp.where(cond, 1, 0)

    def greet(sem):
        for cond, dev in near:
            signal = functools.partial(
                pl.semaphore_signal, sem, inc=1, device_id=dev, device_id_type=MESH
            )
            if cond is None:
                signal()
            else:
                when(cond, signal)

    greet(barrier)
    for load in (load_rows, load_degree, load_density, load_high, load_low):
        load.start()
    for load in (load_rest, load_log, load_back):
        load.start()
    pl.semaphore_wait(barrier, n_near)
    greet(rounds.at[0])

    deep = shells // QUARTERS
    rows_up, rows_down, skip_up, skip_down, hand_up, hand_down = [], [], [], [], [], []
    for c in range(QUARTERS):
        part = pl.ds(c * deep, deep)
        high = x_ref.at[:, part, rows - WIDTH : rows]
        low = x_ref.at[:, part, 0:WIDTH]
        under = ext.at[:, part, PADR - WIDTH : PADR]
        over = ext.at[:, part, PADR + rows : PADR + rows + WIDTH]
        up_sems = ang_send.at[0, c], ang_recv.at[0, c]
        down_sems = ang_send.at[1, c], ang_recv.at[1, c]
        rows_up.append(remote(high, under, *up_sems, (r, a + 1)))
        rows_down.append(remote(low, over, *down_sems, (r, a - 1)))
        if c < QUARTERS - 1:
            spot = row_relay.at[c]
            skip_up.append(remote(high, spot, up_sems[0], skip_recv.at[c], (r, a + 4)))
            skip_down.append(remote(low, spot, down_sems[0], skip_recv.at[c], (r, a - 4)))
            hand_up.append(remote(spot, under, hand_send.at[c], up_sems[1], (r, a - 3)))
            hand_down.append(remote(spot, over, hand_send.at[c], down_sems[1], (r, a + 3)))
    n_up_skip = jnp.where(last & (a + 1 < n_ang), y + 1, 0)
    n_down_skip = jnp.where(first & (a > 0), QUARTERS - y, 0)
    n_up_hand = jnp.where(last, y, 0)
    n_down_hand = jnp.where(first, QUARTERS - 1 - y, 0)

    def start_rows(c):
        when((a + 1 < n_ang) & (c >= n_up_skip), rows_up[c].start)
        when((a > 0) & (c >= n_down_skip), rows_down[c].start)

    def start_skip(c):
        when(c < n_up_skip, skip_up[c].start)
        when(c < n_down_skip, skip_down[c].start)

    def hand_on(c):
        @pl.when(c < n_up_hand)
        def _():
            skip_up[c].wait_recv()
            hand_up[c].start()

        @pl.when(c < n_down_hand)
        def _():
            skip_down[c].wait_recv()
            hand_down[c].start()

    rad_up, rad_down, far_up, far_down, pass_up, pass_down = [], [], [], [], [], []
    for c in range(parts):
        part = pl.ds((c // CUTS) * ROWS, ROWS)
        band = pl.ds((c % CUTS) * wide, wide)
        above = x_ref.at[:, shells - WIDTH : shells, part, band]
        below = x_ref.at[:, 0:WIDTH, part, band]
        lo_part, hi_part = lo.at[:, :, part, band], hi.at[:, :, part, band]
        up_sems = rad_send.at[0, c], rad_recv.at[0, c]
        down_sems = rad_send.at[1, c], rad_recv.at[1, c]
        rad_up.append(remote(above, lo_part, *up_sems, (r + 1, a)))
        rad_down.append(remote(below, hi_part, *down_sems, (r - 1, a)))
        if c < n_far:
            spot = relay.at[c]
            far_up.append(remote(above, spot, up_sems[0], far_recv.at[c], (r + 2, a)))
            far_down.append(remote(below, spot, down_sems[0], far_recv.at[c], (r - 2, a)))
            pass_up.append(remote(spot, lo_part, pass_send.at[c], up_sems[1], (r - 1, a)))
            pass_down.append(remote(spot, hi_part, pass_send.at[c], down_sems[1], (r + 1, a)))
    n_up_far = jnp.where(odd & (r + 2 < n_rad), CUTS * ((r + 1) // 2), 0)
    n_down_far = jnp.where(even & (r > 0), parts - CUTS * (r // 2), 0)
    n_up_pass = jnp.where(odd & (r > 1), CUTS * ((r - 1) // 2), 0)
    n_down_pass = jnp.where(even & (r + 2 < n_rad), n_far - CUTS * (r // 2), 0)

    def start_far(c):
        when(c < n_up_far, far_up[c].start)
        when(c < n_down_far, far_down[c].start)

    def start_pair(c):
        when(even, rad_up[c].start)
        when(odd, rad_down[c].start)

    def start_diagonal(c):
        when(odd & (r + 1 < n_rad) & (c >= n_up_far), rad_up[c].start)
        when(even & (r > 0) & (c >= n_down_far), rad_down[c].start)

    def start_chunk(c):
        start_pair(c)
        start_diagonal(c)

    def pass_on(c):
        @pl.when(c < n_up_pass)
        def _():
            far_up[c].wait_recv()
            pass_up[c].start()

        @pl.when(c < n_down_pass)
        def _():
            far_down[c].wait_recv()
            pass_down[c].start()

    start_pair(0)
    for c in range(n_far):
        start_far(c)
    for c in range(QUARTERS - 1):
        start_skip(c)
    for c in range(1, CUTS):
        start_pair(c)
    pl.semaphore_wait(rounds.at[0], n_near)
    greet(rounds.at[1])
    for c in range(CUTS):
        start_diagonal(c)
    pl.semaphore_wait(rounds.at[1], n_near)
    greet(rounds.at[2])
    pl.semaphore_wait(rounds.at[2], n_near)
    for c in range(QUARTERS):
        start_rows(c)

    @pl.when(a == 0)
    def _():
        ext[:, :, 0:PADR, :] = jnp.zeros((4, shells, PADR, cols), f32)

    @pl.when(a == n_ang - 1)
    def _():
        ext[:, :, PADR + rows : span, :] = jnp.zeros((4, shells, PADR, cols), f32)

    @pl.when(r == 0)
    def _():
        lo[...] = jnp.zeros_like(lo)

    @pl.when(r == n_rad - 1)
    def _():
        hi[...] = jnp.zeros_like(hi)

    @pl.when(r < 2)
    def _():
        chain_up[1:] = jnp.zeros((n_rad // 2 - 1, 8, LANES), f32)

    @pl.when(r + 2 >= n_rad)
    def _():
        chain_down[1:] = jnp.zeros((n_rad // 2 - 1, 8, LANES), f32)

    load_rows.wait()
    load_degree.wait()
    cosine = jnp.broadcast_to(rowtab[:, 0:1], (span, LANES))
    sine = jnp.broadcast_to(rowtab[:, 1:2], (span, LANES))
    order = lax.broadcasted_iota(jnp.int32, (span, LANES), 1) % MPAD
    power = jnp.full((span, LANES), 1.0, f32)
    square = sine
    for bit in range(6):
        power = jnp.where((order // (1 << bit)) % 2 == 1, power * square, power)
        square = square * square
    level = power * degree_ref[0:1, :]
    leg[0] = level

    def next_level(k, carry):
        last, before = carry
        alpha = degree_ref[pl.ds(k, 1), :]
        beta = degree_ref[pl.ds(NK + k, 1), :]
        new = alpha * (cosine * last - beta * before)
        leg[k] = new
        return (new, last)

    lax.fori_loop(1, NK, next_level, (level, jnp.zeros_like(level)))

    for c in range(QUARTERS - 1):
        hand_on(c)

    load_density.wait()
    load_high.wait()
    load_low.wait()
    weight = sine[PADR : PADR + rows] * (step_t * step_p)
    half = shells // 2
    for h in range(2):
        cells = ext[0, h * half : (h + 1) * half, PADR : PADR + rows, :]
        high, low = split(cells.reshape(half * rows, cols))
        sums = dot(high, fwd_high_ref[...]) + (
            dot(low, fwd_high_ref[...]) + dot(high, fwd_low_ref[...])
        )
        for q in range(half):
            spec[pl.ds((h * half + q) * rows, rows), :] = (
                sums[q * rows : (q + 1) * rows] * weight
            )
    spectra = [spec[pl.ds(j, shells, stride=rows), :] for j in range(rows)]

    def moment(k, carry):
        parts = [jnp.zeros((shells, LANES), f32) for _ in range(4)]
        for j in range(rows):
            parts[j % 4] = parts[j % 4] + spectra[j] * leg[k, PADR + j : PADR + j + 1, :]
        partial[k // KD, k % KD] = (parts[0] + parts[1]) + (parts[2] + parts[3])
        return carry

    lax.fori_loop(0, NK, moment, 0)

    def exchange_a(d):
        return remote(
            partial.at[(g + d) % GROUPS], got_a.at[d], a_send.at[d], a_recv.at[d], peer(d)
        )

    for d in range(1, GROUPS):
        exchange_a(d).start()

    load_rest.wait()

    def phi_flux(index, carry):
        i = index // chunks
        at = pl.multiple_of((index % chunks) * ROWS, ROWS)
        cell_radius = inner_radius + step_r * ((r * shells + i).astype(f32) + 0.5)
        sums, jumps = [], []
        for c in range(4):
            u = ext[c, i, pl.ds(PADR + at, ROWS), :]
            left = pltpu.roll(u, 1, 1)
            near = u + left
            mid = pltpu.roll(u, cols - 1, 1) + pltpu.roll(u, 2, 1)
            far = pltpu.roll(u, cols - 2, 1) + pltpu.roll(u, 3, 1)
            sums.append(37.0 * near - 8.0 * mid + far)
            jumps.append(u - left)
        for c, face in enumerate(flux(sums, jumps, 3)):
            tend[c, i, pl.ds(at, ROWS), :] = (face - pltpu.roll(face, cols - 1, 1)) * (
                cell_radius / step_p
            )
        return carry

    lax.fori_loop(0, shells * chunks // 2, phi_flux, 0)

    for d in range(1, GROUPS):
        exchange_a(d).wait_recv()
    total = partial[g]
    for d in range(1, GROUPS):
        total = total + got_a[d]
    mine[...] = total
    exchange_b = remote(mine, got_b, b_send.at[0], b_recv.at[0], partner)
    exchange_b.start()
    for c in range(CUTS, 2 * CUTS):
        start_chunk(c)

    lax.fori_loop(shells * chunks // 2, shells * chunks, phi_flux, 0)

    for c in range(QUARTERS):
        when(a > 0, rows_up[c].wait_recv)
        when(a + 1 < n_ang, rows_down[c].wait_recv)
    tiles = cols // LANES

    def theta_flux(index, carry):
        i = index // tiles
        lanes = pl.ds(pl.multiple_of((index % tiles) * LANES, LANES), LANES)
        cell_radius = inner_radius + step_r * ((r * shells + i).astype(f32) + 0.5)
        area = jnp.broadcast_to(rowtab[:, 2:3], (span, LANES)) * (cell_radius / step_t)
        sums, jumps = [], []
        for c in range(4):
            u = ext[c, i, :, lanes]
            left = pltpu.roll(u, 1, 0)
            near = u + left
            mid = pltpu.roll(u, span - 1, 0) + pltpu.roll(u, 2, 0)
            far = pltpu.roll(u, span - 2, 0) + pltpu.roll(u, 3, 0)
            sums.append(37.0 * near - 8.0 * mid + far)
            jumps.append(u - left)
        for c, face in enumerate(flux(sums, jumps, 2)):
            face = face * area
            change = face - pltpu.roll(face, span - 1, 0)
            tend[c, i, :, lanes] = tend[c, i, :, lanes] + change[PADR : PADR + rows]
        return carry

    lax.fori_loop(0, shells * tiles // 4, theta_flux, 0)

    exchange_b.wait_recv()
    total = mine[...] + got_b[...]
    load_log.wait()
    log_radius = log_ref[...]
    shell = lax.broadcasted_iota(jnp.int32, (shells, LANES), 0)
    radius = inner_radius + step_r * ((r * shells + shell).astype(f32) + 0.5)
    order = lax.broadcasted_iota(jnp.int32, (shells, LANES), 1) % MPAD
    ups, downs, powers, degrees = [], [], [], []
    for q in range(KD):
        degree = (order + (g * KD + q)).astype(f32)
        grow = jnp.exp(degree * log_radius)
        weighted = (radius * radius * step_r) * total[q]
        up = grow * weighted
        down = weighted / (radius * grow)
        for s in (1, 2, 4):
            up = up + jnp.where(shell >= s, pltpu.roll(up, s, 0), 0.0)
            down = down + jnp.where(shell >= s, pltpu.roll(down, s, 0), 0.0)
        totals[0, q : q + 1, :] = up[shells - 1 : shells]
        totals[1, q : q + 1, :] = down[shells - 1 : shells]
        ups.append(up)
        downs.append(down)
        powers.append(grow)
        degrees.append(degree)

    pair = remote(totals, got_pair, c_send.at[0, 0], c_recv.at[0, 0], (r + 1 - 2 * (r % 2), a))
    pair.start()

    def hop_up(d):
        return remote(
            chain_up.at[d - 1], chain_up.at[d], c_send.at[0, d], c_recv.at[0, d], (r + 2, a)
        )

    def hop_down(d):
        return remote(
            chain_down.at[d - 1], chain_down.at[d], c_send.at[1, d], c_recv.at[1, d], (r - 2, a)
        )

    def start_hop(d):
        when(r + 2 < n_rad, hop_up(d).start)
        when(r - 2 >= 0, hop_down(d).start)

    def end_hop(d):
        when(r - 2 >= 0, hop_up(d).wait_recv)
        when(r + 2 < n_rad, hop_down(d).wait_recv)

    for c in range(2 * CUTS, 3 * CUTS):
        pass_on(c - 2 * CUTS)
        start_chunk(c)
    for c in range(CUTS, 2 * CUTS):
        pass_on(c)

    quarter = shells * tiles // 4
    lax.fori_loop(quarter, 2 * quarter, theta_flux, 0)
    pair.wait_recv()
    pair_up = got_pair[0]
    pair_down = got_pair[1]
    chain_up[0] = totals[0] + pair_up
    chain_down[0] = totals[1] + pair_down
    start_hop(1)
    lax.fori_loop(2 * quarter, 3 * quarter, theta_flux, 0)
    end_hop(1)
    start_hop(2)
    lax.fori_loop(3 * quarter, 4 * quarter, theta_flux, 0)
    end_hop(2)
    start_hop(3)
    below = jnp.where(odd, pair_up, 0.0)
    above = jnp.where(even, pair_down, 0.0)
    end_hop(3)
    for d in range(1, n_rad // 2):
        below = below + chain_up[d]
        above = above + chain_down[d]
    inverse_radius = 1.0 / radius
    for q in range(KD):
        inner = below[q : q + 1] + ups[q]
        outer = above[q : q + 1] + (downs[q][shells - 1 : shells] - downs[q])
        degree = degrees[q]
        norm = (-4.0 * math.pi) / (2.0 * degree + 1.0)
        inner_term = inner * inverse_radius / powers[q]
        outer_term = powers[q] * outer
        coef[g, 0, q] = norm * (inner_term + outer_term)
        coef[g, 1, q] = (
            norm * (degree * outer_term - (degree + 1.0) * inner_term) * inverse_radius
        )

    def exchange_d(d):
        return remote(coef.at[g], coef.at[g], d_send.at[d], d_recv.at[d], peer(d))

    for d in range(1, GROUPS):
        exchange_d(d).start()
    for c in range(2 * CUTS, 3 * CUTS):
        pass_on(c)
        start_chunk(c + CUTS)
    for d in range(1, GROUPS):
        exchange_d(d).wait_recv()

    slope_row = degree_ref[2 * NK : 2 * NK + 1, :]
    theta_scale = 1.0 / (2.0 * step_t)
    for i in range(0, shells, 2):

        def synthesize(h, carry):
            sums = list(carry)
            for q in range(KD):
                k = h * KD + q
                full = leg[k]
                value = full[PADR : PADR + rows]
                change = pltpu.roll(full, span - 1, 0) - pltpu.roll(full, 1, 0)
                change = change[PADR : PADR + rows]
                for p in range(2):
                    cp = coef[h, 0, q, i + p : i + p + 1, :]
                    cs = coef[h, 1, q, i + p : i + p + 1, :]
                    sums[3 * p] = sums[3 * p] + value * cp
                    sums[3 * p + 1] = sums[3 * p + 1] + value * cs
                    sums[3 * p + 2] = sums[3 * p + 2] + change * cp
            return tuple(sums)

        zero = jnp.zeros((rows, LANES), f32)
        sums = lax.fori_loop(0, (LMAX + KD) // KD, synthesize, (zero,) * 6)
        for p in range(2):
            base, slope, change = sums[3 * p : 3 * p + 3]
            at = (i + p) * 4 * rows
            table[at : at + rows, :] = base
            table[at + rows : at + 2 * rows, :] = slope
            table[at + 2 * rows : at + 3 * rows, :] = change * theta_scale
            table[at + 3 * rows : at + 4 * rows, :] = pltpu.roll(base, MPAD, 1) * slope_row

    load_back.wait()

    def sources(i, carry):
        at = pl.multiple_of(i * 4 * rows, 4 * rows)
        high, low = split(table[pl.ds(at, 4 * rows), :])
        fields[...] = dot(jnp.concatenate([high, low, high], axis=1), back_ref[...])
        pot[i] = fields[0:rows, :]
        cell_radius = inner_radius + step_r * ((r * shells + i).astype(f32) + 0.5)
        for c in range(chunks):
            at = c * ROWS
            inside = pl.ds(PADR + at, ROWS)
            sine = jnp.broadcast_to(rowtab[inside, 1:2], (ROWS, cols)) * cell_radius
            cosine = jnp.broadcast_to(rowtab[inside, 0:1], (ROWS, cols)) * cell_radius
            density = ext[0, i, inside, :]
            mom_r = ext[1, i, inside, :]
            mom_t = ext[2, i, inside, :]
            mom_p = ext[3, i, inside, :]
            inverse = 1.0 / density
            vel_t = mom_t * inverse
            vel_p = mom_p * inverse
            pull = grav_const * density
            slope = fields[rows + at : rows + at + ROWS, :]
            grad_t = fields[2 * rows + at : 2 * rows + at + ROWS, :]
            grad_p = fields[3 * rows + at : 3 * rows + at + ROWS, :]
            twist = mom_p * vel_p
            source_r = sine * (
                (mom_t * vel_t + twist)
                + (2.0 * sound_sq) * density
                - (cell_radius * pull) * slope
            )
            source_t = cosine * (twist + sound_sq * density) - sine * (
                mom_r * vel_t + pull * grad_t
            )
            source_p = -(
                vel_p * (mom_r * sine + mom_t * cosine) + (cell_radius * pull) * grad_p
            )
            spot = pl.ds(at, ROWS)
            tend[1, i, spot, :] = tend[1, i, spot, :] + source_r
            tend[2, i, spot, :] = tend[2, i, spot, :] + source_t
            tend[3, i, spot, :] = tend[3, i, spot, :] + source_p
        return carry

    lax.fori_loop(0, shells, sources, 0)

    per = wide // LANES
    for chunk in range(parts):
        when(r > 0, rad_up[chunk].wait_recv)
        when(r + 1 < n_rad, rad_down[chunk].wait_recv)
        at = (chunk // CUTS) * ROWS
        spot = pl.ds(at, ROWS)
        first = (chunk % CUTS) * per

        def radial_flux(tile, carry):
            lanes = pl.ds(pl.multiple_of(tile * LANES, LANES), LANES)
            sine = jnp.broadcast_to(
                rowtab[PADR + at : PADR + at + ROWS, 1:2], (ROWS, LANES)
            ) * (section_step / step_r)

            def cell(c, s):
                if s < 0:
                    return lo[c, s + WIDTH, spot, lanes]
                if s >= shells:
                    return hi[c, s - shells, spot, lanes]
                return ext[c, s, pl.ds(PADR + at, ROWS), lanes]

            u = [[cell(c, s) for s in range(-WIDTH, shells + WIDTH)] for c in range(4)]
            last = None
            for f in range(shells + 1):
                place = r * shells + f
                face_radius = inner_radius + step_r * place.astype(f32)
                area = jnp.where(
                    (place > 0) & (place < n_rad * shells), face_radius * face_radius, 0.0
                )
                sums, jumps = [], []
                for c in range(4):
                    w = u[c][f : f + 6]
                    sums.append(37.0 * (w[2] + w[3]) - 8.0 * (w[1] + w[4]) + (w[0] + w[5]))
                    jumps.append(w[3] - w[2])
                face = [value * area for value in flux(sums, jumps, 1)]
                if f > 0:
                    for c in range(4):
                        tend[c, f - 1, spot, lanes] = (
                            section_step * tend[c, f - 1, spot, lanes]
                            - (face[c] - last[c]) * sine
                        )
                last = face
            return carry

        lax.fori_loop(first, first + per, radial_flux, 0)

    for c in range(QUARTERS):
        when(a + 1 < n_ang, rows_up[c].wait_send)
        when(a > 0, rows_down[c].wait_send)
        if c < QUARTERS - 1:
            when((c < n_up_hand) | (c < n_down_hand), hand_up[c].wait_send)
    for c in range(parts):
        when(r + 1 < n_rad, rad_up[c].wait_send)
        when(r > 0, rad_down[c].wait_send)
        if c < n_far:
            when((c < n_up_pass) | (c < n_down_pass), pass_up[c].wait_send)
    for d in range(1, GROUPS):
        exchange_a(d).wait_send()
        exchange_d(d).wait_send()
    exchange_b.wait_send()
    pair.wait_send()
    for d in range(1, n_rad // 2):
        when(r + 2 < n_rad, hop_up(d).wait_send)
        when(r - 2 >= 0, hop_down(d).wait_send)


def store(tend, pot, inc_ref, pot_ref, sem):
    copies = [
        pltpu.make_async_copy(tend.at[c], inc_ref.at[c], sem.at[c]) for c in range(tend.shape[0])
    ]
    copies.append(pltpu.make_async_copy(pot, pot_ref, sem.at[len(copies)]))
    for copy in copies:
        copy.start()
    for copy in copies:
        copy.wait()


def solution(mesh):
    n_rad = mesh.shape["rad"]
    n_ang = mesh.shape["ang"]

    def body(state):
        _, shells, rows, cols = state.shape
        high, low, back, slope = phi_tables(cols)
        operands = (
            state,
            jnp.asarray(high),
            jnp.asarray(low),
            jnp.asarray(back),
            jnp.asarray(row_tables(n_ang, rows)),
            jnp.asarray(degree_tables(slope)),
            jnp.asarray(log_radii(n_rad, shells)),
        )
        span = rows + 2 * PADR
        parts = (rows // ROWS) * CUTS
        inside = pl.BlockSpec(memory_space=pltpu.VMEM)
        dma = pltpu.SemaphoreType.DMA
        increment, potential = pl.pallas_call(
            functools.partial(kernel, n_rad, n_ang, shells, rows, cols),
            out_shape=(
                pltpu.VMEM(state.shape, f32),
                pltpu.VMEM(state.shape[1:], f32),
            ),
            in_specs=[pl.BlockSpec(memory_space=pltpu.HBM)] * 7,
            out_specs=(inside, inside),
            scratch_shapes=[
                pltpu.VMEM((4, shells, span, cols), f32),
                pltpu.VMEM((4, WIDTH, rows, cols), f32),
                pltpu.VMEM((4, WIDTH, rows, cols), f32),
                pltpu.VMEM((parts - CUTS, 4, WIDTH, ROWS, cols // CUTS), f32),
                pltpu.VMEM((QUARTERS - 1, 4, shells // QUARTERS, WIDTH, cols), f32),
                pltpu.VMEM((4 * rows, cols), f32),
                pltpu.VMEM((shells * 4 * rows, LANES), f32),
                pltpu.VMEM((shells * rows, LANES), f32),
                pltpu.VMEM((cols, LANES), bf16),
                pltpu.VMEM((cols, LANES), bf16),
                pltpu.VMEM((3 * LANES, cols), bf16),
                pltpu.VMEM((span, LANES), f32),
                pltpu.VMEM((2 * NK + 8, LANES), f32),
                pltpu.VMEM((shells, LANES), f32),
                pltpu.VMEM((NK, span, LANES), f32),
                pltpu.VMEM((GROUPS, KD, shells, LANES), f32),
                pltpu.VMEM((GROUPS, KD, shells, LANES), f32),
                pltpu.VMEM((KD, shells, LANES), f32),
                pltpu.VMEM((KD, shells, LANES), f32),
                pltpu.VMEM((2, 8, LANES), f32),
                pltpu.VMEM((2, 8, LANES), f32),
                pltpu.VMEM((n_rad // 2, 8, LANES), f32),
                pltpu.VMEM((n_rad // 2, 8, LANES), f32),
                pltpu.VMEM((GROUPS, 2, KD, shells, LANES), f32),
                pltpu.SemaphoreType.REGULAR((3,)),
                dma((8,)),
                dma((2, QUARTERS)),
                dma((2, QUARTERS)),
                dma((QUARTERS - 1,)),
                dma((QUARTERS - 1,)),
                dma((2, parts)),
                dma((2, parts)),
                dma((parts - CUTS,)),
                dma((parts - CUTS,)),
                dma((GROUPS,)),
                dma((GROUPS,)),
                dma((1,)),
                dma((1,)),
                dma((2, n_rad // 2)),
                dma((2, n_rad // 2)),
                dma((GROUPS,)),
                dma((GROUPS,)),
            ],
            compiler_params=pltpu.CompilerParams(
                collective_id=0, has_side_effects=True, vmem_limit_bytes=61_700_000
            ),
        )(*operands)
        outside = pl.BlockSpec(memory_space=pltpu.HBM)
        return pl.pallas_call(
            store,
            out_shape=(
                jax.ShapeDtypeStruct(state.shape, f32),
                jax.ShapeDtypeStruct(state.shape[1:], f32),
            ),
            in_specs=(inside, inside),
            out_specs=(outside, outside),
            scratch_shapes=[dma((5,))],
            compiler_params=pltpu.CompilerParams(vmem_limit_bytes=1 << 20),
        )(increment, potential)

    return jax.shard_map(
        body,
        mesh=mesh,
        in_specs=(P(None, "rad", "ang", None),),
        out_specs=(P(None, "rad", "ang", None), P("rad", "ang", None)),
        check_vma=False,
    )
```

```python
import functools
import math

import jax
import jax.numpy as jnp
import numpy as np
from jax import lax
from jax.experimental import pallas as pl
from jax.experimental.pallas import tpu as pltpu
from jax.sharding import PartitionSpec as P

LMAX = 48
MPAD = 64
LANES = 128
NK = 56
GROUPS = 8
KD = 7
PADR = 8
WIDTH = 3
ROWS = 8
QUARTERS = 4
CUTS = 2

sound_speed = 0.5
sound_sq = 0.25
grav_const = 100.0
section_step = 0.001
inner_radius = 1.0
radial_span = 0.1
MESH = pl.DeviceIdType.MESH
f32 = jnp.float32
bf16 = jnp.bfloat16


def split_np(table):
    high = table.astype(bf16)
    low = (table - high.astype(np.float64)).astype(bf16)
    return high, low


def phi_tables(count):
    order = np.arange(MPAD, dtype=np.float64)
    norm = np.where(order > 0.5, math.sqrt(2.0), 1.0)
    phase = (2.0 * math.pi / count) * (np.outer(np.arange(count), np.arange(MPAD)) % count)
    table = np.concatenate([np.cos(phase) * norm, np.sin(phase) * norm], axis=1)
    high, low = split_np(table)
    back = np.concatenate([high.T, high.T, low.T], axis=0)
    step = 2.0 * math.pi / count
    slope = np.sin(order * step) / step
    return high, low, back, np.concatenate([slope, -slope])


def row_tables(blocks, rows):
    total = blocks * rows
    step_t = math.pi / total
    row = np.arange(blocks)[:, None] * rows + np.arange(rows + 2 * PADR)[None, :] - PADR
    theta = step_t * (row + 0.5)
    face = np.where((row > 0) & (row < total), np.sin(step_t * row), 0.0)
    table = np.zeros((blocks, rows + 2 * PADR, LANES))
    table[:, :, 0] = np.cos(theta)
    table[:, :, 1] = np.sin(theta)
    table[:, :, 2] = face
    return table.astype(np.float32)


def degree_tables(slope):
    m = np.arange(LANES) % MPAD
    k = np.arange(NK)[:, None]
    l = (m + k).astype(np.float64)
    alpha = np.zeros((NK, LANES))
    beta = np.zeros((NK, LANES))
    norm = np.full(LANES, 1.0 / math.sqrt(4.0 * math.pi))
    for q in range(1, MPAD):
        norm = np.where(m >= q, norm * math.sqrt((2.0 * q + 1.0) / (2.0 * q)), norm)
    alpha[0] = norm
    alpha[1:] = np.sqrt((4.0 * l[1:] ** 2 - 1.0) / (l[1:] ** 2 - m**2))
    beta[2:] = np.sqrt(((l[2:] - 1.0) ** 2 - m**2) / (4.0 * (l[2:] - 1.0) ** 2 - 1.0))
    alpha = np.where(l <= LMAX, alpha, 0.0)
    extra = np.zeros((8, LANES))
    extra[0] = slope
    return np.concatenate([alpha, beta, extra]).astype(np.float32)


def log_radii(blocks, shells):
    radius = inner_radius + radial_span / (blocks * shells) * (np.arange(blocks * shells) + 0.5)
    table = np.log(radius).reshape(blocks, shells, 1)
    return np.broadcast_to(table, (blocks, shells, LANES)).astype(np.float32)


def split(value):
    high = value.astype(bf16)
    return high, (value - high.astype(f32)).astype(bf16)


def dot(a, b):
    return jnp.dot(a, b, preferred_element_type=f32)


def flux(sums, jumps, component):
    inverse = 1.0 / sums[0]
    speed = sums[component] * inverse
    scaled = speed * (1.0 / 60.0)
    wave = 0.5 * (sound_speed + jnp.abs(speed))
    out = [s * scaled - wave * j for s, j in zip(sums, jumps)]
    out[component] = out[component] + (sound_sq / 60.0) * sums[0]
    return out


def radial_flux(r, n_rad, shells, at, start, out_at, ext, lo, hi, rowtab, tend, out, tile, carry):
    step_r = radial_span / (n_rad * shells)
    spot = pl.ds(at, ROWS)
    lanes = pl.ds(pl.multiple_of(tile * LANES, LANES), LANES)
    out_spot = pl.ds(out_at, ROWS)
    out_lanes = pl.ds(pl.multiple_of((tile - start) * LANES, LANES), LANES)
    sine = jnp.broadcast_to(rowtab[PADR + at : PADR + at + ROWS, 1:2], (ROWS, LANES)) * (
        section_step / step_r
    )

    def cell(c, s):
        if s < 0:
            return lo[c, s + WIDTH, spot, lanes]
        if s >= shells:
            return hi[c, s - shells, spot, lanes]
        return ext[c, s, pl.ds(PADR + at, ROWS), lanes]

    u = [[cell(c, s) for s in range(-WIDTH, shells + WIDTH)] for c in range(4)]
    last = None
    for f in range(shells + 1):
        place = r * shells + f
        face_radius = inner_radius + step_r * place.astype(f32)
        area = jnp.where((place > 0) & (place < n_rad * shells), face_radius * face_radius, 0.0)
        sums, jumps = [], []
        for c in range(4):
            w = u[c][f : f + 6]
            sums.append(37.0 * (w[2] + w[3]) - 8.0 * (w[1] + w[4]) + (w[0] + w[5]))
            jumps.append(w[3] - w[2])
        face = [value * area for value in flux(sums, jumps, 1)]
        if f > 0:
            for c in range(4):
                out[c, f - 1, out_spot, out_lanes] = (
                    section_step * tend[c, f - 1, spot, lanes] - (face[c] - last[c]) * sine
                )
        last = face
    return carry


def kernel(
    n_rad,
    n_ang,
    shells,
    rows,
    cols,
    x_ref,
    fwd_high_hbm,
    fwd_low_hbm,
    back_hbm,
    row_hbm,
    degree_hbm,
    log_hbm,
    tend,
    pot,
    ext,
    lo,
    hi,
    rowtab,
    lead,
    relay,
    row_relay,
    fields,
    table,
    spec,
    fwd_high_ref,
    fwd_low_ref,
    back_ref,
    degree_ref,
    log_ref,
    leg,
    partial,
    got_a,
    mine,
    got_b,
    totals,
    got_pair,
    chain_up,
    chain_down,
    coef,
    rounds,
    local_sem,
    ang_send,
    ang_recv,
    skip_recv,
    hand_send,
    rad_send,
    rad_recv,
    far_recv,
    pass_send,
    a_send,
    a_recv,
    b_send,
    b_recv,
    c_send,
    c_recv,
    d_send,
    d_recv,
):
    r = lax.axis_index("rad")
    a = lax.axis_index("ang")
    y, x_hi, core = a // 4, (a // 2) % 2, a % 2
    g = y * 2 + core
    chunks = rows // ROWS
    parts = chunks * CUTS
    wide = cols // CUTS
    n_far = parts - CUTS
    span = rows + 2 * PADR
    own = pl.ds(PADR, rows)
    step_r = radial_span / (n_rad * shells)
    step_t = math.pi / (n_ang * rows)
    step_p = 2.0 * math.pi / cols

    def peer(d):
        q = (g + d) % GROUPS
        return (r, (q // 2) * 4 + x_hi * 2 + q % 2)

    partner = (r, y * 4 + (1 - x_hi) * 2 + core)

    def when(cond, run):
        @pl.when(cond)
        def _():
            run()

    def remote(src, dst, send, recv, dev):
        return pltpu.make_async_remote_copy(
            src_ref=src,
            dst_ref=dst,
            send_sem=send,
            recv_sem=recv,
            device_id=dev,
            device_id_type=MESH,
        )

    load_density = pltpu.make_async_copy(x_ref.at[0], ext.at[0, :, own], local_sem.at[0])
    load_rest = pltpu.make_async_copy(
        x_ref.at[1:4], ext.at[1:4, :, own], local_sem.at[1]
    )
    load_rows = pltpu.make_async_copy(row_hbm.at[a], rowtab, local_sem.at[2])
    load_degree = pltpu.make_async_copy(degree_hbm, degree_ref, local_sem.at[3])
    load_high = pltpu.make_async_copy(fwd_high_hbm, fwd_high_ref, local_sem.at[4])
    load_low = pltpu.make_async_copy(fwd_low_hbm, fwd_low_ref, local_sem.at[5])
    load_log = pltpu.make_async_copy(log_hbm.at[r], log_ref, local_sem.at[6])
    load_back = pltpu.make_async_copy(back_hbm, back_ref, local_sem.at[7])
    barrier = pltpu.get_barrier_semaphore()
    first = a % 4 == 0
    last = a % 4 == 3
    odd = r % 2 == 1
    even = r % 2 == 0
    x = x_hi * 2 + r % 2

    def along_x(step):
        to = (x + step) % 4
        return ((r // 2) * 2 + to % 2, y * 4 + (to // 2) * 2 + core)

    near = [
        (x < 3, along_x(1)),
        (x > 0, along_x(3)),
        (r + 2 < n_rad, (r + 2, a)),
        (r - 2 >= 0, (r - 2, a)),
        (a + 4 < n_ang, (r, a + 4)),
        (a - 4 >= 0, (r, a - 4)),
        (None, (r, a + 1 - 2 * core)),
    ]
    n_near = 1
    for cond, _ in near:
        if cond is not None:
            n_near = n_near + jnp.where(cond, 1, 0)

    def greet(sem):
        for cond, dev in near:
            signal = functools.partial(
                pl.semaphore_signal, sem, inc=1, device_id=dev, device_id_type=MESH
            )
            if cond is None:
                signal()
            else:
                when(cond, signal)

    greet(barrier)
    edge = pl.ds(jnp.where(even, shells - WIDTH, 0), WIDTH)
    load_lead = pltpu.make_async_copy(
        x_ref.at[:, edge, 0:ROWS, 0:wide], lead, local_sem.at[8]
    )
    load_lead.start()
    for load in (load_rows, load_degree, load_density, load_high, load_low):
        load.start()
    for load in (load_rest, load_log, load_back):
        load.start()
    pl.semaphore_wait(barrier, n_near)

    deep = shells // QUARTERS
    rows_up, rows_down, skip_up, skip_down, hand_up, hand_down = [], [], [], [], [], []
    for c in range(QUARTERS):
        part = pl.ds(c * deep, deep)
        high = x_ref.at[:, part, rows - WIDTH : rows]
        low = x_ref.at[:, part, 0:WIDTH]
        under = ext.at[:, part, PADR - WIDTH : PADR]
        over = ext.at[:, part, PADR + rows : PADR + rows + WIDTH]
        up_sems = ang_send.at[0, c], ang_recv.at[0, c]
        down_sems = ang_send.at[1, c], ang_recv.at[1, c]
        rows_up.append(remote(high, under, *up_sems, (r, a + 1)))
        rows_down.append(remote(low, over, *down_sems, (r, a - 1)))
        if c < QUARTERS - 1:
            spot = row_relay.at[c]
            skip_up.append(remote(high, spot, up_sems[0], skip_recv.at[c], (r, a + 4)))
            skip_down.append(remote(low, spot, down_sems[0], skip_recv.at[c], (r, a - 4)))
            hand_up.append(remote(spot, under, hand_send.at[c], up_sems[1], (r, a - 3)))
            hand_down.append(remote(spot, over, hand_send.at[c], down_sems[1], (r, a + 3)))
    n_up_skip = jnp.where(last & (a + 1 < n_ang), y + 1, 0)
    n_down_skip = jnp.where(first & (a > 0), QUARTERS - y, 0)
    n_up_hand = jnp.where(last, y, 0)
    n_down_hand = jnp.where(first, QUARTERS - 1 - y, 0)

    def start_rows(c):
        when((a + 1 < n_ang) & (c >= n_up_skip), rows_up[c].start)
        when((a > 0) & (c >= n_down_skip), rows_down[c].start)

    def start_skip(c):
        when(c < n_up_skip, skip_up[c].start)
        when(c < n_down_skip, skip_down[c].start)

    def hand_on(c):
        @pl.when(c < n_up_hand)
        def _():
            skip_up[c].wait_recv()
            hand_up[c].start()

        @pl.when(c < n_down_hand)
        def _():
            skip_down[c].wait_recv()
            hand_down[c].start()

    rad_up, rad_down, far_up, far_down, pass_up, pass_down = [], [], [], [], [], []
    for c in range(parts):
        part = pl.ds((c // CUTS) * ROWS, ROWS)
        band = pl.ds((c % CUTS) * wide, wide)
        above = x_ref.at[:, shells - WIDTH : shells, part, band]
        below = x_ref.at[:, 0:WIDTH, part, band]
        lo_part, hi_part = lo.at[:, :, part, band], hi.at[:, :, part, band]
        up_sems = rad_send.at[0, c], rad_recv.at[0, c]
        down_sems = rad_send.at[1, c], rad_recv.at[1, c]
        rad_up.append(remote(above, lo_part, *up_sems, (r + 1, a)))
        rad_down.append(remote(below, hi_part, *down_sems, (r - 1, a)))
        if c < n_far:
            spot = relay.at[c]
            far_up.append(remote(above, spot, up_sems[0], far_recv.at[c], (r + 2, a)))
            far_down.append(remote(below, spot, down_sems[0], far_recv.at[c], (r - 2, a)))
            pass_up.append(remote(spot, lo_part, pass_send.at[c], up_sems[1], (r - 1, a)))
            pass_down.append(remote(spot, hi_part, pass_send.at[c], down_sems[1], (r + 1, a)))
    n_up_far = jnp.where(odd & (r + 2 < n_rad), CUTS * ((r + 1) // 2), 0)
    n_down_far = jnp.where(even & (r > 0), parts - CUTS * (r // 2), 0)
    n_up_pass = jnp.where(odd & (r > 1), CUTS * ((r - 1) // 2), 0)
    n_down_pass = jnp.where(even & (r + 2 < n_rad), n_far - CUTS * (r // 2), 0)

    def start_far(c):
        when(c < n_up_far, far_up[c].start)
        when(c < n_down_far, far_down[c].start)

    lead_to = pl.ds(0, ROWS), pl.ds(0, wide)
    lead_up = remote(
        lead, lo.at[:, :, *lead_to], rad_send.at[0, 0], rad_recv.at[0, 0], (r + 1, a)
    )
    lead_down = remote(
        lead, hi.at[:, :, *lead_to], rad_send.at[1, 0], rad_recv.at[1, 0], (r - 1, a)
    )

    def start_pair(c):
        when(even, rad_up[c].start)
        when(odd, rad_down[c].start)

    def start_diagonal(c):
        when(odd & (r + 1 < n_rad) & (c >= n_up_far), rad_up[c].start)
        when(even & (r > 0) & (c >= n_down_far), rad_down[c].start)

    def start_chunk(c):
        start_pair(c)
        start_diagonal(c)

    def pass_on(c):
        @pl.when(c < n_up_pass)
        def _():
            far_up[c].wait_recv()
            pass_up[c].start()

        @pl.when(c < n_down_pass)
        def _():
            far_down[c].wait_recv()
            pass_down[c].start()

    load_lead.wait()
    when(even, lead_up.start)
    when(odd, lead_down.start)
    greet(rounds.at[0])
    for c in range(n_far):
        start_far(c)
    for c in range(QUARTERS - 1):
        start_skip(c)
    for c in range(1, CUTS):
        start_pair(c)
    pl.semaphore_wait(rounds.at[0], n_near)
    greet(rounds.at[1])
    for c in range(CUTS):
        start_diagonal(c)
    pl.semaphore_wait(rounds.at[1], n_near)
    greet(rounds.at[2])
    pl.semaphore_wait(rounds.at[2], n_near)
    for c in range(QUARTERS):
        start_rows(c)

    @pl.when(a == 0)
    def _():
        ext[:, :, 0:PADR, :] = jnp.zeros((4, shells, PADR, cols), f32)

    @pl.when(a == n_ang - 1)
    def _():
        ext[:, :, PADR + rows : span, :] = jnp.zeros((4, shells, PADR, cols), f32)

    @pl.when(r == 0)
    def _():
        lo[...] = jnp.zeros_like(lo)

    @pl.when(r == n_rad - 1)
    def _():
        hi[...] = jnp.zeros_like(hi)

    @pl.when(r < 2)
    def _():
        chain_up[1:] = jnp.zeros((n_rad // 2 - 1, 8, LANES), f32)

    @pl.when(r + 2 >= n_rad)
    def _():
        chain_down[1:] = jnp.zeros((n_rad // 2 - 1, 8, LANES), f32)

    load_rows.wait()
    load_degree.wait()
    cosine = jnp.broadcast_to(rowtab[:, 0:1], (span, LANES))
    sine = jnp.broadcast_to(rowtab[:, 1:2], (span, LANES))
    order = lax.broadcasted_iota(jnp.int32, (span, LANES), 1) % MPAD
    power = jnp.full((span, LANES), 1.0, f32)
    square = sine
    for bit in range(6):
        power = jnp.where((order // (1 << bit)) % 2 == 1, power * square, power)
        square = square * square
    level = power * degree_ref[0:1, :]
    leg[0] = level

    def next_level(k, carry):
        last, before = carry
        alpha = degree_ref[pl.ds(k, 1), :]
        beta = degree_ref[pl.ds(NK + k, 1), :]
        new = alpha * (cosine * last - beta * before)
        leg[k] = new
        return (new, last)

    lax.fori_loop(1, NK, next_level, (level, jnp.zeros_like(level)))

    for c in range(QUARTERS - 1):
        hand_on(c)

    load_density.wait()
    load_high.wait()
    load_low.wait()
    weight = sine[PADR : PADR + rows] * (step_t * step_p)
    half = shells // 2
    for h in range(2):
        cells = ext[0, h * half : (h + 1) * half, PADR : PADR + rows, :]
        high, low = split(cells.reshape(half * rows, cols))
        sums = dot(high, fwd_high_ref[...]) + (
            dot(low, fwd_high_ref[...]) + dot(high, fwd_low_ref[...])
        )
        for q in range(half):
            spec[pl.ds((h * half + q) * rows, rows), :] = (
                sums[q * rows : (q + 1) * rows] * weight
            )
    spectra = [spec[pl.ds(j, shells, stride=rows), :] for j in range(rows)]

    def moment(k, carry):
        parts = [jnp.zeros((shells, LANES), f32) for _ in range(4)]
        for j in range(rows):
            parts[j % 4] = parts[j % 4] + spectra[j] * leg[k, PADR + j : PADR + j + 1, :]
        partial[k // KD, k % KD] = (parts[0] + parts[1]) + (parts[2] + parts[3])
        return carry

    lax.fori_loop(0, NK, moment, 0)

    def exchange_a(d):
        return remote(
            partial.at[(g + d) % GROUPS], got_a.at[d], a_send.at[d], a_recv.at[d], peer(d)
        )

    for d in range(1, GROUPS):
        exchange_a(d).start()

    load_rest.wait()

    def phi_flux(index, carry):
        i = index // chunks
        at = pl.multiple_of((index % chunks) * ROWS, ROWS)
        cell_radius = inner_radius + step_r * ((r * shells + i).astype(f32) + 0.5)
        sums, jumps = [], []
        for c in range(4):
            u = ext[c, i, pl.ds(PADR + at, ROWS), :]
            left = pltpu.roll(u, 1, 1)
            near = u + left
            mid = pltpu.roll(u, cols - 1, 1) + pltpu.roll(u, 2, 1)
            far = pltpu.roll(u, cols - 2, 1) + pltpu.roll(u, 3, 1)
            sums.append(37.0 * near - 8.0 * mid + far)
            jumps.append(u - left)
        for c, face in enumerate(flux(sums, jumps, 3)):
            tend[c, i, pl.ds(at, ROWS), :] = (face - pltpu.roll(face, cols - 1, 1)) * (
                cell_radius / step_p
            )
        return carry

    lax.fori_loop(0, shells * chunks // 2, phi_flux, 0)

    for d in range(1, GROUPS):
        exchange_a(d).wait_recv()
    total = partial[g]
    for d in range(1, GROUPS):
        total = total + got_a[d]
    mine[...] = total
    exchange_b = remote(mine, got_b, b_send.at[0], b_recv.at[0], partner)
    exchange_b.start()
    for c in range(CUTS, 2 * CUTS):
        start_chunk(c)

    lax.fori_loop(shells * chunks // 2, shells * chunks, phi_flux, 0)

    for c in range(QUARTERS):
        when(a > 0, rows_up[c].wait_recv)
        when(a + 1 < n_ang, rows_down[c].wait_recv)
    tiles = cols // LANES

    def theta_flux(index, carry):
        i = index // tiles
        lanes = pl.ds(pl.multiple_of((index % tiles) * LANES, LANES), LANES)
        cell_radius = inner_radius + step_r * ((r * shells + i).astype(f32) + 0.5)
        area = jnp.broadcast_to(rowtab[:, 2:3], (span, LANES)) * (cell_radius / step_t)
        sums, jumps = [], []
        for c in range(4):
            u = ext[c, i, :, lanes]
            left = pltpu.roll(u, 1, 0)
            near = u + left
            mid = pltpu.roll(u, span - 1, 0) + pltpu.roll(u, 2, 0)
            far = pltpu.roll(u, span - 2, 0) + pltpu.roll(u, 3, 0)
            sums.append(37.0 * near - 8.0 * mid + far)
            jumps.append(u - left)
        for c, face in enumerate(flux(sums, jumps, 2)):
            face = face * area
            change = face - pltpu.roll(face, span - 1, 0)
            tend[c, i, :, lanes] = tend[c, i, :, lanes] + change[PADR : PADR + rows]
        return carry

    lax.fori_loop(0, shells * tiles // 4, theta_flux, 0)

    exchange_b.wait_recv()
    total = mine[...] + got_b[...]
    load_log.wait()
    log_radius = log_ref[...]
    shell = lax.broadcasted_iota(jnp.int32, (shells, LANES), 0)
    radius = inner_radius + step_r * ((r * shells + shell).astype(f32) + 0.5)
    order = lax.broadcasted_iota(jnp.int32, (shells, LANES), 1) % MPAD
    ups, downs, powers, degrees = [], [], [], []
    for q in range(KD):
        degree = (order + (g * KD + q)).astype(f32)
        grow = jnp.exp(degree * log_radius)
        weighted = (radius * radius * step_r) * total[q]
        up = grow * weighted
        down = weighted / (radius * grow)
        for s in (1, 2, 4):
            up = up + jnp.where(shell >= s, pltpu.roll(up, s, 0), 0.0)
            down = down + jnp.where(shell >= s, pltpu.roll(down, s, 0), 0.0)
        totals[0, q : q + 1, :] = up[shells - 1 : shells]
        totals[1, q : q + 1, :] = down[shells - 1 : shells]
        ups.append(up)
        downs.append(down)
        powers.append(grow)
        degrees.append(degree)

    pair = remote(totals, got_pair, c_send.at[0, 0], c_recv.at[0, 0], (r + 1 - 2 * (r % 2), a))
    pair.start()

    def hop_up(d):
        return remote(
            chain_up.at[d - 1], chain_up.at[d], c_send.at[0, d], c_recv.at[0, d], (r + 2, a)
        )

    def hop_down(d):
        return remote(
            chain_down.at[d - 1], chain_down.at[d], c_send.at[1, d], c_recv.at[1, d], (r - 2, a)
        )

    def start_hop(d):
        when(r + 2 < n_rad, hop_up(d).start)
        when(r - 2 >= 0, hop_down(d).start)

    def end_hop(d):
        when(r - 2 >= 0, hop_up(d).wait_recv)
        when(r + 2 < n_rad, hop_down(d).wait_recv)

    for c in range(2 * CUTS, 3 * CUTS):
        pass_on(c - 2 * CUTS)
        start_chunk(c)
    for c in range(CUTS, 2 * CUTS):
        pass_on(c)

    quarter = shells * tiles // 4
    lax.fori_loop(quarter, 2 * quarter, theta_flux, 0)
    pair.wait_recv()
    pair_up = got_pair[0]
    pair_down = got_pair[1]
    chain_up[0] = totals[0] + pair_up
    chain_down[0] = totals[1] + pair_down
    start_hop(1)
    lax.fori_loop(2 * quarter, 3 * quarter, theta_flux, 0)
    end_hop(1)
    start_hop(2)
    lax.fori_loop(3 * quarter, 4 * quarter, theta_flux, 0)
    end_hop(2)
    start_hop(3)
    below = jnp.where(odd, pair_up, 0.0)
    above = jnp.where(even, pair_down, 0.0)
    end_hop(3)
    for d in range(1, n_rad // 2):
        below = below + chain_up[d]
        above = above + chain_down[d]
    inverse_radius = 1.0 / radius
    for q in range(KD):
        inner = below[q : q + 1] + ups[q]
        outer = above[q : q + 1] + (downs[q][shells - 1 : shells] - downs[q])
        degree = degrees[q]
        norm = (-4.0 * math.pi) / (2.0 * degree + 1.0)
        inner_term = inner * inverse_radius / powers[q]
        outer_term = powers[q] * outer
        coef[g, 0, q] = norm * (inner_term + outer_term)
        coef[g, 1, q] = (
            norm * (degree * outer_term - (degree + 1.0) * inner_term) * inverse_radius
        )

    def exchange_d(d):
        return remote(coef.at[g], coef.at[g], d_send.at[d], d_recv.at[d], peer(d))

    for d in range(1, GROUPS):
        exchange_d(d).start()
    for c in range(2 * CUTS, 3 * CUTS):
        pass_on(c)
        start_chunk(c + CUTS)
    for d in range(1, GROUPS):
        exchange_d(d).wait_recv()

    slope_row = degree_ref[2 * NK : 2 * NK + 1, :]
    theta_scale = 1.0 / (2.0 * step_t)
    for i in range(0, shells, 2):

        def synthesize(h, carry):
            sums = list(carry)
            for q in range(KD):
                k = h * KD + q
                full = leg[k]
                value = full[PADR : PADR + rows]
                change = pltpu.roll(full, span - 1, 0) - pltpu.roll(full, 1, 0)
                change = change[PADR : PADR + rows]
                for p in range(2):
                    cp = coef[h, 0, q, i + p : i + p + 1, :]
                    cs = coef[h, 1, q, i + p : i + p + 1, :]
                    sums[3 * p] = sums[3 * p] + value * cp
                    sums[3 * p + 1] = sums[3 * p + 1] + value * cs
                    sums[3 * p + 2] = sums[3 * p + 2] + change * cp
            return tuple(sums)

        zero = jnp.zeros((rows, LANES), f32)
        sums = lax.fori_loop(0, (LMAX + KD) // KD, synthesize, (zero,) * 6)
        for p in range(2):
            base, slope, change = sums[3 * p : 3 * p + 3]
            at = (i + p) * 4 * rows
            table[at : at + rows, :] = base
            table[at + rows : at + 2 * rows, :] = slope
            table[at + 2 * rows : at + 3 * rows, :] = change * theta_scale
            table[at + 3 * rows : at + 4 * rows, :] = pltpu.roll(base, MPAD, 1) * slope_row

    load_back.wait()

    def sources(i, carry):
        at = pl.multiple_of(i * 4 * rows, 4 * rows)
        high, low = split(table[pl.ds(at, 4 * rows), :])
        fields[...] = dot(jnp.concatenate([high, low, high], axis=1), back_ref[...])
        pot[i] = fields[0:rows, :]
        cell_radius = inner_radius + step_r * ((r * shells + i).astype(f32) + 0.5)
        for c in range(chunks):
            at = c * ROWS
            inside = pl.ds(PADR + at, ROWS)
            sine = jnp.broadcast_to(rowtab[inside, 1:2], (ROWS, cols)) * cell_radius
            cosine = jnp.broadcast_to(rowtab[inside, 0:1], (ROWS, cols)) * cell_radius
            density = ext[0, i, inside, :]
            mom_r = ext[1, i, inside, :]
            mom_t = ext[2, i, inside, :]
            mom_p = ext[3, i, inside, :]
            inverse = 1.0 / density
            vel_t = mom_t * inverse
            vel_p = mom_p * inverse
            pull = grav_const * density
            slope = fields[rows + at : rows + at + ROWS, :]
            grad_t = fields[2 * rows + at : 2 * rows + at + ROWS, :]
            grad_p = fields[3 * rows + at : 3 * rows + at + ROWS, :]
            twist = mom_p * vel_p
            source_r = sine * (
                (mom_t * vel_t + twist)
                + (2.0 * sound_sq) * density
                - (cell_radius * pull) * slope
            )
            source_t = cosine * (twist + sound_sq * density) - sine * (
                mom_r * vel_t + pull * grad_t
            )
            source_p = -(
                vel_p * (mom_r * sine + mom_t * cosine) + (cell_radius * pull) * grad_p
            )
            spot = pl.ds(at, ROWS)
            tend[1, i, spot, :] = tend[1, i, spot, :] + source_r
            tend[2, i, spot, :] = tend[2, i, spot, :] + source_t
            tend[3, i, spot, :] = tend[3, i, spot, :] + source_p
        return carry

    lax.fori_loop(0, shells, sources, 0)

    per = wide // LANES
    for chunk in range(parts):
        when(r > 0, rad_up[chunk].wait_recv)
        when(r + 1 < n_rad, rad_down[chunk].wait_recv)
        if chunk < parts - 1:
            at = (chunk // CUTS) * ROWS
            first = (chunk % CUTS) * per
            radial_tile = functools.partial(
                radial_flux, r, n_rad, shells, at, 0, at, ext, lo, hi, rowtab, tend, tend
            )
            lax.fori_loop(first, first + per, radial_tile, 0)

    for c in range(QUARTERS):
        when(a + 1 < n_ang, rows_up[c].wait_send)
        when(a > 0, rows_down[c].wait_send)
        if c < QUARTERS - 1:
            when((c < n_up_hand) | (c < n_down_hand), hand_up[c].wait_send)
    for c in range(parts):
        when(r + 1 < n_rad, rad_up[c].wait_send)
        when(r > 0, rad_down[c].wait_send)
        if c < n_far:
            when((c < n_up_pass) | (c < n_down_pass), pass_up[c].wait_send)
    for d in range(1, GROUPS):
        exchange_a(d).wait_send()
        exchange_d(d).wait_send()
    exchange_b.wait_send()
    pair.wait_send()
    for d in range(1, n_rad // 2):
        when(r + 2 < n_rad, hop_up(d).wait_send)
        when(r - 2 >= 0, hop_down(d).wait_send)


def close(n_rad, tend, pot, ext, lo, hi, rowtab, inc_ref, pot_ref, final, sem):
    _, shells, rows, cols = tend.shape
    ahead = pl.ds(0, rows - ROWS)
    behind = pl.ds(rows - ROWS, ROWS)
    done = pl.ds(0, cols - cols // CUTS)
    rest = pl.ds(cols - cols // CUTS, cols // CUTS)
    copies = [
        pltpu.make_async_copy(tend.at[c, :, ahead], inc_ref.at[c, :, ahead], sem.at[c])
        for c in range(4)
    ]
    copies.append(
        pltpu.make_async_copy(
            tend.at[:, :, behind, done], inc_ref.at[:, :, behind, done], sem.at[4]
        )
    )
    copies.append(pltpu.make_async_copy(pot, pot_ref, sem.at[5]))
    for copy in copies:
        copy.start()
    r = lax.axis_index("rad")
    tiles = cols // LANES
    start = tiles - tiles // CUTS
    radial_tile = functools.partial(
        radial_flux, r, n_rad, shells, rows - ROWS, start, 0, ext, lo, hi, rowtab, tend, final
    )
    lax.fori_loop(start, tiles, radial_tile, 0)
    copies.append(
        pltpu.make_async_copy(final, inc_ref.at[:, :, behind, rest], sem.at[6])
    )
    copies[-1].start()
    for copy in copies:
        copy.wait()


def solution(mesh):
    n_rad = mesh.shape["rad"]
    n_ang = mesh.shape["ang"]

    def body(state):
        _, shells, rows, cols = state.shape
        high, low, back, slope = phi_tables(cols)
        operands = (
            state,
            jnp.asarray(high),
            jnp.asarray(low),
            jnp.asarray(back),
            jnp.asarray(row_tables(n_ang, rows)),
            jnp.asarray(degree_tables(slope)),
            jnp.asarray(log_radii(n_rad, shells)),
        )
        span = rows + 2 * PADR
        parts = (rows // ROWS) * CUTS
        inside = pl.BlockSpec(memory_space=pltpu.VMEM)
        dma = pltpu.SemaphoreType.DMA
        results = pl.pallas_call(
            functools.partial(kernel, n_rad, n_ang, shells, rows, cols),
            out_shape=(
                pltpu.VMEM(state.shape, f32),
                pltpu.VMEM(state.shape[1:], f32),
                pltpu.VMEM((4, shells, span, cols), f32),
                pltpu.VMEM((4, WIDTH, rows, cols), f32),
                pltpu.VMEM((4, WIDTH, rows, cols), f32),
                pltpu.VMEM((span, LANES), f32),
            ),
            in_specs=[pl.BlockSpec(memory_space=pltpu.HBM)] * 7,
            out_specs=(inside,) * 6,
            scratch_shapes=[
                pltpu.VMEM((4, WIDTH, ROWS, cols // CUTS), f32),
                pltpu.VMEM((parts - CUTS, 4, WIDTH, ROWS, cols // CUTS), f32),
                pltpu.VMEM((QUARTERS - 1, 4, shells // QUARTERS, WIDTH, cols), f32),
                pltpu.VMEM((4 * rows, cols), f32),
                pltpu.VMEM((shells * 4 * rows, LANES), f32),
                pltpu.VMEM((shells * rows, LANES), f32),
                pltpu.VMEM((cols, LANES), bf16),
                pltpu.VMEM((cols, LANES), bf16),
                pltpu.VMEM((3 * LANES, cols), bf16),
                pltpu.VMEM((2 * NK + 8, LANES), f32),
                pltpu.VMEM((shells, LANES), f32),
                pltpu.VMEM((NK, span, LANES), f32),
                pltpu.VMEM((GROUPS, KD, shells, LANES), f32),
                pltpu.VMEM((GROUPS, KD, shells, LANES), f32),
                pltpu.VMEM((KD, shells, LANES), f32),
                pltpu.VMEM((KD, shells, LANES), f32),
                pltpu.VMEM((2, 8, LANES), f32),
                pltpu.VMEM((2, 8, LANES), f32),
                pltpu.VMEM((n_rad // 2, 8, LANES), f32),
                pltpu.VMEM((n_rad // 2, 8, LANES), f32),
                pltpu.VMEM((GROUPS, 2, KD, shells, LANES), f32),
                pltpu.SemaphoreType.REGULAR((3,)),
                dma((9,)),
                dma((2, QUARTERS)),
                dma((2, QUARTERS)),
                dma((QUARTERS - 1,)),
                dma((QUARTERS - 1,)),
                dma((2, parts)),
                dma((2, parts)),
                dma((parts - CUTS,)),
                dma((parts - CUTS,)),
                dma((GROUPS,)),
                dma((GROUPS,)),
                dma((1,)),
                dma((1,)),
                dma((2, n_rad // 2)),
                dma((2, n_rad // 2)),
                dma((GROUPS,)),
                dma((GROUPS,)),
            ],
            compiler_params=pltpu.CompilerParams(
                collective_id=0, has_side_effects=True, vmem_limit_bytes=52_200_000
            ),
        )(*operands)
        outside = pl.BlockSpec(memory_space=pltpu.HBM)
        return pl.pallas_call(
            functools.partial(close, n_rad),
            out_shape=(
                jax.ShapeDtypeStruct(state.shape, f32),
                jax.ShapeDtypeStruct(state.shape[1:], f32),
            ),
            in_specs=(inside,) * 6,
            out_specs=(outside, outside),
            scratch_shapes=[
                pltpu.VMEM((4, shells, ROWS, cols // CUTS), f32),
                dma((7,)),
            ],
            compiler_params=pltpu.CompilerParams(vmem_limit_bytes=4 << 20),
        )(*results)

    return jax.shard_map(
        body,
        mesh=mesh,
        in_specs=(P(None, "rad", "ang", None),),
        out_specs=(P(None, "rad", "ang", None), P("rad", "ang", None)),
        check_vma=False,
    )
```

```python
import functools
import math

import jax
import jax.numpy as jnp
import numpy as np
from jax import lax
from jax.experimental import pallas as pl
from jax.experimental.pallas import tpu as pltpu
from jax.sharding import PartitionSpec as P

LMAX = 48
MPAD = 64
LANES = 128
NK = 56
GROUPS = 8
KD = 7
PADR = 8
WIDTH = 3
ROWS = 8
QUARTERS = 4
CUTS = 2

sound_speed = 0.5
sound_sq = 0.25
grav_const = 100.0
section_step = 0.001
inner_radius = 1.0
radial_span = 0.1
MESH = pl.DeviceIdType.MESH
f32 = jnp.float32
bf16 = jnp.bfloat16


def split_np(table):
    high = table.astype(bf16)
    low = (table - high.astype(np.float64)).astype(bf16)
    return high, low


def phi_tables(count):
    order = np.arange(MPAD, dtype=np.float64)
    norm = np.where(order > 0.5, math.sqrt(2.0), 1.0)
    phase = (2.0 * math.pi / count) * (np.outer(np.arange(count), np.arange(MPAD)) % count)
    table = np.concatenate([np.cos(phase) * norm, np.sin(phase) * norm], axis=1)
    high, low = split_np(table)
    back = np.concatenate([high.T, high.T, low.T], axis=0)
    step = 2.0 * math.pi / count
    slope = np.sin(order * step) / step
    return high, low, back, np.concatenate([slope, -slope])


def row_tables(blocks, rows):
    total = blocks * rows
    step_t = math.pi / total
    row = np.arange(blocks)[:, None] * rows + np.arange(rows + 2 * PADR)[None, :] - PADR
    theta = step_t * (row + 0.5)
    face = np.where((row > 0) & (row < total), np.sin(step_t * row), 0.0)
    table = np.zeros((blocks, rows + 2 * PADR, LANES))
    table[:, :, 0] = np.cos(theta)
    table[:, :, 1] = np.sin(theta)
    table[:, :, 2] = face
    return table.astype(np.float32)


def degree_tables(slope):
    m = np.arange(LANES) % MPAD
    k = np.arange(NK)[:, None]
    l = (m + k).astype(np.float64)
    alpha = np.zeros((NK, LANES))
    beta = np.zeros((NK, LANES))
    norm = np.full(LANES, 1.0 / math.sqrt(4.0 * math.pi))
    for q in range(1, MPAD):
        norm = np.where(m >= q, norm * math.sqrt((2.0 * q + 1.0) / (2.0 * q)), norm)
    alpha[0] = norm
    alpha[1:] = np.sqrt((4.0 * l[1:] ** 2 - 1.0) / (l[1:] ** 2 - m**2))
    beta[2:] = np.sqrt(((l[2:] - 1.0) ** 2 - m**2) / (4.0 * (l[2:] - 1.0) ** 2 - 1.0))
    alpha = np.where(l <= LMAX, alpha, 0.0)
    extra = np.zeros((8, LANES))
    extra[0] = slope
    return np.concatenate([alpha, beta, extra]).astype(np.float32)


def log_radii(blocks, shells):
    radius = inner_radius + radial_span / (blocks * shells) * (np.arange(blocks * shells) + 0.5)
    table = np.log(radius).reshape(blocks, shells, 1)
    return np.broadcast_to(table, (blocks, shells, LANES)).astype(np.float32)


def split(value):
    high = value.astype(bf16)
    return high, (value - high.astype(f32)).astype(bf16)


def dot(a, b):
    return jnp.dot(a, b, preferred_element_type=f32)


def flux(sums, jumps, component):
    inverse = 1.0 / sums[0]
    speed = sums[component] * inverse
    scaled = speed * (1.0 / 60.0)
    wave = 0.5 * (sound_speed + jnp.abs(speed))
    out = [s * scaled - wave * j for s, j in zip(sums, jumps)]
    out[component] = out[component] + (sound_sq / 60.0) * sums[0]
    return out


def radial_flux(r, n_rad, shells, at, start, out_at, ext, lo, hi, rowtab, tend, out, tile, carry):
    step_r = radial_span / (n_rad * shells)
    spot = pl.ds(at, ROWS)
    lanes = pl.ds(pl.multiple_of(tile * LANES, LANES), LANES)
    out_spot = pl.ds(out_at, ROWS)
    out_lanes = pl.ds(pl.multiple_of((tile - start) * LANES, LANES), LANES)
    sine = jnp.broadcast_to(rowtab[PADR + at : PADR + at + ROWS, 1:2], (ROWS, LANES)) * (
        section_step / step_r
    )

    def cell(c, s):
        if s < 0:
            return lo[c, s + WIDTH, spot, lanes]
        if s >= shells:
            return hi[c, s - shells, spot, lanes]
        return ext[c, s, pl.ds(PADR + at, ROWS), lanes]

    u = [[cell(c, s) for s in range(-WIDTH, shells + WIDTH)] for c in range(4)]
    last = None
    for f in range(shells + 1):
        place = r * shells + f
        face_radius = inner_radius + step_r * place.astype(f32)
        area = jnp.where((place > 0) & (place < n_rad * shells), face_radius * face_radius, 0.0)
        sums, jumps = [], []
        for c in range(4):
            w = u[c][f : f + 6]
            sums.append(37.0 * (w[2] + w[3]) - 8.0 * (w[1] + w[4]) + (w[0] + w[5]))
            jumps.append(w[3] - w[2])
        face = [value * area for value in flux(sums, jumps, 1)]
        if f > 0:
            for c in range(4):
                out[c, f - 1, out_spot, out_lanes] = (
                    section_step * tend[c, f - 1, spot, lanes] - (face[c] - last[c]) * sine
                )
        last = face
    return carry


def kernel(
    n_rad,
    n_ang,
    shells,
    rows,
    cols,
    x_ref,
    fwd_high_hbm,
    fwd_low_hbm,
    back_hbm,
    row_hbm,
    degree_hbm,
    log_hbm,
    tend,
    pot,
    ext,
    lo,
    hi,
    rowtab,
    lead,
    relay,
    row_relay,
    fields,
    table,
    spec,
    fwd_high_ref,
    fwd_low_ref,
    back_ref,
    degree_ref,
    log_ref,
    leg,
    partial,
    got_a,
    mine,
    got_b,
    totals,
    got_pair,
    chain_up,
    chain_down,
    coef,
    rounds,
    local_sem,
    ang_send,
    ang_recv,
    skip_recv,
    hand_send,
    rad_send,
    rad_recv,
    far_recv,
    pass_send,
    a_send,
    a_recv,
    b_send,
    b_recv,
    c_send,
    c_recv,
    d_send,
    d_recv,
):
    r = lax.axis_index("rad")
    a = lax.axis_index("ang")
    y, x_hi, core = a // 4, (a // 2) % 2, a % 2
    g = y * 2 + core
    chunks = rows // ROWS
    parts = chunks * CUTS
    wide = cols // CUTS
    n_far = parts - CUTS
    span = rows + 2 * PADR
    own = pl.ds(PADR, rows)
    step_r = radial_span / (n_rad * shells)
    step_t = math.pi / (n_ang * rows)
    step_p = 2.0 * math.pi / cols

    def peer(d):
        q = (g + d) % GROUPS
        return (r, (q // 2) * 4 + x_hi * 2 + q % 2)

    partner = (r, y * 4 + (1 - x_hi) * 2 + core)

    def when(cond, run):
        @pl.when(cond)
        def _():
            run()

    def remote(src, dst, send, recv, dev):
        return pltpu.make_async_remote_copy(
            src_ref=src,
            dst_ref=dst,
            send_sem=send,
            recv_sem=recv,
            device_id=dev,
            device_id_type=MESH,
        )

    load_density = pltpu.make_async_copy(x_ref.at[0], ext.at[0, :, own], local_sem.at[0])
    load_rest = pltpu.make_async_copy(
        x_ref.at[1:4], ext.at[1:4, :, own], local_sem.at[1]
    )
    load_rows = pltpu.make_async_copy(row_hbm.at[a], rowtab, local_sem.at[2])
    load_degree = pltpu.make_async_copy(degree_hbm, degree_ref, local_sem.at[3])
    load_high = pltpu.make_async_copy(fwd_high_hbm, fwd_high_ref, local_sem.at[4])
    load_low = pltpu.make_async_copy(fwd_low_hbm, fwd_low_ref, local_sem.at[5])
    load_log = pltpu.make_async_copy(log_hbm.at[r], log_ref, local_sem.at[6])
    load_back = pltpu.make_async_copy(back_hbm, back_ref, local_sem.at[7])
    barrier = pltpu.get_barrier_semaphore()
    first = a % 4 == 0
    last = a % 4 == 3
    odd = r % 2 == 1
    even = r % 2 == 0
    x = x_hi * 2 + r % 2

    def along_x(step):
        to = (x + step) % 4
        return ((r // 2) * 2 + to % 2, y * 4 + (to // 2) * 2 + core)

    near = [
        (x < 3, along_x(1)),
        (x > 0, along_x(3)),
        (r + 2 < n_rad, (r + 2, a)),
        (r - 2 >= 0, (r - 2, a)),
        (a + 4 < n_ang, (r, a + 4)),
        (a - 4 >= 0, (r, a - 4)),
        (None, (r, a + 1 - 2 * core)),
    ]
    n_near = 1
    for cond, _ in near:
        if cond is not None:
            n_near = n_near + jnp.where(cond, 1, 0)

    def greet(sem):
        for cond, dev in near:
            signal = functools.partial(
                pl.semaphore_signal, sem, inc=1, device_id=dev, device_id_type=MESH
            )
            if cond is None:
                signal()
            else:
                when(cond, signal)

    greet(barrier)
    edge = pl.ds(jnp.where(even, shells - WIDTH, 0), WIDTH)
    load_lead = pltpu.make_async_copy(
        x_ref.at[:, edge, 0:ROWS, 0:wide], lead, local_sem.at[8]
    )
    load_lead.start()
    for load in (load_rows, load_degree, load_density, load_high, load_low):
        load.start()
    for load in (load_rest, load_log, load_back):
        load.start()
    pl.semaphore_wait(barrier, n_near)

    deep = shells // QUARTERS
    rows_up, rows_down, skip_up, skip_down, hand_up, hand_down = [], [], [], [], [], []
    for c in range(QUARTERS):
        part = pl.ds(c * deep, deep)
        high = x_ref.at[:, part, rows - WIDTH : rows]
        low = x_ref.at[:, part, 0:WIDTH]
        under = ext.at[:, part, PADR - WIDTH : PADR]
        over = ext.at[:, part, PADR + rows : PADR + rows + WIDTH]
        up_sems = ang_send.at[0, c], ang_recv.at[0, c]
        down_sems = ang_send.at[1, c], ang_recv.at[1, c]
        rows_up.append(remote(high, under, *up_sems, (r, a + 1)))
        rows_down.append(remote(low, over, *down_sems, (r, a - 1)))
        if c < QUARTERS - 1:
            spot = row_relay.at[c]
            skip_up.append(remote(high, spot, up_sems[0], skip_recv.at[c], (r, a + 4)))
            skip_down.append(remote(low, spot, down_sems[0], skip_recv.at[c], (r, a - 4)))
            hand_up.append(remote(spot, under, hand_send.at[c], up_sems[1], (r, a - 3)))
            hand_down.append(remote(spot, over, hand_send.at[c], down_sems[1], (r, a + 3)))
    n_up_skip = jnp.where(last & (a + 1 < n_ang), y + 1, 0)
    n_down_skip = jnp.where(first & (a > 0), QUARTERS - y, 0)
    n_up_hand = jnp.where(last, y, 0)
    n_down_hand = jnp.where(first, QUARTERS - 1 - y, 0)

    def start_rows(c):
        when((a + 1 < n_ang) & (c >= n_up_skip), rows_up[c].start)
        when((a > 0) & (c >= n_down_skip), rows_down[c].start)

    def start_skip(c):
        when(c < n_up_skip, skip_up[c].start)
        when(c < n_down_skip, skip_down[c].start)

    def hand_on(c):
        @pl.when(c < n_up_hand)
        def _():
            skip_up[c].wait_recv()
            hand_up[c].start()

        @pl.when(c < n_down_hand)
        def _():
            skip_down[c].wait_recv()
            hand_down[c].start()

    rad_up, rad_down, far_up, far_down, pass_up, pass_down = [], [], [], [], [], []
    for c in range(parts):
        part = pl.ds((c // CUTS) * ROWS, ROWS)
        band = pl.ds((c % CUTS) * wide, wide)
        above = x_ref.at[:, shells - WIDTH : shells, part, band]
        below = x_ref.at[:, 0:WIDTH, part, band]
        lo_part, hi_part = lo.at[:, :, part, band], hi.at[:, :, part, band]
        up_sems = rad_send.at[0, c], rad_recv.at[0, c]
        down_sems = rad_send.at[1, c], rad_recv.at[1, c]
        if c < CUTS:
            near_above, near_below = above, below
        else:
            held = pl.ds(PADR + (c // CUTS) * ROWS, ROWS)
            near_above = ext.at[:, shells - WIDTH : shells, held, band]
            near_below = ext.at[:, 0:WIDTH, held, band]
        rad_up.append(remote(near_above, lo_part, *up_sems, (r + 1, a)))
        rad_down.append(remote(near_below, hi_part, *down_sems, (r - 1, a)))
        if c < n_far:
            spot = relay.at[c]
            far_up.append(remote(above, spot, up_sems[0], far_recv.at[c], (r + 2, a)))
            far_down.append(remote(below, spot, down_sems[0], far_recv.at[c], (r - 2, a)))
            pass_up.append(remote(spot, lo_part, pass_send.at[c], up_sems[1], (r - 1, a)))
            pass_down.append(remote(spot, hi_part, pass_send.at[c], down_sems[1], (r + 1, a)))
    n_up_far = jnp.where(odd & (r + 2 < n_rad), CUTS * ((r + 1) // 2), 0)
    n_down_far = jnp.where(even & (r > 0), parts - CUTS * (r // 2), 0)
    n_up_pass = jnp.where(odd & (r > 1), CUTS * ((r - 1) // 2), 0)
    n_down_pass = jnp.where(even & (r + 2 < n_rad), n_far - CUTS * (r // 2), 0)

    def start_far(c):
        when(c < n_up_far, far_up[c].start)
        when(c < n_down_far, far_down[c].start)

    lead_to = pl.ds(0, ROWS), pl.ds(0, wide)
    lead_up = remote(
        lead, lo.at[:, :, *lead_to], rad_send.at[0, 0], rad_recv.at[0, 0], (r + 1, a)
    )
    lead_down = remote(
        lead, hi.at[:, :, *lead_to], rad_send.at[1, 0], rad_recv.at[1, 0], (r - 1, a)
    )

    def start_pair(c):
        when(even, rad_up[c].start)
        when(odd, rad_down[c].start)

    def start_diagonal(c):
        when(odd & (r + 1 < n_rad) & (c >= n_up_far), rad_up[c].start)
        when(even & (r > 0) & (c >= n_down_far), rad_down[c].start)

    def start_chunk(c):
        start_pair(c)
        start_diagonal(c)

    def pass_on(c):
        @pl.when(c < n_up_pass)
        def _():
            far_up[c].wait_recv()
            pass_up[c].start()

        @pl.when(c < n_down_pass)
        def _():
            far_down[c].wait_recv()
            pass_down[c].start()

    load_lead.wait()
    when(even, lead_up.start)
    when(odd, lead_down.start)
    greet(rounds.at[0])
    for c in range(n_far):
        start_far(c)
    for c in range(QUARTERS - 1):
        start_skip(c)
    for c in range(1, CUTS):
        start_pair(c)
    pl.semaphore_wait(rounds.at[0], n_near)
    greet(rounds.at[1])
    for c in range(CUTS):
        start_diagonal(c)
    pl.semaphore_wait(rounds.at[1], n_near)
    greet(rounds.at[2])
    pl.semaphore_wait(rounds.at[2], n_near)
    for c in range(QUARTERS):
        start_rows(c)

    @pl.when(a == 0)
    def _():
        ext[:, :, 0:PADR, :] = jnp.zeros((4, shells, PADR, cols), f32)

    @pl.when(a == n_ang - 1)
    def _():
        ext[:, :, PADR + rows : span, :] = jnp.zeros((4, shells, PADR, cols), f32)

    @pl.when(r == 0)
    def _():
        lo[...] = jnp.zeros_like(lo)

    @pl.when(r == n_rad - 1)
    def _():
        hi[...] = jnp.zeros_like(hi)

    @pl.when(r < 2)
    def _():
        chain_up[1:] = jnp.zeros((n_rad // 2 - 1, 8, LANES), f32)

    @pl.when(r + 2 >= n_rad)
    def _():
        chain_down[1:] = jnp.zeros((n_rad // 2 - 1, 8, LANES), f32)

    load_rows.wait()
    load_degree.wait()
    cosine = jnp.broadcast_to(rowtab[:, 0:1], (span, LANES))
    sine = jnp.broadcast_to(rowtab[:, 1:2], (span, LANES))
    order = lax.broadcasted_iota(jnp.int32, (span, LANES), 1) % MPAD
    power = jnp.full((span, LANES), 1.0, f32)
    square = sine
    for bit in range(6):
        power = jnp.where((order // (1 << bit)) % 2 == 1, power * square, power)
        square = square * square
    level = power * degree_ref[0:1, :]
    leg[0] = level

    def next_level(k, carry):
        last, before = carry
        alpha = degree_ref[pl.ds(k, 1), :]
        beta = degree_ref[pl.ds(NK + k, 1), :]
        new = alpha * (cosine * last - beta * before)
        leg[k] = new
        return (new, last)

    lax.fori_loop(1, NK, next_level, (level, jnp.zeros_like(level)))

    for c in range(QUARTERS - 1):
        hand_on(c)

    load_density.wait()
    load_high.wait()
    load_low.wait()
    weight = sine[PADR : PADR + rows] * (step_t * step_p)
    half = shells // 2
    for h in range(2):
        cells = ext[0, h * half : (h + 1) * half, PADR : PADR + rows, :]
        high, low = split(cells.reshape(half * rows, cols))
        sums = dot(high, fwd_high_ref[...]) + (
            dot(low, fwd_high_ref[...]) + dot(high, fwd_low_ref[...])
        )
        for q in range(half):
            spec[pl.ds((h * half + q) * rows, rows), :] = (
                sums[q * rows : (q + 1) * rows] * weight
            )
    spectra = [spec[pl.ds(j, shells, stride=rows), :] for j in range(rows)]

    def moment(k, carry):
        parts = [jnp.zeros((shells, LANES), f32) for _ in range(4)]
        for j in range(rows):
            parts[j % 4] = parts[j % 4] + spectra[j] * leg[k, PADR + j : PADR + j + 1, :]
        partial[k // KD, k % KD] = (parts[0] + parts[1]) + (parts[2] + parts[3])
        return carry

    lax.fori_loop(0, NK, moment, 0)

    def exchange_a(d):
        return remote(
            partial.at[(g + d) % GROUPS], got_a.at[d], a_send.at[d], a_recv.at[d], peer(d)
        )

    for d in range(1, GROUPS):
        exchange_a(d).start()

    load_rest.wait()

    def phi_flux(index, carry):
        i = index // chunks
        at = pl.multiple_of((index % chunks) * ROWS, ROWS)
        cell_radius = inner_radius + step_r * ((r * shells + i).astype(f32) + 0.5)
        sums, jumps = [], []
        for c in range(4):
            u = ext[c, i, pl.ds(PADR + at, ROWS), :]
            left = pltpu.roll(u, 1, 1)
            near = u + left
            mid = pltpu.roll(u, cols - 1, 1) + pltpu.roll(u, 2, 1)
            far = pltpu.roll(u, cols - 2, 1) + pltpu.roll(u, 3, 1)
            sums.append(37.0 * near - 8.0 * mid + far)
            jumps.append(u - left)
        for c, face in enumerate(flux(sums, jumps, 3)):
            tend[c, i, pl.ds(at, ROWS), :] = (face - pltpu.roll(face, cols - 1, 1)) * (
                cell_radius / step_p
            )
        return carry

    lax.fori_loop(0, shells * chunks // 2, phi_flux, 0)

    for d in range(1, GROUPS):
        exchange_a(d).wait_recv()
    total = partial[g]
    for d in range(1, GROUPS):
        total = total + got_a[d]
    mine[...] = total
    exchange_b = remote(mine, got_b, b_send.at[0], b_recv.at[0], partner)
    exchange_b.start()
    for c in range(CUTS, 2 * CUTS):
        start_chunk(c)

    lax.fori_loop(shells * chunks // 2, shells * chunks, phi_flux, 0)

    for c in range(QUARTERS):
        when(a > 0, rows_up[c].wait_recv)
        when(a + 1 < n_ang, rows_down[c].wait_recv)
    tiles = cols // LANES

    def theta_flux(index, carry):
        i = index // tiles
        lanes = pl.ds(pl.multiple_of((index % tiles) * LANES, LANES), LANES)
        cell_radius = inner_radius + step_r * ((r * shells + i).astype(f32) + 0.5)
        area = jnp.broadcast_to(rowtab[:, 2:3], (span, LANES)) * (cell_radius / step_t)
        sums, jumps = [], []
        for c in range(4):
            u = ext[c, i, :, lanes]
            left = pltpu.roll(u, 1, 0)
            near = u + left
            mid = pltpu.roll(u, span - 1, 0) + pltpu.roll(u, 2, 0)
            far = pltpu.roll(u, span - 2, 0) + pltpu.roll(u, 3, 0)
            sums.append(37.0 * near - 8.0 * mid + far)
            jumps.append(u - left)
        for c, face in enumerate(flux(sums, jumps, 2)):
            face = face * area
            change = face - pltpu.roll(face, span - 1, 0)
            tend[c, i, :, lanes] = tend[c, i, :, lanes] + change[PADR : PADR + rows]
        return carry

    lax.fori_loop(0, shells * tiles // 4, theta_flux, 0)

    exchange_b.wait_recv()
    total = mine[...] + got_b[...]
    load_log.wait()
    log_radius = log_ref[...]
    shell = lax.broadcasted_iota(jnp.int32, (shells, LANES), 0)
    radius = inner_radius + step_r * ((r * shells + shell).astype(f32) + 0.5)
    order = lax.broadcasted_iota(jnp.int32, (shells, LANES), 1) % MPAD
    ups, downs, powers, degrees = [], [], [], []
    for q in range(KD):
        degree = (order + (g * KD + q)).astype(f32)
        grow = jnp.exp(degree * log_radius)
        weighted = (radius * radius * step_r) * total[q]
        up = grow * weighted
        down = weighted / (radius * grow)
        for s in (1, 2, 4):
            up = up + jnp.where(shell >= s, pltpu.roll(up, s, 0), 0.0)
            down = down + jnp.where(shell >= s, pltpu.roll(down, s, 0), 0.0)
        totals[0, q : q + 1, :] = up[shells - 1 : shells]
        totals[1, q : q + 1, :] = down[shells - 1 : shells]
        ups.append(up)
        downs.append(down)
        powers.append(grow)
        degrees.append(degree)

    pair = remote(totals, got_pair, c_send.at[0, 0], c_recv.at[0, 0], (r + 1 - 2 * (r % 2), a))
    pair.start()

    def hop_up(d):
        return remote(
            chain_up.at[d - 1], chain_up.at[d], c_send.at[0, d], c_recv.at[0, d], (r + 2, a)
        )

    def hop_down(d):
        return remote(
            chain_down.at[d - 1], chain_down.at[d], c_send.at[1, d], c_recv.at[1, d], (r - 2, a)
        )

    def start_hop(d):
        when(r + 2 < n_rad, hop_up(d).start)
        when(r - 2 >= 0, hop_down(d).start)

    def end_hop(d):
        when(r - 2 >= 0, hop_up(d).wait_recv)
        when(r + 2 < n_rad, hop_down(d).wait_recv)

    for c in range(2 * CUTS, 3 * CUTS):
        pass_on(c - 2 * CUTS)
        start_chunk(c)
    for c in range(CUTS, 2 * CUTS):
        pass_on(c)

    quarter = shells * tiles // 4
    lax.fori_loop(quarter, 2 * quarter, theta_flux, 0)
    pair.wait_recv()
    pair_up = got_pair[0]
    pair_down = got_pair[1]
    chain_up[0] = totals[0] + pair_up
    chain_down[0] = totals[1] + pair_down
    start_hop(1)
    lax.fori_loop(2 * quarter, 3 * quarter, theta_flux, 0)
    end_hop(1)
    start_hop(2)
    lax.fori_loop(3 * quarter, 4 * quarter, theta_flux, 0)
    end_hop(2)
    start_hop(3)
    below = jnp.where(odd, pair_up, 0.0)
    above = jnp.where(even, pair_down, 0.0)
    end_hop(3)
    for d in range(1, n_rad // 2):
        below = below + chain_up[d]
        above = above + chain_down[d]
    inverse_radius = 1.0 / radius
    for q in range(KD):
        inner = below[q : q + 1] + ups[q]
        outer = above[q : q + 1] + (downs[q][shells - 1 : shells] - downs[q])
        degree = degrees[q]
        norm = (-4.0 * math.pi) / (2.0 * degree + 1.0)
        inner_term = inner * inverse_radius / powers[q]
        outer_term = powers[q] * outer
        coef[g, 0, q] = norm * (inner_term + outer_term)
        coef[g, 1, q] = (
            norm * (degree * outer_term - (degree + 1.0) * inner_term) * inverse_radius
        )

    def exchange_d(d):
        return remote(coef.at[g], coef.at[g], d_send.at[d], d_recv.at[d], peer(d))

    for d in range(1, GROUPS):
        exchange_d(d).start()
    for c in range(2 * CUTS, 3 * CUTS):
        pass_on(c)
        start_chunk(c + CUTS)
    for d in range(1, GROUPS):
        exchange_d(d).wait_recv()

    slope_row = degree_ref[2 * NK : 2 * NK + 1, :]
    theta_scale = 1.0 / (2.0 * step_t)
    for i in range(0, shells, 2):

        def synthesize(h, carry):
            sums = list(carry)
            for q in range(KD):
                k = h * KD + q
                full = leg[k]
                value = full[PADR : PADR + rows]
                change = pltpu.roll(full, span - 1, 0) - pltpu.roll(full, 1, 0)
                change = change[PADR : PADR + rows]
                for p in range(2):
                    cp = coef[h, 0, q, i + p : i + p + 1, :]
                    cs = coef[h, 1, q, i + p : i + p + 1, :]
                    sums[3 * p] = sums[3 * p] + value * cp
                    sums[3 * p + 1] = sums[3 * p + 1] + value * cs
                    sums[3 * p + 2] = sums[3 * p + 2] + change * cp
            return tuple(sums)

        zero = jnp.zeros((rows, LANES), f32)
        sums = lax.fori_loop(0, (LMAX + KD) // KD, synthesize, (zero,) * 6)
        for p in range(2):
            base, slope, change = sums[3 * p : 3 * p + 3]
            at = (i + p) * 4 * rows
            table[at : at + rows, :] = base
            table[at + rows : at + 2 * rows, :] = slope
            table[at + 2 * rows : at + 3 * rows, :] = change * theta_scale
            table[at + 3 * rows : at + 4 * rows, :] = pltpu.roll(base, MPAD, 1) * slope_row

    load_back.wait()

    def sources(i, carry):
        at = pl.multiple_of(i * 4 * rows, 4 * rows)
        high, low = split(table[pl.ds(at, 4 * rows), :])
        fields[...] = dot(jnp.concatenate([high, low, high], axis=1), back_ref[...])
        pot[i] = fields[0:rows, :]
        cell_radius = inner_radius + step_r * ((r * shells + i).astype(f32) + 0.5)
        for c in range(chunks):
            at = c * ROWS
            inside = pl.ds(PADR + at, ROWS)
            sine = jnp.broadcast_to(rowtab[inside, 1:2], (ROWS, cols)) * cell_radius
            cosine = jnp.broadcast_to(rowtab[inside, 0:1], (ROWS, cols)) * cell_radius
            density = ext[0, i, inside, :]
            mom_r = ext[1, i, inside, :]
            mom_t = ext[2, i, inside, :]
            mom_p = ext[3, i, inside, :]
            inverse = 1.0 / density
            vel_t = mom_t * inverse
            vel_p = mom_p * inverse
            pull = grav_const * density
            slope = fields[rows + at : rows + at + ROWS, :]
            grad_t = fields[2 * rows + at : 2 * rows + at + ROWS, :]
            grad_p = fields[3 * rows + at : 3 * rows + at + ROWS, :]
            twist = mom_p * vel_p
            source_r = sine * (
                (mom_t * vel_t + twist)
                + (2.0 * sound_sq) * density
                - (cell_radius * pull) * slope
            )
            source_t = cosine * (twist + sound_sq * density) - sine * (
                mom_r * vel_t + pull * grad_t
            )
            source_p = -(
                vel_p * (mom_r * sine + mom_t * cosine) + (cell_radius * pull) * grad_p
            )
            spot = pl.ds(at, ROWS)
            tend[1, i, spot, :] = tend[1, i, spot, :] + source_r
            tend[2, i, spot, :] = tend[2, i, spot, :] + source_t
            tend[3, i, spot, :] = tend[3, i, spot, :] + source_p
        return carry

    lax.fori_loop(0, shells, sources, 0)

    per = wide // LANES
    for chunk in range(parts):
        when(r > 0, rad_up[chunk].wait_recv)
        when(r + 1 < n_rad, rad_down[chunk].wait_recv)
        if chunk < parts - 1:
            at = (chunk // CUTS) * ROWS
            first = (chunk % CUTS) * per
            radial_tile = functools.partial(
                radial_flux, r, n_rad, shells, at, 0, at, ext, lo, hi, rowtab, tend, tend
            )
            lax.fori_loop(first, first + per, radial_tile, 0)

    for c in range(QUARTERS):
        when(a + 1 < n_ang, rows_up[c].wait_send)
        when(a > 0, rows_down[c].wait_send)
        if c < QUARTERS - 1:
            when((c < n_up_hand) | (c < n_down_hand), hand_up[c].wait_send)
    for c in range(parts):
        when(r + 1 < n_rad, rad_up[c].wait_send)
        when(r > 0, rad_down[c].wait_send)
        if c < n_far:
            when((c < n_up_pass) | (c < n_down_pass), pass_up[c].wait_send)
    for d in range(1, GROUPS):
        exchange_a(d).wait_send()
        exchange_d(d).wait_send()
    exchange_b.wait_send()
    pair.wait_send()
    for d in range(1, n_rad // 2):
        when(r + 2 < n_rad, hop_up(d).wait_send)
        when(r - 2 >= 0, hop_down(d).wait_send)


def close(n_rad, tend, pot, ext, lo, hi, rowtab, inc_ref, pot_ref, final, sem):
    _, shells, rows, cols = tend.shape
    ahead = pl.ds(0, rows - ROWS)
    behind = pl.ds(rows - ROWS, ROWS)
    done = pl.ds(0, cols - cols // CUTS)
    rest = pl.ds(cols - cols // CUTS, cols // CUTS)
    copies = [
        pltpu.make_async_copy(tend.at[c, half, ahead], inc_ref.at[c, half, ahead], sem.at[7 + k])
        for k, (c, half) in enumerate(
            (c, pl.ds(h * (shells // 2), shells // 2)) for c in range(4) for h in range(2)
        )
    ]
    copies.append(
        pltpu.make_async_copy(
            tend.at[:, :, behind, done], inc_ref.at[:, :, behind, done], sem.at[4]
        )
    )
    copies.append(pltpu.make_async_copy(pot, pot_ref, sem.at[5]))
    for copy in copies:
        copy.start()
    r = lax.axis_index("rad")
    tiles = cols // LANES
    start = tiles - tiles // CUTS
    radial_tile = functools.partial(
        radial_flux, r, n_rad, shells, rows - ROWS, start, 0, ext, lo, hi, rowtab, tend, final
    )
    lax.fori_loop(start, tiles, radial_tile, 0)
    copies.append(
        pltpu.make_async_copy(final, inc_ref.at[:, :, behind, rest], sem.at[6])
    )
    copies[-1].start()
    for copy in copies:
        copy.wait()


def solution(mesh):
    n_rad = mesh.shape["rad"]
    n_ang = mesh.shape["ang"]

    def body(state):
        _, shells, rows, cols = state.shape
        high, low, back, slope = phi_tables(cols)
        operands = (
            state,
            jnp.asarray(high),
            jnp.asarray(low),
            jnp.asarray(back),
            jnp.asarray(row_tables(n_ang, rows)),
            jnp.asarray(degree_tables(slope)),
            jnp.asarray(log_radii(n_rad, shells)),
        )
        span = rows + 2 * PADR
        parts = (rows // ROWS) * CUTS
        inside = pl.BlockSpec(memory_space=pltpu.VMEM)
        dma = pltpu.SemaphoreType.DMA
        results = pl.pallas_call(
            functools.partial(kernel, n_rad, n_ang, shells, rows, cols),
            out_shape=(
                pltpu.VMEM(state.shape, f32),
                pltpu.VMEM(state.shape[1:], f32),
                pltpu.VMEM((4, shells, span, cols), f32),
                pltpu.VMEM((4, WIDTH, rows, cols), f32),
                pltpu.VMEM((4, WIDTH, rows, cols), f32),
                pltpu.VMEM((span, LANES), f32),
            ),
            in_specs=[pl.BlockSpec(memory_space=pltpu.HBM)] * 7,
            out_specs=(inside,) * 6,
            scratch_shapes=[
                pltpu.VMEM((4, WIDTH, ROWS, cols // CUTS), f32),
                pltpu.VMEM((parts - CUTS, 4, WIDTH, ROWS, cols // CUTS), f32),
                pltpu.VMEM((QUARTERS - 1, 4, shells // QUARTERS, WIDTH, cols), f32),
                pltpu.VMEM((4 * rows, cols), f32),
                pltpu.VMEM((shells * 4 * rows, LANES), f32),
                pltpu.VMEM((shells * rows, LANES), f32),
                pltpu.VMEM((cols, LANES), bf16),
                pltpu.VMEM((cols, LANES), bf16),
                pltpu.VMEM((3 * LANES, cols), bf16),
                pltpu.VMEM((2 * NK + 8, LANES), f32),
                pltpu.VMEM((shells, LANES), f32),
                pltpu.VMEM((NK, span, LANES), f32),
                pltpu.VMEM((GROUPS, KD, shells, LANES), f32),
                pltpu.VMEM((GROUPS, KD, shells, LANES), f32),
                pltpu.VMEM((KD, shells, LANES), f32),
                pltpu.VMEM((KD, shells, LANES), f32),
                pltpu.VMEM((2, 8, LANES), f32),
                pltpu.VMEM((2, 8, LANES), f32),
                pltpu.VMEM((n_rad // 2, 8, LANES), f32),
                pltpu.VMEM((n_rad // 2, 8, LANES), f32),
                pltpu.VMEM((GROUPS, 2, KD, shells, LANES), f32),
                pltpu.SemaphoreType.REGULAR((3,)),
                dma((9,)),
                dma((2, QUARTERS)),
                dma((2, QUARTERS)),
                dma((QUARTERS - 1,)),
                dma((QUARTERS - 1,)),
                dma((2, parts)),
                dma((2, parts)),
                dma((parts - CUTS,)),
                dma((parts - CUTS,)),
                dma((GROUPS,)),
                dma((GROUPS,)),
                dma((1,)),
                dma((1,)),
                dma((2, n_rad // 2)),
                dma((2, n_rad // 2)),
                dma((GROUPS,)),
                dma((GROUPS,)),
            ],
            compiler_params=pltpu.CompilerParams(
                collective_id=0, has_side_effects=True, vmem_limit_bytes=52_200_000
            ),
        )(*operands)
        outside = pl.BlockSpec(memory_space=pltpu.HBM)
        return pl.pallas_call(
            functools.partial(close, n_rad),
            out_shape=(
                jax.ShapeDtypeStruct(state.shape, f32),
                jax.ShapeDtypeStruct(state.shape[1:], f32),
            ),
            in_specs=(inside,) * 6,
            out_specs=(outside, outside),
            scratch_shapes=[
                pltpu.VMEM((4, shells, ROWS, cols // CUTS), f32),
                dma((15,)),
            ],
            compiler_params=pltpu.CompilerParams(vmem_limit_bytes=4 << 20),
        )(*results)

    return jax.shard_map(
        body,
        mesh=mesh,
        in_specs=(P(None, "rad", "ang", None),),
        out_specs=(P(None, "rad", "ang", None), P("rad", "ang", None)),
        check_vma=False,
    )
```
